512 devices in a mesh: dp: 32 (over x, z), patch: 16 (over y, core).
Axes of the slice: x: 4, y: 8, z: 8, core: 2. Of those that a mesh axis runs over, the one named last changes fastest.
Arguments:
- query_rows: bfloat16 [32, 2048, 576], P('dp', 'patch'), may hold values from -6 to 6
- key_rows: bfloat16 [32, 2048, 576], P('dp', 'patch'), may hold values from -6 to 6
- value_rows: bfloat16 [32, 2048, 576], P('dp', 'patch'), may hold values from -6 to 6
- out_weight: bfloat16 [576, 1152], replicated, may hold values from -0.25 to 0.25
- target: bfloat16 [32, 2048, 1152], P('dp', 'patch'), may hold values from -6 to 6
- lengths: int32 [32], P('dp'), may hold values from 256 to 2048
- segments: int32 [32, 2048], P('dp', 'patch'), may hold values from 0 to 7, never falling along the last dimension, each value on 1 to 1024 neighbouring positions
Outputs:
- query_grad: float32 [32, 2048, 576], P('dp', 'patch')
- key_grad: float32 [32, 2048, 576], P('dp', 'patch')
- value_grad: float32 [32, 2048, 576], P('dp', 'patch')
- weight_grad: float32 [576, 1152], P('patch', 'dp')
- loss: float32 [], replicated
The draws below stay inside these ranges and needn't reach their ends.
All inputs are finite; a program needn't handle non-finite values.
Results may differ from the reference program's by a relative error of at most 0.024.
Values may be sent and summed in bfloat16 or wider, within the bound.
A program may use at most 64 MiB of HBM per device.

```python
import math
import jax
import jax.numpy as jnp
import numpy as np
from jax import lax

WIDTH = 1152
HEADS = 8
HEAD_DIM = 72
TOK_DEV = 128
FEAT = 576
SEQ = 2048
SAMPLES = 32


def draw_rows(key, salt, chosen_rows):
    fresh_key = jax.random.fold_in(key, salt)
    sampled = jnp.clip(1.5 * jax.random.normal(fresh_key, (SAMPLES, SEQ, FEAT), jnp.float32), -6.0, 6.0)
    return sampled.astype(jnp.bfloat16)


def draw_query_rows(key, part):
    positions = jnp.arange(SEQ)
    return draw_rows(key, 1, positions % TOK_DEV == 0)


def draw_key_rows(key, part):
    positions = jnp.arange(SEQ)
    return draw_rows(key, 2, positions % TOK_DEV == 0)


def plant(entries, key, low, largest):
    longest = entries.shape.index(max(entries.shape))
    spots = []
    for shift in (0, 1):
        where = [jax.random.randint(jax.random.fold_in(key, axis), (), 0, length) for axis, length in enumerate(entries.shape)]
        where[longest] = (where[longest] + shift) % entries.shape[longest]
        spots.append(tuple(where))
    return entries.at[spots[0]].set(low).at[spots[1]].set(largest)


def steps_of(stream_key, extent, split, least, largest):
    level = 1.0
    for position, shards_of in split:
        heights = jax.random.uniform(jax.random.fold_in(jax.random.fold_in(stream_key, 6), position), (shards_of,), jnp.float32, least / len(split), largest / len(split))
        level = level * jnp.repeat(jnp.exp(heights), extent[position] // shards_of).reshape((-1,) + (1,) * (len(extent) - 1 - position))
    return level


def profile(count, total, most, skew):
    weights = [(1 << 20) // math.isqrt(rank ** skew) + 1 for rank in range(2, count + 1)]
    surplus, counts = total - most - (count - 1), [1] * (count - 1)
    while surplus > 0:
        candidates = [i for i in range(count - 1) if counts[i] < most]
        pool, remaining = sum([weights[i] for i in candidates]), surplus
        for i in candidates:
            more = min(most - counts[i], max(1, remaining * weights[i] // pool), surplus)
            counts[i] = counts[i] + more
            surplus = surplus - more
    return np.array([most] + counts)


def uneven_parts(key, number_of, total, most, skew):
    if number_of == 2:
        one = jax.random.randint(key, (), max(1, total - most), min(most, total - 1) + 1)
        return jnp.stack([one, total - one])
    tallies = jnp.asarray(profile(number_of, total, most, skew), jnp.int32)
    pairs = (number_of - 1) // 2
    donor, sink = tallies[1:1 + 2 * pairs:2], tallies[2:2 + 2 * pairs:2]
    slack = jnp.minimum(donor - 1, most - sink)
    shifted = jax.random.randint(jax.random.fold_in(key, 1), (pairs,), 0, 1 << 20) % (slack + 1)
    tallies = tallies.at[1:1 + 2 * pairs:2].set(donor - shifted).at[2:2 + 2 * pairs:2].set(sink + shifted)
    return tallies[jax.random.permutation(jax.random.fold_in(key, 2), number_of)]


def normal_values(rng, shape, spread, most, split=(), kind=jnp.bfloat16):
    array = spread * jax.random.normal(rng, shape, jnp.float32)
    if split:
        array = array * steps_of(rng, shape, split, -0.22, 0.18)
    return jnp.clip(array, -most, most).astype(kind)


def setup_inputs(seed: int = 0) -> dict:
    arg_keys = jax.random.split(jax.random.key(seed), 8)
    query_rows = draw_query_rows(jax.random.fold_in(arg_keys[7], 71), 0)
    key_rows = draw_key_rows(jax.random.fold_in(arg_keys[7], 71), 0)
    value_rows = normal_values(arg_keys[2], (SAMPLES, SEQ, FEAT), 1.0, 6.0, ((0, 32), (1, 16)))
    out_weight = normal_values(arg_keys[3], (FEAT, WIDTH), FEAT ** -0.5, 0.25)
    target = normal_values(arg_keys[4], (SAMPLES, SEQ, WIDTH), 1.0, 6.0, ((0, 32), (1, 16)))
    lengths = plant(jax.random.randint(arg_keys[5], (SAMPLES,), SEQ // 8, SEQ + 1), jax.random.fold_in(arg_keys[5], 1), SEQ // 8, SEQ).astype(jnp.int32)
    segments = jax.vmap(lambda own: jnp.searchsorted(jnp.cumsum(uneven_parts(own, 8, SEQ, SEQ // 2, 2)), jnp.arange(SEQ), side="right"))(jax.random.split(arg_keys[6], SAMPLES)).reshape((SAMPLES, SEQ)).astype(jnp.int32)
    return {"query_rows": query_rows, "key_rows": key_rows, "value_rows": value_rows, "out_weight": out_weight, "target": target, "lengths": lengths, "segments": segments}


NEG_LARGE = -1e+30

def widen(value):
    return lax.optimization_barrier(value).astype(jnp.float32)

def one_sample(packed, out_weight):
    query_rows, key_rows, value_rows, target_rows, length, segment_row = packed
    score_scale = 1.0 / math.sqrt(HEAD_DIM)
    query_heads = query_rows.astype(jnp.float32).reshape(SEQ, HEADS, HEAD_DIM)
    key_heads = key_rows.astype(jnp.float32).reshape(SEQ, HEADS, HEAD_DIM)
    value_heads = value_rows.astype(jnp.float32).reshape(SEQ, HEADS, HEAD_DIM)
    live = lax.iota(jnp.int32, SEQ) < length
    group = jnp.where(live, segment_row, -1)
    allowed = (group[:, None] == group[None, :])[None, :, :]
    scores = jnp.einsum('qhe,khe->hqk', query_heads, key_heads) * score_scale
    masked = jnp.where(allowed, scores, NEG_LARGE)
    row_max = lax.optimization_barrier(jnp.max(masked, axis=2))
    probs = jnp.where(allowed, jnp.exp(masked - row_max[:, :, None]), 0.0)
    denom = lax.optimization_barrier(jnp.sum(probs, axis=2))
    weights = widen(probs.astype(jnp.bfloat16))
    accum = jnp.einsum('hqk,khe->qhe', weights, value_heads)
    attn = (accum / denom.T[:, :, None]).reshape(SEQ, FEAT).astype(jnp.bfloat16)
    log_norm = row_max + jnp.log(denom)
    output = jnp.dot(attn, out_weight, preferred_element_type=jnp.float32)
    error = jnp.where(live[:, None], output - target_rows.astype(jnp.float32), 0.0)
    grad_out = (2.0 * error).astype(jnp.bfloat16)
    attn_wide = widen(attn)
    grad_wide = widen(grad_out)
    weight_part = jnp.einsum('tf,td->fd', attn_wide, grad_wide)
    grad_attn = jnp.einsum('td,fd->tf', grad_wide, out_weight.astype(jnp.float32)).astype(jnp.bfloat16)
    grad_attn_wide = widen(grad_attn)
    delta = lax.optimization_barrier(jnp.sum((grad_attn_wide * attn_wide).reshape(SEQ, HEADS, HEAD_DIM), axis=2)).T
    back_probs = jnp.where(allowed, jnp.exp(masked - log_norm[:, :, None]), 0.0)
    grad_heads = grad_attn_wide.reshape(SEQ, HEADS, HEAD_DIM)
    dprobs = jnp.einsum('qhe,khe->hqk', grad_heads, value_heads)
    dscores = widen((back_probs * (dprobs - delta[:, :, None])).astype(jnp.bfloat16))
    query_raw = jnp.einsum('hqk,khe->qhe', dscores, key_heads) * score_scale
    key_raw = jnp.einsum('hqk,qhe->khe', dscores, query_heads) * score_scale
    back_weights = widen(back_probs.astype(jnp.bfloat16))
    value_raw = jnp.einsum('hqk,qhe->khe', back_weights, grad_heads)
    return (query_raw.reshape(SEQ, FEAT), key_raw.reshape(SEQ, FEAT), value_raw.reshape(SEQ, FEAT), weight_part, jnp.sum(error * error))

def reference(query_rows, key_rows, value_rows, out_weight, target, lengths, segments):

    def per_sample(packed):
        return one_sample(packed, out_weight)
    results = lax.map(per_sample, (query_rows, key_rows, value_rows, target, lengths, segments))
    count = jnp.sum(lengths).astype(jnp.float32)
    ratio = jnp.float32(SAMPLES * SEQ) / count
    query_grad = ratio * results[0]
    key_grad = ratio * results[1]
    value_grad = ratio * results[2]
    weight_grad = lax.optimization_barrier(jnp.sum(results[3], axis=0)) * (ratio / SEQ)
    loss = jnp.sum(results[4]) / (count * WIDTH)
    return (query_grad, key_grad, value_grad, weight_grad, loss)
```

```python
import functools
import math

import jax
import jax.numpy as jnp
from jax import lax
from jax.experimental import pallas as pl
from jax.experimental.pallas import tpu as pltpu
from jax.sharding import PartitionSpec as P

MESH = pl.DeviceIdType.MESH
WIDTH = 1152
HEADS = 8
HEAD_DIM = 72
FEAT = 576
FEAT_PAD = 640
FM = 80
LANES = 128
SPAN = 256
TILE = 256
CHUNK = 512
NEG_LARGE = -1e30
F32 = jnp.float32
BF16 = jnp.bfloat16
XS, ZS = 4, 8
ZH = ZS // 2


def nt(left, right):
    return lax.dot_general(left, right, (((1,), (1,)), ((), ())), preferred_element_type=F32)


def nn(left, right):
    return lax.dot_general(left, right, (((1,), (0,)), ((), ())), preferred_element_type=F32)


def tn(left, right):
    return lax.dot_general(left, right, (((0,), (0,)), ((), ())), preferred_element_type=F32)


def span_start(owner, features):
    return pl.multiple_of(jnp.minimum(owner * features // 128 * 128, FEAT_PAD - SPAN), 128)


def kernel(
    members,
    groups,
    len_ref,
    seg_ref,
    q_ref,
    k_ref,
    v_ref,
    w_hbm,
    t_hbm,
    dq_ref,
    dk_ref,
    dv_ref,
    dw_ref,
    sum_ref,
    q_in,
    k_in,
    v_in,
    w_ref,
    t_ref,
    seg_row,
    seg_all,
    q_slab,
    k_slab,
    v_slab,
    k_tm,
    v_tm,
    k_fm,
    v_fm,
    q_fm,
    g_fm,
    qs_fm,
    gs_fm,
    s_ref,
    p_ref,
    ds_ref,
    att_out,
    attn_all,
    attn_tm,
    dout_ref,
    g_out,
    g_slab,
    xv_out,
    xv_in,
    xk_out,
    xk_in,
    v_own,
    k_own,
    oq,
    ok,
    ov,
    part_ref,
    w1_ref,
    sum1_ref,
    keep_ref,
    w2_ref,
    wz_ref,
    w3_ref,
    fin_ref,
    w4_ref,
    tile_own,
    tile_all,
    sum_own,
    sum_all,
    load_sem,
    send_sem,
    seg_recv,
    q_recv,
    k_recv,
    v_recv,
    attn_recv,
    g_recv,
    xv_recv,
    xk_recv,
    dq_recv,
    dk_recv,
    dv_recv,
    tile_recv,
    sum_recv,
    r1,
    r2,
    r3,
    r4,
):
    rows = t_ref.shape[0]
    chips = members // 2
    features = dw_ref.shape[0]
    queries = chips * rows
    me = lax.axis_index("patch")
    dp = lax.axis_index("dp")
    chip, core = me // 2, me % 2
    cx, cz = dp // ZS, dp % ZS
    partner = chip * 2 + 1 - core

    loads = [
        pltpu.make_async_copy(src, dst, load_sem.at[i])
        for i, (src, dst) in enumerate(
            [(seg_ref, seg_row), (k_ref, k_in), (q_ref, q_in), (v_ref, v_in), (w_hbm, w_ref), (t_hbm, t_ref)]
        )
    ]
    for load in loads:
        load.start()

    barrier = pltpu.get_barrier_semaphore()
    for shift in range(1, members):
        pl.semaphore_signal(barrier, inc=1, device_id=(dp, lax.rem(me + shift, members)), device_id_type=MESH)
    for shift in range(1, groups):
        pl.semaphore_signal(barrier, inc=1, device_id=(lax.rem(dp + shift, groups), me), device_id_type=MESH)
    for load in loads[:4]:
        load.wait()
    seg_all[0] = seg_row[...]
    pl.semaphore_wait(barrier, members + groups - 2)

    count = [0]
    pending = []

    def copy(src, dst, recv, device, send=None):
        if send is None:
            send = send_sem.at[count[0]]
            count[0] += 1
        return pltpu.make_async_remote_copy(
            src_ref=src, dst_ref=dst, send_sem=send, recv_sem=recv, device_id=device, device_id_type=MESH
        )

    def start(item):
        item.start()
        pending.append(item)

    def arrived(slot, recv):
        copy(slot, slot, recv, (dp, partner), send=send_sem.at[0]).wait_recv()

    def far(shift):
        return lax.rem(chip + shift, chips)

    def same(shift):
        return (dp, far(shift) * 2 + core)

    def cross(shift):
        return (dp, far(shift) * 2 + 1 - core)

    shifts = list(range(1, chips))
    for s in shifts:
        start(copy(seg_row, seg_all.at[chips - s], seg_recv.at[chips - s], same(s)))
    for s in range(chips):
        slot = chips + (chips - s) % chips
        start(copy(seg_row, seg_all.at[slot], seg_recv.at[slot], cross(s)))
    order = [4, 3, 5, 2, 6, 1, 7]
    start(copy(k_in.at[chip], k_slab.at[chips], k_recv.at[chips], cross(0)))
    start(copy(v_in.at[chip], v_slab.at[chips], v_recv.at[chips], cross(0)))
    for source, slab, recv in ((k_in, k_slab, k_recv), (q_in, q_slab, q_recv), (v_in, v_slab, v_recv)):
        for s in order:
            start(copy(source.at[far(s)], slab.at[chips - s], recv.at[chips - s], same(s)))

    length = len_ref[0]
    lane = lax.broadcasted_iota(jnp.int32, (1, rows), 1)
    sublane = lax.broadcasted_iota(jnp.int32, (16, rows), 0)

    def is_group(slot):
        owner = far(slot % chips) * 2 + (core if slot < chips else 1 - core)
        group = jnp.where(owner * rows + lane < length, seg_all[slot], -1) + 1
        return jnp.broadcast_to(group, (16, rows)) == sublane

    zeros40 = jnp.zeros((40, rows), F32)
    zeros48 = jnp.zeros((48, rows), F32)
    zeros8 = jnp.zeros((8, rows), F32)
    ones8 = jnp.ones((8, rows), F32)

    def columns(slot):
        return slice(slot * rows, (slot + 1) * rows)

    def take_key(slot, value):
        code = jnp.where(is_group(slot), 1.0, 0.0)
        full = jnp.concatenate([value.astype(F32), code, zeros40], axis=0)
        k_fm[:, columns(slot)] = full[:FM].astype(BF16)
        k_tm[columns(slot), :] = full.T.astype(BF16)

    def take_value(slot, value):
        full = jnp.concatenate([value.astype(F32), ones8, zeros48], axis=0)
        v_fm[:, columns(slot)] = full[:FM].astype(BF16)
        v_tm[columns(slot), :] = full.T.astype(BF16)

    def take_query(slot, value):
        code = jnp.where(is_group(slot), 0.0, NEG_LARGE)
        q_fm[:, columns(slot)] = jnp.concatenate([value.astype(F32), code, zeros40], axis=0).astype(BF16)

    for slot in range(1, members):
        arrived(seg_all.at[slot], seg_recv.at[slot])

    take_key(0, k_in[chip])
    for s in order:
        slot = chips - s
        arrived(k_slab.at[slot], k_recv.at[slot])
        start(copy(k_slab.at[slot], k_slab.at[chips + slot], k_recv.at[chips + slot], cross(0)))
        take_key(slot, k_slab[slot])
    for s in [0] + order:
        slot = chips + (chips - s) % chips
        arrived(k_slab.at[slot], k_recv.at[slot])
        take_key(slot, k_slab[slot])
    take_query(0, q_in[chip])
    for s in order:
        slot = chips - s
        arrived(q_slab.at[slot], q_recv.at[slot])
        take_query(slot, q_slab[slot])

    log_scale = math.log2(math.e) / math.sqrt(HEAD_DIM)
    score_scale = 1.0 / math.sqrt(HEAD_DIM)
    total = rows * members
    tiles = queries // TILE
    per_tile = TILE // rows
    chunks = [slice(low, low + CHUNK) for low in range(0, total, CHUNK)]

    def score_tile(t):
        span = slice(t * TILE, (t + 1) * TILE)
        tile = q_fm[:, span]
        top = None
        for chunk in chunks:
            scores = nn(k_tm[chunk, :], tile)
            s_ref[t % 2, chunk, :] = scores
            peak = jnp.max(scores, axis=0, keepdims=True)
            top = peak if top is None else jnp.maximum(top, peak)
        top = top * log_scale
        for chunk in chunks:
            p_ref[chunk, span] = jnp.exp2(s_ref[t % 2, chunk, :] * log_scale - top).astype(BF16)

    tile_order = list(range(1, tiles)) + [0]
    for t in tile_order[:2]:
        score_tile(t)
    take_value(0, v_in[chip])
    for s in order:
        slot = chips - s
        arrived(v_slab.at[slot], v_recv.at[slot])
        start(copy(v_slab.at[slot], v_slab.at[chips + slot], v_recv.at[chips + slot], cross(0)))
        take_value(slot, v_slab[slot])
    for t in tile_order[2:]:
        score_tile(t)
    for s in [0] + order:
        slot = chips + (chips - s) % chips
        arrived(v_slab.at[slot], v_recv.at[slot])
        take_value(slot, v_slab[slot])

    inverse = [None] * chips
    for t in tile_order:
        accum = nn(v_fm[...], p_ref[:, t * TILE : (t + 1) * TILE])
        for i in range(per_tile):
            slot = t * per_tile + i
            denom = accum[HEAD_DIM : HEAD_DIM + 1, i * rows : (i + 1) * rows]
            inverse[slot] = 1.0 / denom
            attn = (accum[:HEAD_DIM, i * rows : (i + 1) * rows] / denom).astype(BF16)
            att_out[slot] = attn
            if slot:
                start(copy(att_out.at[slot], attn_all.at[chip], attn_recv.at[chips - slot], same(slot)))
            else:
                attn_all[chip] = attn
    for slot in range(chips):
        scaled = q_fm[:HEAD_DIM, columns(slot)].astype(F32) * (inverse[slot] * score_scale)
        qs_fm[:, columns(slot)] = jnp.concatenate([scaled, zeros8], axis=0).astype(BF16)

    loads[4].wait()
    loads[5].wait()
    for s in order:
        arrived(attn_all.at[far(s)], attn_recv.at[s])
    stacked = [attn_all[h].astype(F32) for h in range(HEADS)] + [jnp.zeros((FEAT_PAD - FEAT, rows), F32)]
    attn_tm[...] = jnp.concatenate(stacked, axis=0).T.astype(BF16)
    own_live = me * rows + lax.broadcasted_iota(jnp.int32, (rows, 1), 0) < length
    output = nn(attn_tm[:, :FEAT], w_ref[...])
    error = jnp.where(own_live, output - t_ref[...].astype(F32), 0.0)
    dout_ref[...] = (2.0 * error).astype(BF16)
    grad = nt(w_ref[...], dout_ref[...])
    for h in range(HEADS):
        g_out[h] = grad[HEAD_DIM * h : HEAD_DIM * (h + 1)].astype(BF16)
    for s in order:
        start(copy(g_out.at[far(s)], g_slab.at[chips - s], g_recv.at[chips - s], same(s)))

    loss_part = jnp.sum(jnp.sum(error * error, axis=0, keepdims=True), axis=1, keepdims=True)
    tile_own[...] = jnp.broadcast_to(loss_part, tile_own.shape)
    for shift in range(1, members):
        peer = lax.rem(me + shift, members)
        start(copy(tile_own, tile_all.at[members - shift], tile_recv.at[members - shift], (dp, peer)))
    tile_all[0] = tile_own[...]

    share = WIDTH // groups
    part = tn(dout_ref[...], attn_tm[...])
    for block in range(groups):
        x, z = block // ZS, block % ZS
        part_ref[z % 2, x, z // 2] = part[block * share : (block + 1) * share].astype(BF16)
    start(copy(part_ref.at[1 - core], w1_ref, r1, (dp, partner)))

    arrived(w1_ref, r1)
    for x in range(XS):
        for z in range(ZH):
            sum1_ref[x, z] = (part_ref[core, x, z].astype(F32) + w1_ref[x, z].astype(F32)).astype(BF16)
    for d in range(1, XS):
        x = lax.rem(cx + d, XS)
        start(copy(sum1_ref.at[x], w2_ref.at[XS - d - 1], r2.at[XS - d - 1], (x * ZS + cz, me)))
    for z in range(ZH):
        keep_ref[z] = part_ref[core, cx, z].astype(F32) + w1_ref[cx, z].astype(F32)

    def take_grad(slot, value):
        wide = value.astype(F32)
        delta = -jnp.sum(wide * att_out[slot].astype(F32), axis=0, keepdims=True)
        high = delta.astype(BF16).astype(F32)
        middle = (delta - high).astype(BF16).astype(F32)
        low = delta - high - middle
        index = lax.broadcasted_iota(jnp.int32, (8, rows), 0)
        extra = jnp.where(index == 0, high, jnp.where(index == 1, middle, jnp.where(index == 2, low, 0.0)))
        g_fm[:, columns(slot)] = jnp.concatenate([wide, extra, zeros48], axis=0).astype(BF16)
        gs_fm[:, columns(slot)] = jnp.concatenate([wide * inverse[slot], zeros8], axis=0).astype(BF16)

    take_grad(0, g_out[chip])
    for s in order:
        slot = chips - s
        arrived(g_slab.at[slot], g_recv.at[slot])
        take_grad(slot, g_slab[slot])

    def key_side(left, right_ref, mine, out_ref, in_ref, recv):
        for i in list(range(chips, members, 2)) + list(range(0, chips, 2)):
            result = nt(left, right_ref[i * rows : (i + 2) * rows, :])
            target, base = (out_ref, i - chips) if i >= chips else (mine, i)
            for j in range(2):
                target[base + j] = result[:HEAD_DIM, j * rows : (j + 1) * rows]
            if i >= chips:
                pair = pl.ds(base, 2)
                start(copy(out_ref.at[pair], in_ref.at[pair], recv.at[base // 2], (dp, partner)))

    def send_home(slot, out, ref, recv):
        if slot:
            start(copy(out.at[slot], ref.at[chip], recv.at[chips - slot], same(slot)))
        else:
            item = pltpu.make_async_copy(out.at[0], ref.at[chip], send_sem.at[count[0]])
            count[0] += 1
            item.start()
            local.append(item)

    local = []

    def key_home(mine, in_ref, recv, out, ref, home):
        for base in (2, 4, 6, 0):
            pair = in_ref.at[pl.ds(base, 2)]
            arrived(pair, recv.at[base // 2])
            for slot in (base, base + 1):
                out[slot] = (mine[slot] + in_ref[slot]).astype(BF16)
                send_home(slot, out, ref, home)

    key_side(gs_fm[...], p_ref, v_own, xv_out, xv_in, xv_recv)
    key_home(v_own, xv_in, xv_recv, ov, dv_ref, dv_recv)

    for t in tile_order:
        span = slice(t * TILE, (t + 1) * TILE)
        tile = g_fm[:, span]
        for chunk in chunks:
            dprobs = nn(v_tm[chunk, :], tile)
            ds_ref[chunk, span] = (p_ref[chunk, span].astype(F32) * dprobs).astype(BF16)
        dq = nn(k_fm[...], ds_ref[:, span])
        for i in range(per_tile):
            slot = t * per_tile + i
            oq[slot] = (dq[:HEAD_DIM, i * rows : (i + 1) * rows] * (inverse[slot] * score_scale)).astype(BF16)
            send_home(slot, oq, dq_ref, dq_recv)

    key_side(qs_fm[...], ds_ref, k_own, xk_out, xk_in, xk_recv)
    key_home(k_own, xk_in, xk_recv, ok, dk_ref, dk_recv)

    for slot in range(1, members):
        arrived(tile_all.at[slot], tile_recv.at[slot])
    pack_loss = tile_all[0]
    for slot in range(1, members):
        pack_loss = pack_loss + tile_all[slot]
    sum_own[...] = jnp.where(lane == 0, pack_loss, length.astype(F32))
    for shift in range(1, groups):
        peer = lax.rem(dp + shift, groups)
        start(copy(sum_own, sum_all.at[groups - shift], sum_recv.at[groups - shift], (peer, me)))
    sum_all[0] = sum_own[...]

    for d in range(1, XS):
        arrived(w2_ref.at[d - 1], r2.at[d - 1])
    for z in range(ZH):
        summed = keep_ref[z]
        for d in range(XS - 1):
            summed = summed + w2_ref[d, z].astype(F32)
        wz_ref[z] = summed.astype(BF16)
    stage3 = []
    for z in range(ZH):
        target = 2 * z + core
        item = copy(wz_ref.at[z], w3_ref.at[cz], r3.at[cz], (cx * ZS + target, me))
        stage3.append((target, item))

        @pl.when(target != cz)
        def _():
            item.start()

    is_collector = core == cz % 2
    stage4 = []
    for shift in range(1, members):
        target = lax.rem(me + shift, members)
        span = fin_ref.at[:, pl.ds(span_start(target, features), SPAN)]
        stage4.append(copy(span, w4_ref.at[chip], r4.at[chip], (dp, target)))

    @pl.when(is_collector)
    def _():
        summed = wz_ref[cz // 2].astype(F32)
        for shift in range(1, ZS):
            source = lax.rem(cz + shift, ZS)
            arrived(w3_ref.at[source], r3.at[source])
            summed = summed + w3_ref[source].astype(F32)
        fin_ref[...] = summed.astype(BF16)
        for item in stage4:
            item.start()
        w4_ref[chip] = fin_ref[:, pl.ds(span_start(me, features), SPAN)]

    for shift in range(1, groups):
        arrived(sum_all.at[shift], sum_recv.at[shift])
    totals = sum_all[0]
    for shift in range(1, groups):
        totals = totals + sum_all[shift]
    sum_ref[...] = totals

    for s in order:
        for ref, recv in ((dv_ref, dv_recv), (dq_ref, dq_recv), (dk_ref, dk_recv)):
            arrived(ref.at[far(s)], recv.at[s])

    @pl.when(jnp.logical_not(is_collector))
    def _():
        arrived(w4_ref.at[chip], r4.at[chip])

    for s in shifts:
        arrived(w4_ref.at[far(s)], r4.at[far(s)])
    shape = (features, SPAN)
    start_lane = me * features - span_start(me, features)
    chosen = (
        lax.broadcasted_iota(jnp.int32, shape, 1) == start_lane + lax.broadcasted_iota(jnp.int32, shape, 0)
    ).astype(F32).astype(BF16)
    result = nt(chosen, w4_ref[0])
    for j in range(1, chips):
        result = result + nt(chosen, w4_ref[j])
    dw_ref[...] = result

    for item in local:
        item.wait()
    for item in pending:
        item.wait_send()
    for target, item in stage3:

        @pl.when(target != cz)
        def _():
            item.wait_send()

    @pl.when(is_collector)
    def _():
        for item in stage4:
            item.wait_send()


def scale_kernel(slots, total, sum_ref, dq_ref, dk_ref, dv_ref, dw_ref, query_ref, key_ref, value_ref, weight_ref, loss_ref):
    count = sum_ref[0:1, 1:2]
    ratio = slots / count
    for source, target in ((dq_ref, query_ref), (dk_ref, key_ref), (dv_ref, value_ref)):
        for h in range(HEADS):
            target[HEAD_DIM * h : HEAD_DIM * (h + 1), :] = source[h].astype(F32) * ratio
    weight_ref[...] = dw_ref[...] * (ratio / total)
    loss_ref[...] = sum_ref[0:1, 0:1] / (count * WIDTH)


def solution(mesh):
    members, groups = mesh.shape["patch"], mesh.shape["dp"]

    def local(query_rows, key_rows, value_rows, out_weight, target, lengths, segments):
        rows = query_rows.shape[1]
        total = rows * members
        chips = members // 2
        queries = rows * chips
        share = WIDTH // groups
        vmem = pl.BlockSpec(memory_space=pltpu.VMEM)
        hbm = pl.BlockSpec(memory_space=pltpu.HBM)
        dma = pltpu.SemaphoreType.DMA
        slab = (HEAD_DIM, rows)

        def heads(value):
            return value[0].T.reshape(HEADS, HEAD_DIM, rows)

        def bf(*shape):
            return pltpu.VMEM(shape, BF16)

        def fl(*shape):
            return pltpu.VMEM(shape, F32)

        outs = pl.pallas_call(
            functools.partial(kernel, members, groups),
            out_shape=(
                jax.ShapeDtypeStruct((HEADS, HEAD_DIM, rows), BF16),
                jax.ShapeDtypeStruct((HEADS, HEAD_DIM, rows), BF16),
                jax.ShapeDtypeStruct((HEADS, HEAD_DIM, rows), BF16),
                jax.ShapeDtypeStruct((FEAT // members, share), F32),
                jax.ShapeDtypeStruct((1, LANES), F32),
            ),
            in_specs=[pl.BlockSpec(memory_space=pltpu.SMEM)] + [hbm] * 6,
            out_specs=(hbm, hbm, hbm, vmem, vmem),
            scratch_shapes=[
                bf(HEADS, *slab),
                bf(HEADS, *slab),
                bf(HEADS, *slab),
                bf(FEAT, WIDTH),
                bf(rows, WIDTH),
                pltpu.VMEM((1, rows), jnp.int32),
                pltpu.VMEM((members, 1, rows), jnp.int32),
                bf(chips, *slab),
                bf(members, *slab),
                bf(members, *slab),
                bf(total, LANES),
                bf(total, LANES),
                bf(FM, total),
                bf(FM, total),
                bf(LANES, queries),
                bf(LANES, queries),
                bf(FM, queries),
                bf(FM, queries),
                fl(2, total, TILE),
                bf(total, queries),
                bf(total, queries),
                bf(chips, *slab),
                bf(HEADS, *slab),
                bf(rows, FEAT_PAD),
                bf(rows, WIDTH),
                bf(HEADS, *slab),
                bf(chips, *slab),
                fl(chips, *slab),
                fl(chips, *slab),
                fl(chips, *slab),
                fl(chips, *slab),
                fl(chips, *slab),
                fl(chips, *slab),
                bf(chips, *slab),
                bf(chips, *slab),
                bf(chips, *slab),
                bf(2, XS, ZH, share, FEAT_PAD),
                bf(XS, ZH, share, FEAT_PAD),
                bf(XS, ZH, share, FEAT_PAD),
                fl(ZH, share, FEAT_PAD),
                bf(XS - 1, ZH, share, FEAT_PAD),
                bf(ZH, share, FEAT_PAD),
                bf(ZS, share, FEAT_PAD),
                bf(share, FEAT_PAD),
                bf(chips, share, SPAN),
                fl(1, LANES),
                fl(members, 1, LANES),
                fl(1, LANES),
                fl(groups, 1, LANES),
                dma((6,)),
                dma((200,)),
                dma((members,)),
                dma((chips,)),
                dma((members,)),
                dma((members,)),
                dma((chips,)),
                dma((chips,)),
                dma((chips // 2,)),
                dma((chips // 2,)),
                dma((chips,)),
                dma((chips,)),
                dma((chips,)),
                dma((members,)),
                dma((groups,)),
                dma,
                dma((XS - 1,)),
                dma((ZS,)),
                dma((chips,)),
            ],
            compiler_params=pltpu.CompilerParams(collective_id=0, has_side_effects=True, vmem_limit_bytes=65900000),
            name="sublayer",
        )(
            lengths,
            segments,
            heads(query_rows),
            heads(key_rows),
            heads(value_rows),
            out_weight,
            target[0],
        )
        final = pl.pallas_call(
            functools.partial(scale_kernel, groups * total, total),
            out_shape=(
                jax.ShapeDtypeStruct((FEAT, rows), F32),
                jax.ShapeDtypeStruct((FEAT, rows), F32),
                jax.ShapeDtypeStruct((FEAT, rows), F32),
                jax.ShapeDtypeStruct((FEAT // members, share), F32),
                jax.ShapeDtypeStruct((1, 1), F32),
            ),
            in_specs=[vmem] * 5,
            out_specs=(vmem,) * 5,
            compiler_params=pltpu.CompilerParams(vmem_limit_bytes=65900000),
            name="scale",
        )(outs[4], *outs[:4])
        return (final[0].T[None], final[1].T[None], final[2].T[None], final[3], final[4].reshape(()))

    placed = (
        P("dp", "patch", None),
        P("dp", "patch", None),
        P("dp", "patch", None),
        P(),
        P("dp", "patch", None),
        P("dp"),
        P("dp", "patch"),
    )
    return jax.shard_map(
        local,
        mesh=mesh,
        in_specs=placed,
        out_specs=(
            P("dp", "patch", None),
            P("dp", "patch", None),
            P("dp", "patch", None),
            P("patch", "dp"),
            P(),
        ),
        check_vma=False,
    )
```

```python
import functools
import math

import jax
import jax.numpy as jnp
from jax import lax
from jax.experimental import pallas as pl
from jax.experimental.pallas import tpu as pltpu
from jax.sharding import PartitionSpec as P

MESH = pl.DeviceIdType.MESH
WIDTH = 1152
HEADS = 8
HEAD_DIM = 72
FEAT = 576
FEAT_PAD = 640
FM = 80
LANES = 128
SPAN = 256
TILE = 256
CHUNK = 512
NEG_LARGE = -1e30
F32 = jnp.float32
BF16 = jnp.bfloat16
XS, ZS = 4, 8
ZH = ZS // 2
X_LANES = 384
Z_LANES = 256
PAIRS = ((4, 0), (3, 5), (2, 6), (1, 7))


def nt(left, right):
    return lax.dot_general(left, right, (((1,), (1,)), ((), ())), preferred_element_type=F32)


def nn(left, right):
    return lax.dot_general(left, right, (((1,), (0,)), ((), ())), preferred_element_type=F32)


def tn(left, right):
    return lax.dot_general(left, right, (((0,), (0,)), ((), ())), preferred_element_type=F32)


def kernel(
    members,
    groups,
    len_ref,
    seg_ref,
    q_ref,
    k_ref,
    v_ref,
    w_hbm,
    t_hbm,
    dq_ref,
    dk_ref,
    dv_ref,
    dw_ref,
    sum_ref,
    q_in,
    k_in,
    v_in,
    w_ref,
    t_ref,
    seg_row,
    seg_all,
    q_slab,
    k_slab,
    v_slab,
    k_tm,
    v_tm,
    k_fm,
    v_fm,
    q_fm,
    g_fm,
    qs_fm,
    gs_fm,
    s_ref,
    p_ref,
    ds_ref,
    att_out,
    attn_all,
    attn_tm,
    attn_in,
    dt_ref,
    dt_in,
    g_out,
    g_slab,
    xv_out,
    xv_in,
    xk_out,
    xk_in,
    v_own,
    k_own,
    oq,
    ok,
    ov,
    xa_ref,
    xa_in,
    za_ref,
    za_in,
    zb_ref,
    zb_in,
    xb_ref,
    xb_in,
    piece_ref,
    yb_ref,
    tile_own,
    tile_all,
    sum_own,
    sum_all,
    load_sem,
    send_sem,
    recv_sem,
    k_recv,
    v_recv,
    q_recv,
    g_recv,
):
    rows = t_ref.shape[0]
    chips = members // 2
    features, share = dw_ref.shape
    me = lax.axis_index("patch")
    dp = lax.axis_index("dp")
    chip, core = me // 2, me % 2
    cx, cz = dp // ZS, dp % ZS
    partner = chip * 2 + 1 - core

    loads = [
        pltpu.make_async_copy(src, dst, load_sem.at[i])
        for i, (src, dst) in enumerate(
            [(seg_ref, seg_row), (k_ref, k_in), (v_ref, v_in), (q_ref, q_in), (w_hbm, w_ref), (t_hbm, t_ref)]
        )
    ]
    for load in loads:
        load.start()

    barrier = pltpu.get_barrier_semaphore()
    for shift in range(1, members):
        pl.semaphore_signal(barrier, inc=1, device_id=(dp, lax.rem(me + shift, members)), device_id_type=MESH)
    for shift in range(1, groups):
        pl.semaphore_signal(barrier, inc=1, device_id=(lax.rem(dp + shift, groups), me), device_id_type=MESH)
    for load in loads[:4]:
        load.wait()
    seg_all[0] = seg_row[...]
    pl.semaphore_wait(barrier, members + groups - 2)

    def copy(src, dst, send, recv, device):
        return pltpu.make_async_remote_copy(
            src_ref=src, dst_ref=dst, send_sem=send, recv_sem=recv, device_id=device, device_id_type=MESH
        )

    def arrived(ref, recv):
        copy(ref, ref, send_sem.at[0], recv, (dp, partner)).wait_recv()

    def sent(ref, send):
        copy(ref, ref, send, recv_sem.at[0], (dp, partner)).wait_send()

    def some(ref, n):
        return ref.at[pl.ds(0, n)]

    SEG, ATTN, XV, XK, DQ, DK, DV, TILE_SUM, ALL_SUM, DT, AT, XA, ZA, ZB, XB, Y, K, V, Q, G = range(20)
    twin = (dp, partner)

    def far(shift):
        return lax.rem(chip + shift, chips)

    def same(shift):
        return (dp, far(shift) * 2 + core)

    def cross(shift):
        return (dp, far(shift) * 2 + 1 - core)

    group_of = {slot: i for i, pair in enumerate(PAIRS) for slot in pair}
    order = [slot for pair in PAIRS for slot in pair if slot]
    position = {slot: i for i, slot in enumerate(slot for pair in PAIRS for slot in pair)}

    for s in order:
        copy(seg_row, seg_all.at[chips - s], send_sem.at[SEG], recv_sem.at[SEG], same(s)).start()
    for s in order + [0]:
        slot = chips + (chips - s) % chips
        copy(seg_row, seg_all.at[slot], send_sem.at[SEG], recv_sem.at[SEG], cross(s)).start()
    for number, source, slab, recv in ((K, k_in, k_slab, k_recv), (V, v_in, v_slab, v_recv)):
        copy(source.at[chip], slab.at[chips], send_sem.at[number], recv.at[len(PAIRS)], twin).start()
    for number, source, slab, recv in ((K, k_in, k_slab, k_recv), (V, v_in, v_slab, v_recv), (Q, q_in, q_slab, q_recv)):
        for s in order:
            slot = chips - s
            copy(source.at[far(s)], slab.at[slot], send_sem.at[number], recv.at[group_of[slot]], same(s)).start()

    length = len_ref[0]
    lane = lax.broadcasted_iota(jnp.int32, (1, rows), 1)
    sublane = lax.broadcasted_iota(jnp.int32, (16, rows), 0)

    def is_group(slot):
        owner = far(slot % chips) * 2 + (core if slot < chips else 1 - core)
        group = jnp.where(owner * rows + lane < length, seg_all[slot], -1) + 1
        return jnp.broadcast_to(group, (16, rows)) == sublane

    zeros40 = jnp.zeros((40, rows), F32)
    zeros48 = jnp.zeros((48, rows), F32)
    zeros8 = jnp.zeros((8, rows), F32)
    ones8 = jnp.ones((8, rows), F32)

    def columns(slot):
        return slice(slot * rows, (slot + 1) * rows)

    def query_columns(slot):
        return columns(position[slot])

    def take_key(slot, value):
        code = jnp.where(is_group(slot), 1.0, 0.0)
        full = jnp.concatenate([value.astype(F32), code, zeros40], axis=0)
        k_fm[:, columns(slot)] = full[:FM].astype(BF16)
        k_tm[columns(slot), :] = full.T.astype(BF16)

    def take_value(slot, value):
        full = jnp.concatenate([value.astype(F32), ones8, zeros48], axis=0)
        v_fm[:, columns(slot)] = full[:FM].astype(BF16)
        v_tm[columns(slot), :] = full.T.astype(BF16)

    def take_query(slot, value):
        code = jnp.where(is_group(slot), 0.0, NEG_LARGE)
        q_fm[:, query_columns(slot)] = jnp.concatenate([value.astype(F32), code, zeros40], axis=0).astype(BF16)

    arrived(some(seg_all, members - 1), recv_sem.at[SEG])

    def gather(number, own, slab, recv, take):
        take(0, own[chip])
        for i, pair in enumerate(PAIRS):
            pair = [slot for slot in pair if slot]
            arrived(some(slab, len(pair)), recv.at[i])
            for slot in pair:
                relay = recv.at[len(PAIRS) + i]
                copy(slab.at[slot], slab.at[chips + slot], send_sem.at[number], relay, twin).start()
            for slot in pair:
                take(slot, slab[slot])

    def gather_twin(slab, recv, take):
        for i, pair in enumerate(PAIRS):
            arrived(some(slab, 2), recv.at[len(PAIRS) + i])
            for slot in pair:
                take(chips + slot, slab[chips + slot])

    gather(K, k_in, k_slab, k_recv, take_key)
    gather_twin(k_slab, k_recv, take_key)
    gather(V, v_in, v_slab, v_recv, take_value)
    gather_twin(v_slab, v_recv, take_value)

    log_scale = math.log2(math.e) / math.sqrt(HEAD_DIM)
    score_scale = 1.0 / math.sqrt(HEAD_DIM)
    total = rows * members
    chunks = [slice(low, low + CHUNK) for low in range(0, total, CHUNK)]

    inverse = {}
    for i, pair in enumerate(PAIRS):
        remote = [slot for slot in pair if slot]
        arrived(some(q_slab, len(remote)), q_recv.at[i])
        for slot in pair:
            take_query(slot, q_slab[slot] if slot else q_in[chip])
        span = slice(i * TILE, (i + 1) * TILE)
        tile = q_fm[:, span]
        top = None
        for chunk in chunks:
            scores = nn(k_tm[chunk, :], tile)
            s_ref[i % 2, chunk, :] = scores
            peak = jnp.max(scores, axis=0, keepdims=True)
            top = peak if top is None else jnp.maximum(top, peak)
        top = top * log_scale
        for chunk in chunks:
            p_ref[chunk, span] = jnp.exp2(s_ref[i % 2, chunk, :] * log_scale - top).astype(BF16)
        accum = nn(v_fm[...], p_ref[:, span])
        for j, slot in enumerate(pair):
            denom = accum[HEAD_DIM : HEAD_DIM + 1, columns(j)]
            inverse[slot] = 1.0 / denom
            attn = (accum[:HEAD_DIM, columns(j)] / denom).astype(BF16)
            att_out[slot] = attn
            if slot:
                copy(att_out.at[slot], attn_all.at[chip], send_sem.at[ATTN], recv_sem.at[ATTN], same(slot)).start()
            else:
                attn_all[chip] = attn
    for slot in range(chips):
        scaled = q_fm[:HEAD_DIM, query_columns(slot)].astype(F32) * (inverse[slot] * score_scale)
        qs_fm[:, query_columns(slot)] = jnp.concatenate([scaled, zeros8], axis=0).astype(BF16)

    loads[4].wait()
    loads[5].wait()
    arrived(some(attn_all, chips - 1), recv_sem.at[ATTN])
    stacked = [attn_all[h].astype(F32) for h in range(HEADS)] + [jnp.zeros((FEAT_PAD - FEAT, rows), F32)]
    attn_tm[...] = jnp.concatenate(stacked, axis=0).T.astype(BF16)
    copy(attn_tm, attn_in, send_sem.at[AT], recv_sem.at[AT], twin).start()
    own_live = me * rows + lax.broadcasted_iota(jnp.int32, (rows, 1), 0) < length
    output = nn(attn_tm[:, :FEAT], w_ref[...])
    error = jnp.where(own_live, output - t_ref[...].astype(F32), 0.0)
    dout_t = (2.0 * error).T
    dout_t = dout_t.astype(BF16)
    dt_ref[...] = dout_t.reshape(dt_ref.shape)
    grad = nn(w_ref[...], dout_t)
    for h in range(HEADS):
        g_out[h] = grad[HEAD_DIM * h : HEAD_DIM * (h + 1)].astype(BF16)
    for s in order:
        slot = chips - s
        copy(g_out.at[far(s)], g_slab.at[slot], send_sem.at[G], g_recv.at[group_of[slot]], same(s)).start()

    for x in range(XS):
        copy(dt_ref.at[2 * x + 1 - core], dt_in.at[x], send_sem.at[DT], recv_sem.at[DT], twin).start()
    loss_part = jnp.sum(jnp.sum(error * error, axis=0, keepdims=True), axis=1, keepdims=True)
    tile_own[...] = jnp.broadcast_to(loss_part, tile_own.shape)
    for shift in range(1, members):
        peer = (dp, lax.rem(me + shift, members))
        copy(tile_own, tile_all.at[members - shift], send_sem.at[TILE_SUM], recv_sem.at[TILE_SUM], peer).start()
    tile_all[0] = tile_own[...]
    arrived(attn_in, recv_sem.at[AT])
    arrived(dt_in, recv_sem.at[DT])
    tall = ZH * share
    left = jnp.concatenate(
        [jnp.concatenate([dt_ref[2 * x + core], dt_in[x]], axis=1) for x in range(XS)], axis=0
    )
    right = jnp.concatenate([attn_tm[...], attn_in[...]], axis=0)
    xa_ref[...] = nn(left, right[:, :X_LANES]).astype(BF16).reshape(XS, tall, X_LANES)
    for d in range(1, XS):
        x = lax.rem(cx + d, XS)
        item = copy(xa_ref.at[x], xa_in.at[XS - d - 1], send_sem.at[XA], recv_sem.at[XA], (x * ZS + cz, me))
        item.start()
    part = nn(left, right[:, X_LANES:])
    for x in range(XS):
        for j in range(ZH):
            low = x * tall + j * share
            za_ref[j, x] = part[low : low + share].astype(BF16)

    def along_z(source, landing, number):
        for j in range(ZH):
            target = ZH * core + j

            @pl.when(target != cz)
            def _():
                slot = lax.rem(cz - target + 2 * ZS - 1, ZS)
                device = (cx * ZS + target, me)
                copy(source.at[j], landing.at[slot], send_sem.at[number], recv_sem.at[number], device).start()

    along_z(za_ref, za_in, ZA)
    near = core == cz // ZH
    away = core != cz // ZH
    mine = lax.rem(cz, ZH)

    def take_grad(slot, value):
        wide = value.astype(F32)
        delta = -jnp.sum(wide * att_out[slot].astype(F32), axis=0, keepdims=True)
        high = delta.astype(BF16).astype(F32)
        middle = (delta - high).astype(BF16).astype(F32)
        low = delta - high - middle
        index = lax.broadcasted_iota(jnp.int32, (8, rows), 0)
        extra = jnp.where(index == 0, high, jnp.where(index == 1, middle, jnp.where(index == 2, low, 0.0)))
        g_fm[:, query_columns(slot)] = jnp.concatenate([wide, extra, zeros48], axis=0).astype(BF16)
        gs_fm[:, query_columns(slot)] = jnp.concatenate([wide * inverse[slot], zeros8], axis=0).astype(BF16)

    def send_home(slot, out, ref, number):
        if slot:
            copy(out.at[slot], ref.at[chip], send_sem.at[number], recv_sem.at[number], same(slot)).start()
        else:
            item = pltpu.make_async_copy(out.at[0], ref.at[chip], load_sem.at[len(local)])
            item.start()
            local.append(item)

    local = []
    for i, pair in enumerate(PAIRS):
        remote = [slot for slot in pair if slot]
        arrived(some(g_slab, len(remote)), g_recv.at[i])
        for slot in pair:
            take_grad(slot, g_slab[slot] if slot else g_out[chip])
        span = slice(i * TILE, (i + 1) * TILE)
        tile = g_fm[:, span]
        for chunk in chunks:
            dprobs = nn(v_tm[chunk, :], tile)
            ds_ref[chunk, span] = (p_ref[chunk, span].astype(F32) * dprobs).astype(BF16)
        dq = nn(k_fm[...], ds_ref[:, span])
        for j, slot in enumerate(pair):
            oq[slot] = (dq[:HEAD_DIM, columns(j)] * (inverse[slot] * score_scale)).astype(BF16)
            send_home(slot, oq, dq_ref, DQ)

    def key_side(left, right_ref, mine, out_ref, in_ref, number):
        for i in list(range(chips, members, 2)) + list(range(0, chips, 2)):
            result = nt(left, right_ref[i * rows : (i + 2) * rows, :])
            target, base = (out_ref, i - chips) if i >= chips else (mine, i)
            for j in range(2):
                target[base + j] = result[:HEAD_DIM, columns(j)]
            if i >= chips:
                pair = pl.ds(base, 2)
                copy(out_ref.at[pair], in_ref.at[pair], send_sem.at[number], recv_sem.at[number], twin).start()

    def key_home(mine, in_ref, number, out, ref, home):
        arrived(in_ref, recv_sem.at[number])
        for slot in order + [0]:
            out[slot] = (mine[slot] + in_ref[slot]).astype(BF16)
            send_home(slot, out, ref, home)

    arrived(some(tile_all, members - 1), recv_sem.at[TILE_SUM])
    pack_loss = tile_all[0]
    for slot in range(1, members):
        pack_loss = pack_loss + tile_all[slot]
    sum_own[...] = jnp.where(lane == 0, pack_loss, length.astype(F32))
    for shift in range(1, groups):
        peer = (lax.rem(dp + shift, groups), me)
        copy(sum_own, sum_all.at[groups - shift], send_sem.at[ALL_SUM], recv_sem.at[ALL_SUM], peer).start()
    sum_all[0] = sum_own[...]

    key_side(gs_fm[...], p_ref, v_own, xv_out, xv_in, XV)
    key_home(v_own, xv_in, XV, ov, dv_ref, DV)

    arrived(xa_in, recv_sem.at[XA])
    summed = xa_ref[cx].astype(F32)
    for i in range(XS - 1):
        summed = summed + xa_in[i].astype(F32)
    for j in range(ZH):
        zb_ref[j] = summed[j * share : (j + 1) * share].astype(BF16)
    along_z(zb_ref, zb_in, ZB)

    key_side(qs_fm[...], ds_ref, k_own, xk_out, xk_in, XK)
    key_home(k_own, xk_in, XK, ok, dk_ref, DK)

    @pl.when(near)
    def _():
        arrived(some(za_in, ZS - 1), recv_sem.at[ZA])
        for x in range(XS):
            summed = za_ref[mine, x].astype(F32)
            for i in range(ZS - 1):
                summed = summed + za_in[i, x].astype(F32)
            xb_ref[x] = summed.astype(BF16)
        for d in range(1, XS):
            x = lax.rem(cx + d, XS)
            item = copy(xb_ref.at[x], xb_in.at[XS - d - 1], send_sem.at[XB], recv_sem.at[XB], (x * ZS + cz, me))
            item.start()

    @pl.when(near)
    def _():
        arrived(some(zb_in, ZS - 1), recv_sem.at[ZB])
        summed = zb_ref[mine].astype(F32)
        for i in range(ZS - 1):
            summed = summed + zb_in[i].astype(F32)
        arrived(xb_in, recv_sem.at[XB])
        other = xb_ref[cx].astype(F32)
        for i in range(XS - 1):
            other = other + xb_in[i].astype(F32)
        whole = jnp.concatenate([summed, other], axis=1)
        turned = jnp.concatenate([whole, jnp.zeros((LANES - share, FEAT_PAD), F32)], axis=0).T
        for t in range(members):
            piece_ref[t] = turned[t * features : (t + 1) * features].astype(BF16)
        for shift in range(1, members):
            target = lax.rem(me + shift, members)
            copy(piece_ref.at[target], yb_ref.at[chip], send_sem.at[Y], recv_sem.at[Y], (dp, target)).start()
        yb_ref[chip] = piece_ref[me]

    arrived(some(sum_all, groups - 1), recv_sem.at[ALL_SUM])
    totals = sum_all[0]
    for slot in range(1, groups):
        totals = totals + sum_all[slot]
    sum_ref[...] = totals

    for ref, number in ((dv_ref, DV), (dq_ref, DQ), (dk_ref, DK)):
        arrived(some(ref, chips - 1), recv_sem.at[number])

    @pl.when(near)
    def _():
        arrived(some(yb_ref, chips - 1), recv_sem.at[Y])

    @pl.when(away)
    def _():
        arrived(yb_ref, recv_sem.at[Y])

    result = yb_ref[0].astype(F32)
    for j in range(1, chips):
        result = result + yb_ref[j].astype(F32)
    dw_ref[...] = result[:, :share]

    for item in local:
        item.wait()
    sent(some(seg_all, members - 1), send_sem.at[SEG])
    sent(some(k_slab, members - 1), send_sem.at[K])
    sent(some(v_slab, members - 1), send_sem.at[V])
    for ref, number in ((q_slab, Q), (attn_all, ATTN), (g_slab, G), (dq_ref, DQ), (dv_ref, DV), (dk_ref, DK)):
        sent(some(ref, chips - 1), send_sem.at[number])
    for ref, number in ((attn_tm, AT), (dt_in, DT), (xv_in, XV), (xk_in, XK)):
        sent(ref, send_sem.at[number])
    sent(some(tile_all, members - 1), send_sem.at[TILE_SUM])
    sent(some(sum_all, groups - 1), send_sem.at[ALL_SUM])

    sent(xa_in, send_sem.at[XA])

    @pl.when(near)
    def _():
        sent(some(za_ref, ZH - 1), send_sem.at[ZA])
        sent(some(zb_ref, ZH - 1), send_sem.at[ZB])
        sent(xb_in, send_sem.at[XB])
        sent(some(piece_ref, members - 1), send_sem.at[Y])

    @pl.when(away)
    def _():
        sent(za_ref, send_sem.at[ZA])
        sent(zb_ref, send_sem.at[ZB])


def scale_kernel(slots, total, sum_ref, dq_ref, dk_ref, dv_ref, dw_ref, query_ref, key_ref, value_ref, weight_ref, loss_ref):
    count = sum_ref[0:1, 1:2]
    ratio = slots / count
    for source, target in ((dq_ref, query_ref), (dk_ref, key_ref), (dv_ref, value_ref)):
        for h in range(HEADS):
            target[HEAD_DIM * h : HEAD_DIM * (h + 1), :] = source[h].astype(F32) * ratio
    weight_ref[...] = dw_ref[...] * (ratio / total)
    loss_ref[...] = sum_ref[0:1, 0:1] / (count * WIDTH)


def solution(mesh):
    members, groups = mesh.shape["patch"], mesh.shape["dp"]

    def local(query_rows, key_rows, value_rows, out_weight, target, lengths, segments):
        rows = query_rows.shape[1]
        total = rows * members
        chips = members // 2
        queries = rows * chips
        share = WIDTH // groups
        vmem = pl.BlockSpec(memory_space=pltpu.VMEM)
        hbm = pl.BlockSpec(memory_space=pltpu.HBM)
        dma = pltpu.SemaphoreType.DMA
        slab = (HEAD_DIM, rows)

        def heads(value):
            return value[0].T.reshape(HEADS, HEAD_DIM, rows)

        def bf(*shape):
            return pltpu.VMEM(shape, BF16)

        def fl(*shape):
            return pltpu.VMEM(shape, F32)

        outs = pl.pallas_call(
            functools.partial(kernel, members, groups),
            out_shape=(
                jax.ShapeDtypeStruct((HEADS, HEAD_DIM, rows), BF16),
                jax.ShapeDtypeStruct((HEADS, HEAD_DIM, rows), BF16),
                jax.ShapeDtypeStruct((HEADS, HEAD_DIM, rows), BF16),
                jax.ShapeDtypeStruct((FEAT // members, share), F32),
                jax.ShapeDtypeStruct((1, LANES), F32),
            ),
            in_specs=[pl.BlockSpec(memory_space=pltpu.SMEM)] + [hbm] * 6,
            out_specs=(hbm, hbm, hbm, vmem, vmem),
            scratch_shapes=[
                bf(HEADS, *slab),
                bf(HEADS, *slab),
                bf(HEADS, *slab),
                bf(FEAT, WIDTH),
                bf(rows, WIDTH),
                pltpu.VMEM((1, rows), jnp.int32),
                pltpu.VMEM((members, 1, rows), jnp.int32),
                bf(chips, *slab),
                bf(members, *slab),
                bf(members, *slab),
                bf(total, LANES),
                bf(total, LANES),
                bf(FM, total),
                bf(FM, total),
                bf(LANES, queries),
                bf(LANES, queries),
                bf(FM, queries),
                bf(FM, queries),
                fl(2, total, TILE),
                bf(total, queries),
                bf(total, queries),
                bf(chips, *slab),
                bf(HEADS, *slab),
                bf(rows, FEAT_PAD),
                bf(rows, FEAT_PAD),
                bf(2 * XS, ZH * share, rows),
                bf(XS, ZH * share, rows),
                bf(HEADS, *slab),
                bf(chips, *slab),
                fl(chips, *slab),
                fl(chips, *slab),
                fl(chips, *slab),
                fl(chips, *slab),
                fl(chips, *slab),
                fl(chips, *slab),
                bf(chips, *slab),
                bf(chips, *slab),
                bf(chips, *slab),
                bf(XS, ZH * share, X_LANES),
                bf(XS - 1, ZH * share, X_LANES),
                bf(ZH, XS, share, Z_LANES),
                bf(ZS, XS, share, Z_LANES),
                bf(ZH, share, X_LANES),
                bf(ZS, share, X_LANES),
                bf(XS, share, Z_LANES),
                bf(XS - 1, share, Z_LANES),
                bf(members, FEAT // members, LANES),
                bf(chips, FEAT // members, LANES),
                fl(1, LANES),
                fl(members, 1, LANES),
                fl(1, LANES),
                fl(groups, 1, LANES),
                dma((6,)),
                dma((20,)),
                dma((16,)),
                dma((2 * len(PAIRS),)),
                dma((2 * len(PAIRS),)),
                dma((len(PAIRS),)),
                dma((len(PAIRS),)),
            ],
            compiler_params=pltpu.CompilerParams(collective_id=0, has_side_effects=True, vmem_limit_bytes=65900000),
            name="sublayer",
        )(
            lengths,
            segments,
            heads(query_rows),
            heads(key_rows),
            heads(value_rows),
            out_weight,
            target[0],
        )
        final = pl.pallas_call(
            functools.partial(scale_kernel, groups * total, total),
            out_shape=(
                jax.ShapeDtypeStruct((FEAT, rows), F32),
                jax.ShapeDtypeStruct((FEAT, rows), F32),
                jax.ShapeDtypeStruct((FEAT, rows), F32),
                jax.ShapeDtypeStruct((FEAT // members, share), F32),
                jax.ShapeDtypeStruct((1, 1), F32),
            ),
            in_specs=[vmem] * 5,
            out_specs=(vmem,) * 5,
            compiler_params=pltpu.CompilerParams(vmem_limit_bytes=65900000),
            name="scale",
        )(outs[4], *outs[:4])
        return (final[0].T[None], final[1].T[None], final[2].T[None], final[3], final[4].reshape(()))

    placed = (
        P("dp", "patch", None),
        P("dp", "patch", None),
        P("dp", "patch", None),
        P(),
        P("dp", "patch", None),
        P("dp"),
        P("dp", "patch"),
    )
    return jax.shard_map(
        local,
        mesh=mesh,
        in_specs=placed,
        out_specs=(
            P("dp", "patch", None),
            P("dp", "patch", None),
            P("dp", "patch", None),
            P("patch", "dp"),
            P(),
        ),
        check_vma=False,
    )
```

```python
import functools
import math

import jax
import jax.numpy as jnp
from jax import lax
from jax.experimental import pallas as pl
from jax.experimental.pallas import tpu as pltpu
from jax.sharding import PartitionSpec as P

MESH = pl.DeviceIdType.MESH
WIDTH = 1152
HEADS = 8
HEAD_DIM = 72
FEAT = 576
FEAT_PAD = 640
FM = 80
LANES = 128
SPAN = 256
TILE = 256
CHUNK = 256
NEG_LARGE = -1e30
F32 = jnp.float32
BF16 = jnp.bfloat16
XS, ZS = 4, 8
ZH = ZS // 2
X_LANES = 384
Z_LANES = 256
PAIRS = ((4, 0), (3, 5), (2, 6), (1, 7))


def nt(left, right):
    return lax.dot_general(left, right, (((1,), (1,)), ((), ())), preferred_element_type=F32)


def nn(left, right):
    return lax.dot_general(left, right, (((1,), (0,)), ((), ())), preferred_element_type=F32)


def tn(left, right):
    return lax.dot_general(left, right, (((0,), (0,)), ((), ())), preferred_element_type=F32)


def kernel(
    members,
    groups,
    len_ref,
    seg_ref,
    q_ref,
    k_ref,
    v_ref,
    w_hbm,
    t_hbm,
    dq_ref,
    dk_ref,
    dv_ref,
    dw_ref,
    sum_ref,
    q_in,
    k_in,
    v_in,
    w_ref,
    t_ref,
    seg_row,
    seg_all,
    q_slab,
    k_slab,
    v_slab,
    k_tm,
    v_tm,
    k_fm,
    v_fm,
    q_fm,
    g_fm,
    qs_fm,
    gs_fm,
    p_ref,
    ds_ref,
    att_out,
    attn_all,
    attn_tm,
    attn_in,
    dt_ref,
    dt_in,
    g_out,
    g_slab,
    xv_out,
    xv_in,
    xk_out,
    xk_in,
    v_own,
    k_own,
    oq,
    ok,
    ov,
    xa_ref,
    xa_in,
    za_ref,
    za_in,
    zb_ref,
    zb_in,
    xb_ref,
    xb_in,
    piece_ref,
    yb_ref,
    tile_own,
    tile_all,
    sum_own,
    sum_all,
    load_sem,
    send_sem,
    recv_sem,
    k_recv,
    v_recv,
    q_recv,
    g_recv,
):
    rows = t_ref.shape[0]
    chips = members // 2
    features, share = dw_ref.shape
    me = lax.axis_index("patch")
    dp = lax.axis_index("dp")
    chip, core = me // 2, me % 2
    cx, cz = dp // ZS, dp % ZS
    partner = chip * 2 + 1 - core

    loads = [
        pltpu.make_async_copy(src, dst, load_sem.at[i])
        for i, (src, dst) in enumerate(
            [(seg_ref, seg_row), (k_ref, k_in), (v_ref, v_in), (q_ref, q_in), (w_hbm, w_ref), (t_hbm, t_ref)]
        )
    ]
    for load in loads:
        load.start()

    barrier = pltpu.get_barrier_semaphore()
    for shift in range(1, members):
        pl.semaphore_signal(barrier, inc=1, device_id=(dp, lax.rem(me + shift, members)), device_id_type=MESH)
    for shift in range(1, groups):
        pl.semaphore_signal(barrier, inc=1, device_id=(lax.rem(dp + shift, groups), me), device_id_type=MESH)
    for load in loads[:4]:
        load.wait()
    seg_all[0] = seg_row[...]
    pl.semaphore_wait(barrier, members + groups - 2)

    def copy(src, dst, send, recv, device):
        return pltpu.make_async_remote_copy(
            src_ref=src, dst_ref=dst, send_sem=send, recv_sem=recv, device_id=device, device_id_type=MESH
        )

    def arrived(ref, recv):
        copy(ref, ref, send_sem.at[0], recv, (dp, partner)).wait_recv()

    def sent(ref, send):
        copy(ref, ref, send, recv_sem.at[0], (dp, partner)).wait_send()

    def some(ref, n):
        return ref.at[pl.ds(0, n)]

    SEG, ATTN, XV, XK, DQ, DK, DV, TILE_SUM, ALL_SUM, DT, AT, XA, ZA, ZB, XB, Y, K, V, Q, G = range(20)
    twin = (dp, partner)

    def far(shift):
        return lax.rem(chip + shift, chips)

    def same(shift):
        return (dp, far(shift) * 2 + core)

    def cross(shift):
        return (dp, far(shift) * 2 + 1 - core)

    group_of = {slot: i for i, pair in enumerate(PAIRS) for slot in pair}
    order = [slot for pair in PAIRS for slot in pair if slot]
    position = {slot: i for i, slot in enumerate(slot for pair in PAIRS for slot in pair)}

    for s in order:
        copy(seg_row, seg_all.at[chips - s], send_sem.at[SEG], recv_sem.at[SEG], same(s)).start()
    for s in order + [0]:
        slot = chips + (chips - s) % chips
        copy(seg_row, seg_all.at[slot], send_sem.at[SEG], recv_sem.at[SEG], cross(s)).start()
    for number, source, slab, recv in ((K, k_in, k_slab, k_recv), (V, v_in, v_slab, v_recv)):
        copy(source.at[chip], slab.at[chips], send_sem.at[number], recv.at[len(PAIRS)], twin).start()
    for number, source, slab, recv in ((K, k_in, k_slab, k_recv), (V, v_in, v_slab, v_recv), (Q, q_in, q_slab, q_recv)):
        for s in order:
            slot = chips - s
            copy(source.at[far(s)], slab.at[slot], send_sem.at[number], recv.at[group_of[slot]], same(s)).start()

    length = len_ref[0]
    lane = lax.broadcasted_iota(jnp.int32, (1, rows), 1)
    sublane = lax.broadcasted_iota(jnp.int32, (16, rows), 0)

    def is_group(slot):
        owner = far(slot % chips) * 2 + (core if slot < chips else 1 - core)
        group = jnp.where(owner * rows + lane < length, seg_all[slot], -1) + 1
        return jnp.where(jnp.broadcast_to(group, (16, rows)) == sublane, 1.0, 0.0)

    zeros40 = jnp.zeros((40, rows), F32)
    zeros48 = jnp.zeros((48, rows), F32)
    zeros8 = jnp.zeros((8, rows), F32)
    ones8 = jnp.ones((8, rows), F32)

    def columns(slot):
        return slice(slot * rows, (slot + 1) * rows)

    def query_columns(slot):
        return columns(position[slot])

    def take_key(slot, value):
        full = jnp.concatenate([value.astype(F32), is_group(slot), zeros40], axis=0)
        k_fm[:, columns(slot)] = full[:FM].astype(BF16)
        k_tm[columns(slot), :] = full.T.astype(BF16)

    def take_value(slot, value):
        full = jnp.concatenate([value.astype(F32), ones8, zeros48], axis=0)
        v_fm[:, columns(slot)] = full[:FM].astype(BF16)
        v_tm[columns(slot), :] = full.T.astype(BF16)

    def beside(pair, slots):
        return jnp.concatenate([slots(slot) for slot in pair], axis=1)

    def take_queries(pair, span):
        code = (1.0 - beside(pair, is_group)) * NEG_LARGE
        value = beside(pair, lambda slot: (q_slab[slot] if slot else q_in[chip]).astype(F32))
        wide40 = jnp.concatenate([zeros40, zeros40], axis=1)
        q_fm[:, span] = jnp.concatenate([value, code, wide40], axis=0).astype(BF16)

    arrived(some(seg_all, members - 1), recv_sem.at[SEG])

    def gather(number, own, slab, recv, take):
        take(0, own[chip])
        for i, pair in enumerate(PAIRS):
            pair = [slot for slot in pair if slot]
            arrived(some(slab, len(pair)), recv.at[i])
            for slot in pair:
                relay = recv.at[len(PAIRS) + i]
                copy(slab.at[slot], slab.at[chips + slot], send_sem.at[number], relay, twin).start()
            for slot in pair:
                take(slot, slab[slot])

    def gather_twin(slab, recv, take):
        for i, pair in enumerate(PAIRS):
            arrived(some(slab, 2), recv.at[len(PAIRS) + i])
            for slot in pair:
                take(chips + slot, slab[chips + slot])

    gather(K, k_in, k_slab, k_recv, take_key)
    gather_twin(k_slab, k_recv, take_key)
    gather(V, v_in, v_slab, v_recv, take_value)
    gather_twin(v_slab, v_recv, take_value)

    log_scale = math.log2(math.e) / math.sqrt(HEAD_DIM)
    score_scale = 1.0 / math.sqrt(HEAD_DIM)
    total = rows * members
    chunks = [slice(low, low + CHUNK) for low in range(0, total, CHUNK)]

    inverse = []
    for i, pair in enumerate(PAIRS):
        remote = [slot for slot in pair if slot]
        arrived(some(q_slab, len(remote)), q_recv.at[i])
        span = slice(i * TILE, (i + 1) * TILE)
        take_queries(pair, span)
        tile = q_fm[:, span]
        top = None
        for chunk in chunks:
            peak = jnp.max(nn(k_tm[chunk, :], tile), axis=0, keepdims=True)
            top = peak if top is None else jnp.maximum(top, peak)
        top = top * log_scale
        for chunk in chunks:
            p_ref[chunk, span] = jnp.exp2(nn(k_tm[chunk, :], tile) * log_scale - top).astype(BF16)
        accum = nn(v_fm[...], p_ref[:, span])
        denom = accum[HEAD_DIM : HEAD_DIM + 1]
        inverse.append(1.0 / denom)
        attn = (accum[:HEAD_DIM] / denom).astype(BF16)
        for j, slot in enumerate(pair):
            att_out[slot] = attn[:, columns(j)]
            if slot:
                copy(att_out.at[slot], attn_all.at[chip], send_sem.at[ATTN], recv_sem.at[ATTN], same(slot)).start()
            else:
                attn_all[chip] = attn[:, columns(j)]
        scaled = q_fm[:HEAD_DIM, span].astype(F32) * (inverse[i] * score_scale)
        qs_fm[:, span] = jnp.concatenate([scaled, jnp.zeros((FM - HEAD_DIM, TILE), F32)], axis=0).astype(BF16)

    loads[4].wait()
    loads[5].wait()
    arrived(some(attn_all, chips - 1), recv_sem.at[ATTN])
    stacked = [attn_all[h].astype(F32) for h in range(HEADS)] + [jnp.zeros((FEAT_PAD - FEAT, rows), F32)]
    attn_tm[...] = jnp.concatenate(stacked, axis=0).T.astype(BF16)
    copy(attn_tm, attn_in, send_sem.at[AT], recv_sem.at[AT], twin).start()
    own_live = me * rows + lax.broadcasted_iota(jnp.int32, (rows, 1), 0) < length
    output = nn(attn_tm[:, :FEAT], w_ref[...])
    error = jnp.where(own_live, output - t_ref[...].astype(F32), 0.0)
    dout_t = (2.0 * error).T
    dout_t = dout_t.astype(BF16)
    dt_ref[...] = dout_t.reshape(dt_ref.shape)
    grad = nn(w_ref[...], dout_t)
    for h in range(HEADS):
        g_out[h] = grad[HEAD_DIM * h : HEAD_DIM * (h + 1)].astype(BF16)
    for s in order:
        slot = chips - s
        copy(g_out.at[far(s)], g_slab.at[slot], send_sem.at[G], g_recv.at[group_of[slot]], same(s)).start()

    for x in range(XS):
        copy(dt_ref.at[2 * x + 1 - core], dt_in.at[x], send_sem.at[DT], recv_sem.at[DT], twin).start()
    loss_part = jnp.sum(jnp.sum(error * error, axis=0, keepdims=True), axis=1, keepdims=True)
    tile_own[...] = jnp.broadcast_to(loss_part, tile_own.shape)
    for shift in range(1, members):
        peer = (dp, lax.rem(me + shift, members))
        copy(tile_own, tile_all.at[members - shift], send_sem.at[TILE_SUM], recv_sem.at[TILE_SUM], peer).start()
    tile_all[0] = tile_own[...]
    arrived(attn_in, recv_sem.at[AT])
    arrived(dt_in, recv_sem.at[DT])
    tall = ZH * share
    left = jnp.concatenate(
        [jnp.concatenate([dt_ref[2 * x + core], dt_in[x]], axis=1) for x in range(XS)], axis=0
    )
    right = jnp.concatenate([attn_tm[...], attn_in[...]], axis=0)
    xa_ref[...] = nn(left, right[:, :X_LANES]).astype(BF16).reshape(XS, tall, X_LANES)
    for d in range(1, XS):
        x = lax.rem(cx + d, XS)
        item = copy(xa_ref.at[x], xa_in.at[XS - d - 1], send_sem.at[XA], recv_sem.at[XA], (x * ZS + cz, me))
        item.start()
    part = nn(left, right[:, X_LANES:])
    for x in range(XS):
        for j in range(ZH):
            low = x * tall + j * share
            za_ref[j, x] = part[low : low + share].astype(BF16)

    def along_z(source, landing, number):
        for j in range(ZH):
            target = ZH * core + j

            @pl.when(target != cz)
            def _():
                slot = lax.rem(cz - target + 2 * ZS - 1, ZS)
                device = (cx * ZS + target, me)
                copy(source.at[j], landing.at[slot], send_sem.at[number], recv_sem.at[number], device).start()

    along_z(za_ref, za_in, ZA)
    near = core == cz // ZH
    away = core != cz // ZH
    mine = lax.rem(cz, ZH)

    def take_grads(i, pair, span):
        wide = beside(pair, lambda slot: (g_slab[slot] if slot else g_out[chip]).astype(F32))
        attn = beside(pair, lambda slot: att_out[slot].astype(F32))
        delta = -jnp.sum(wide * attn, axis=0, keepdims=True)
        high = delta.astype(BF16).astype(F32)
        middle = (delta - high).astype(BF16).astype(F32)
        low = delta - high - middle
        index = lax.broadcasted_iota(jnp.int32, (8, TILE), 0)
        extra = jnp.where(index == 0, high, jnp.where(index == 1, middle, jnp.where(index == 2, low, 0.0)))
        g_fm[:, span] = jnp.concatenate([wide, extra, jnp.zeros((48, TILE), F32)], axis=0).astype(BF16)
        scaled = jnp.concatenate([wide * inverse[i], jnp.zeros((FM - HEAD_DIM, TILE), F32)], axis=0)
        gs_fm[:, span] = scaled.astype(BF16)

    def send_home(slot, out, ref, number):
        if slot:
            copy(out.at[slot], ref.at[chip], send_sem.at[number], recv_sem.at[number], same(slot)).start()
        else:
            item = pltpu.make_async_copy(out.at[0], ref.at[chip], load_sem.at[len(local)])
            item.start()
            local.append(item)

    local = []
    for i, pair in enumerate(PAIRS):
        remote = [slot for slot in pair if slot]
        arrived(some(g_slab, len(remote)), g_recv.at[i])
        span = slice(i * TILE, (i + 1) * TILE)
        take_grads(i, pair, span)
        tile = g_fm[:, span]
        for c, chunk in enumerate(chunks):
            dprobs = nn(v_tm[chunk, :], tile)
            ds_ref[chunk, span] = (p_ref[chunk, span].astype(F32) * dprobs).astype(BF16)
        dq = nn(k_fm[...], ds_ref[:, span])
        dq = (dq[:HEAD_DIM] * (inverse[i] * score_scale)).astype(BF16)
        for j, slot in enumerate(pair):
            oq[slot] = dq[:, columns(j)]
            send_home(slot, oq, dq_ref, DQ)

    half = len(chunks) // 2

    def key_side(c, left, right_ref, target):
        result = nt(left, right_ref[chunks[c], :])
        for j in range(CHUNK // rows):
            target[(c % half) * (CHUNK // rows) + j] = result[:HEAD_DIM, columns(j)]

    def swap(out_ref, in_ref, number):
        copy(out_ref, in_ref, send_sem.at[number], recv_sem.at[number], twin).start()

    def key_home(mine, in_ref, number, out, ref, home):
        arrived(in_ref, recv_sem.at[number])
        for slot in order + [0]:
            out[slot] = (mine[slot] + in_ref[slot]).astype(BF16)
            send_home(slot, out, ref, home)

    arrived(some(tile_all, members - 1), recv_sem.at[TILE_SUM])
    pack_loss = tile_all[0]
    for slot in range(1, members):
        pack_loss = pack_loss + tile_all[slot]
    sum_own[...] = jnp.where(lane == 0, pack_loss, length.astype(F32))
    for shift in range(1, groups):
        peer = (lax.rem(dp + shift, groups), me)
        copy(sum_own, sum_all.at[groups - shift], send_sem.at[ALL_SUM], recv_sem.at[ALL_SUM], peer).start()
    sum_all[0] = sum_own[...]

    for c in range(half, 2 * half):
        key_side(c, gs_fm[...], p_ref, xv_out)
    swap(xv_out, xv_in, XV)
    for c in range(half):
        key_side(c, gs_fm[...], p_ref, v_own)
    arrived(xa_in, recv_sem.at[XA])
    summed = xa_ref[cx].astype(F32)
    for i in range(XS - 1):
        summed = summed + xa_in[i].astype(F32)
    for j in range(ZH):
        zb_ref[j] = summed[j * share : (j + 1) * share].astype(BF16)
    along_z(zb_ref, zb_in, ZB)

    for c in range(half, 2 * half):
        key_side(c, qs_fm[...], ds_ref, xk_out)
    swap(xk_out, xk_in, XK)
    key_home(v_own, xv_in, XV, ov, dv_ref, DV)
    for c in range(half):
        key_side(c, qs_fm[...], ds_ref, k_own)
    key_home(k_own, xk_in, XK, ok, dk_ref, DK)

    @pl.when(near)
    def _():
        arrived(some(za_in, ZS - 1), recv_sem.at[ZA])
        for x in range(XS):
            summed = za_ref[mine, x].astype(F32)
            for i in range(ZS - 1):
                summed = summed + za_in[i, x].astype(F32)
            xb_ref[x] = summed.astype(BF16)
        for d in range(1, XS):
            x = lax.rem(cx + d, XS)
            item = copy(xb_ref.at[x], xb_in.at[XS - d - 1], send_sem.at[XB], recv_sem.at[XB], (x * ZS + cz, me))
            item.start()

    third = features // 3

    @pl.when(near)
    def _():
        arrived(some(zb_in, ZS - 1), recv_sem.at[ZB])
        summed = zb_ref[mine].astype(F32)
        for i in range(ZS - 1):
            summed = summed + zb_in[i].astype(F32)
        arrived(xb_in, recv_sem.at[XB])
        other = xb_ref[cx].astype(F32)
        for i in range(XS - 1):
            other = other + xb_in[i].astype(F32)
        whole = jnp.concatenate([summed, other], axis=1)
        rolled = [whole] + [pltpu.roll(whole, FEAT_PAD - third * i, 1) for i in (1, 2)]
        turned = jnp.concatenate(rolled + [jnp.zeros((LANES - 3 * share, FEAT_PAD), F32)], axis=0).T
        for t in range(members):
            piece_ref[t] = turned[t * features : t * features + third].astype(BF16)
        for shift in range(1, members):
            target = lax.rem(me + shift, members)
            copy(piece_ref.at[target], yb_ref.at[chip], send_sem.at[Y], recv_sem.at[Y], (dp, target)).start()
        yb_ref[chip] = piece_ref[me]

    arrived(some(sum_all, groups - 1), recv_sem.at[ALL_SUM])
    totals = sum_all[0]
    for slot in range(1, groups):
        totals = totals + sum_all[slot]
    sum_ref[...] = totals

    for ref, number in ((dv_ref, DV), (dq_ref, DQ), (dk_ref, DK)):
        arrived(some(ref, chips - 1), recv_sem.at[number])

    @pl.when(near)
    def _():
        arrived(some(yb_ref, chips - 1), recv_sem.at[Y])

    @pl.when(away)
    def _():
        arrived(yb_ref, recv_sem.at[Y])

    result = yb_ref[0].astype(F32)
    for j in range(1, chips):
        result = result + yb_ref[j].astype(F32)
    for i in range(3):
        dw_ref[i * third : (i + 1) * third, :] = result[:, i * share : (i + 1) * share]

    for item in local:
        item.wait()
    sent(some(seg_all, members - 1), send_sem.at[SEG])
    sent(some(k_slab, members - 1), send_sem.at[K])
    sent(some(v_slab, members - 1), send_sem.at[V])
    for ref, number in ((q_slab, Q), (attn_all, ATTN), (g_slab, G), (dq_ref, DQ), (dv_ref, DV), (dk_ref, DK)):
        sent(some(ref, chips - 1), send_sem.at[number])
    for ref, number in ((attn_tm, AT), (dt_in, DT), (xv_in, XV), (xk_in, XK)):
        sent(ref, send_sem.at[number])
    sent(some(tile_all, members - 1), send_sem.at[TILE_SUM])
    sent(some(sum_all, groups - 1), send_sem.at[ALL_SUM])

    sent(xa_in, send_sem.at[XA])

    @pl.when(near)
    def _():
        sent(some(za_ref, ZH - 1), send_sem.at[ZA])
        sent(some(zb_ref, ZH - 1), send_sem.at[ZB])
        sent(xb_in, send_sem.at[XB])
        sent(some(piece_ref, members - 1), send_sem.at[Y])

    @pl.when(away)
    def _():
        sent(za_ref, send_sem.at[ZA])
        sent(zb_ref, send_sem.at[ZB])


def scale_kernel(slots, total, sum_ref, dq_ref, dk_ref, dv_ref, dw_ref, query_ref, key_ref, value_ref, weight_ref, loss_ref):
    count = sum_ref[0:1, 1:2]
    ratio = slots / count
    for source, target in ((dq_ref, query_ref), (dk_ref, key_ref), (dv_ref, value_ref)):
        for h in range(HEADS):
            target[HEAD_DIM * h : HEAD_DIM * (h + 1), :] = source[h].astype(F32) * ratio
    weight_ref[...] = dw_ref[...] * (ratio / total)
    loss_ref[...] = sum_ref[0:1, 0:1] / (count * WIDTH)


def solution(mesh):
    members, groups = mesh.shape["patch"], mesh.shape["dp"]

    def local(query_rows, key_rows, value_rows, out_weight, target, lengths, segments):
        rows = query_rows.shape[1]
        total = rows * members
        chips = members // 2
        queries = rows * chips
        share = WIDTH // groups
        vmem = pl.BlockSpec(memory_space=pltpu.VMEM)
        hbm = pl.BlockSpec(memory_space=pltpu.HBM)
        dma = pltpu.SemaphoreType.DMA
        slab = (HEAD_DIM, rows)

        def heads(value):
            return value[0].T.reshape(HEADS, HEAD_DIM, rows)

        def bf(*shape):
            return pltpu.VMEM(shape, BF16)

        def fl(*shape):
            return pltpu.VMEM(shape, F32)

        outs = pl.pallas_call(
            functools.partial(kernel, members, groups),
            out_shape=(
                jax.ShapeDtypeStruct((HEADS, HEAD_DIM, rows), BF16),
                jax.ShapeDtypeStruct((HEADS, HEAD_DIM, rows), BF16),
                jax.ShapeDtypeStruct((HEADS, HEAD_DIM, rows), BF16),
                jax.ShapeDtypeStruct((FEAT // members, share), F32),
                jax.ShapeDtypeStruct((1, LANES), F32),
            ),
            in_specs=[pl.BlockSpec(memory_space=pltpu.SMEM)] + [hbm] * 6,
            out_specs=(hbm, hbm, hbm, vmem, vmem),
            scratch_shapes=[
                bf(HEADS, *slab),
                bf(HEADS, *slab),
                bf(HEADS, *slab),
                bf(FEAT, WIDTH),
                bf(rows, WIDTH),
                pltpu.VMEM((1, rows), jnp.int32),
                pltpu.VMEM((members, 1, rows), jnp.int32),
                bf(chips, *slab),
                bf(members, *slab),
                bf(members, *slab),
                bf(total, LANES),
                bf(total, LANES),
                bf(FM, total),
                bf(FM, total),
                bf(LANES, queries),
                bf(LANES, queries),
                bf(FM, queries),
                bf(FM, queries),
                bf(total, queries),
                bf(total, queries),
                bf(chips, *slab),
                bf(HEADS, *slab),
                bf(rows, FEAT_PAD),
                bf(rows, FEAT_PAD),
                bf(2 * XS, ZH * share, rows),
                bf(XS, ZH * share, rows),
                bf(HEADS, *slab),
                bf(chips, *slab),
                fl(chips, *slab),
                fl(chips, *slab),
                fl(chips, *slab),
                fl(chips, *slab),
                fl(chips, *slab),
                fl(chips, *slab),
                bf(chips, *slab),
                bf(chips, *slab),
                bf(chips, *slab),
                bf(XS, ZH * share, X_LANES),
                bf(XS - 1, ZH * share, X_LANES),
                bf(ZH, XS, share, Z_LANES),
                bf(ZS, XS, share, Z_LANES),
                bf(ZH, share, X_LANES),
                bf(ZS, share, X_LANES),
                bf(XS, share, Z_LANES),
                bf(XS - 1, share, Z_LANES),
                bf(members, FEAT // members // 3, LANES),
                bf(chips, FEAT // members // 3, LANES),
                fl(1, LANES),
                fl(members, 1, LANES),
                fl(1, LANES),
                fl(groups, 1, LANES),
                dma((6,)),
                dma((20,)),
                dma((16,)),
                dma((2 * len(PAIRS),)),
                dma((2 * len(PAIRS),)),
                dma((len(PAIRS),)),
                dma((len(PAIRS),)),
            ],
            compiler_params=pltpu.CompilerParams(collective_id=0, has_side_effects=True, vmem_limit_bytes=65900000),
            name="sublayer",
        )(
            lengths,
            segments,
            heads(query_rows),
            heads(key_rows),
            heads(value_rows),
            out_weight,
            target[0],
        )
        final = pl.pallas_call(
            functools.partial(scale_kernel, groups * total, total),
            out_shape=(
                jax.ShapeDtypeStruct((FEAT, rows), F32),
                jax.ShapeDtypeStruct((FEAT, rows), F32),
                jax.ShapeDtypeStruct((FEAT, rows), F32),
                jax.ShapeDtypeStruct((FEAT // members, share), F32),
                jax.ShapeDtypeStruct((1, 1), F32),
            ),
            in_specs=[vmem] * 5,
            out_specs=(vmem,) * 5,
            compiler_params=pltpu.CompilerParams(vmem_limit_bytes=65900000),
            name="scale",
        )(outs[4], *outs[:4])
        return (final[0].T[None], final[1].T[None], final[2].T[None], final[3], final[4].reshape(()))

    placed = (
        P("dp", "patch", None),
        P("dp", "patch", None),
        P("dp", "patch", None),
        P(),
        P("dp", "patch", None),
        P("dp"),
        P("dp", "patch"),
    )
    return jax.shard_map(
        local,
        mesh=mesh,
        in_specs=placed,
        out_specs=(
            P("dp", "patch", None),
            P("dp", "patch", None),
            P("dp", "patch", None),
            P("patch", "dp"),
            P(),
        ),
        check_vma=False,
    )
```

```python
import functools
import math

import jax
import jax.numpy as jnp
from jax import lax
from jax.experimental import pallas as pl
from jax.experimental.pallas import tpu as pltpu
from jax.sharding import PartitionSpec as P

MESH = pl.DeviceIdType.MESH
WIDTH = 1152
HEADS = 8
HEAD_DIM = 72
FEAT = 576
FEAT_PAD = 640
FM = 80
LANES = 128
SPAN = 256
TILE = 256
CHUNK = 256
NEG_LARGE = -1e30
F32 = jnp.float32
BF16 = jnp.bfloat16
XS, ZS = 4, 8
ZH = ZS // 2
X_LANES = 384
LEADER = 1
Z_LANES = 256
PAIRS = ((4, 0), (3, 5), (2, 6), (1, 7))


def nt(left, right):
    return lax.dot_general(left, right, (((1,), (1,)), ((), ())), preferred_element_type=F32)


def nn(left, right):
    return lax.dot_general(left, right, (((1,), (0,)), ((), ())), preferred_element_type=F32)


def tn(left, right):
    return lax.dot_general(left, right, (((0,), (0,)), ((), ())), preferred_element_type=F32)


def kernel(
    members,
    groups,
    len_ref,
    seg_ref,
    q_ref,
    k_ref,
    v_ref,
    w_hbm,
    t_hbm,
    dq_ref,
    dk_ref,
    dv_ref,
    yb_ref,
    sum_all,
    q_in,
    k_in,
    v_in,
    w_ref,
    t_ref,
    seg_row,
    seg_all,
    q_slab,
    k_slab,
    v_slab,
    k_tm,
    v_tm,
    k_fm,
    v_fm,
    q_fm,
    g_fm,
    qs_fm,
    gs_fm,
    p_ref,
    ds_ref,
    att_out,
    attn_all,
    attn_tm,
    attn_in,
    dt_ref,
    dt_in,
    g_out,
    g_slab,
    xv_out,
    xv_in,
    xk_out,
    xk_in,
    v_own,
    k_own,
    oq,
    ok,
    ov,
    xa_ref,
    xa_in,
    za_ref,
    za_in,
    zb_ref,
    zb_in,
    xb_ref,
    xb_in,
    piece_ref,
    tile_own,
    tile_all,
    sum_own,
    ready,
    load_sem,
    send_sem,
    recv_sem,
    k_recv,
    v_recv,
    q_recv,
    g_recv,
):
    rows = t_ref.shape[0]
    chips = members // 2
    share = WIDTH // groups
    features = FEAT // members
    me = lax.axis_index("patch")
    dp = lax.axis_index("dp")
    chip, core = me // 2, me % 2
    cx, cz = dp // ZS, dp % ZS
    partner = chip * 2 + 1 - core

    loads = [
        pltpu.make_async_copy(src, dst, load_sem.at[i])
        for i, (src, dst) in enumerate(
            [(seg_ref, seg_row), (k_ref, k_in), (v_ref, v_in), (q_ref, q_in), (w_hbm, w_ref), (t_hbm, t_ref)]
        )
    ]
    for load in loads:
        load.start()

    barrier = pltpu.get_barrier_semaphore()
    for shift in range(1, members):
        pl.semaphore_signal(barrier, inc=1, device_id=(dp, lax.rem(me + shift, members)), device_id_type=MESH)
    for load in loads[:4]:
        load.wait()
    seg_all[0] = seg_row[...]
    leads = me == LEADER

    @pl.when(jnp.logical_not(leads))
    def _():
        pl.semaphore_wait(barrier, members - 1)

    @pl.when(me == LEADER - 1)
    def _():
        pl.semaphore_signal(ready, inc=1, device_id=(dp, LEADER), device_id_type=MESH)

    @pl.when(leads)
    def _():
        pl.semaphore_wait(ready, 1)
        for shift in range(1, groups):
            pl.semaphore_signal(barrier, inc=1, device_id=(lax.rem(dp + shift, groups), me), device_id_type=MESH)

    def copy(src, dst, send, recv, device):
        return pltpu.make_async_remote_copy(
            src_ref=src, dst_ref=dst, send_sem=send, recv_sem=recv, device_id=device, device_id_type=MESH
        )

    def arrived(ref, recv):
        copy(ref, ref, send_sem.at[0], recv, (dp, partner)).wait_recv()

    def sent(ref, send):
        copy(ref, ref, send, recv_sem.at[0], (dp, partner)).wait_send()

    def some(ref, n):
        return ref.at[pl.ds(0, n)]

    SEG, ATTN, XV, XK, DQ, DK, DV, TILE_SUM, ALL_SUM, DT, AT, XA, ZA, ZB, XB, Y, K, V, Q, G = range(20)
    twin = (dp, partner)

    def far(shift):
        return lax.rem(chip + shift, chips)

    def same(shift):
        return (dp, far(shift) * 2 + core)

    def cross(shift):
        return (dp, far(shift) * 2 + 1 - core)

    group_of = {slot: i for i, pair in enumerate(PAIRS) for slot in pair}
    order = [slot for pair in PAIRS for slot in pair if slot]
    position = {slot: i for i, slot in enumerate(slot for pair in PAIRS for slot in pair)}

    for s in order:
        copy(seg_row, seg_all.at[chips - s], send_sem.at[SEG], recv_sem.at[SEG], same(s)).start()
    for s in order + [0]:
        slot = chips + (chips - s) % chips
        copy(seg_row, seg_all.at[slot], send_sem.at[SEG], recv_sem.at[SEG], cross(s)).start()
    for number, source, slab, recv in ((K, k_in, k_slab, k_recv), (V, v_in, v_slab, v_recv)):
        copy(source.at[chip], slab.at[chips], send_sem.at[number], recv.at[len(PAIRS)], twin).start()
    for number, source, slab, recv in ((K, k_in, k_slab, k_recv), (V, v_in, v_slab, v_recv), (Q, q_in, q_slab, q_recv)):
        for s in order:
            slot = chips - s
            copy(source.at[far(s)], slab.at[slot], send_sem.at[number], recv.at[group_of[slot]], same(s)).start()

    length = len_ref[0]
    lane = lax.broadcasted_iota(jnp.int32, (1, rows), 1)
    sublane = lax.broadcasted_iota(jnp.int32, (16, rows), 0)

    def is_group(slot):
        owner = far(slot % chips) * 2 + (core if slot < chips else 1 - core)
        group = jnp.where(owner * rows + lane < length, seg_all[slot], -1) + 1
        return jnp.where(jnp.broadcast_to(group, (16, rows)) == sublane, 1.0, 0.0)

    zeros40 = jnp.zeros((40, rows), F32)
    zeros48 = jnp.zeros((48, rows), F32)
    zeros8 = jnp.zeros((8, rows), F32)
    ones8 = jnp.ones((8, rows), F32)

    def columns(slot):
        return slice(slot * rows, (slot + 1) * rows)

    def query_columns(slot):
        return columns(position[slot])

    def take_key(slot, value):
        full = jnp.concatenate([value.astype(F32), is_group(slot), zeros40], axis=0)
        k_fm[:, columns(slot)] = full[:FM].astype(BF16)
        k_tm[columns(slot), :] = full.T.astype(BF16)

    def take_value(slot, value):
        full = jnp.concatenate([value.astype(F32), ones8, zeros48], axis=0)
        v_fm[:, columns(slot)] = full[:FM].astype(BF16)
        v_tm[columns(slot), :] = full.T.astype(BF16)

    def beside(pair, slots):
        return jnp.concatenate([slots(slot) for slot in pair], axis=1)

    def take_queries(pair, span):
        code = (1.0 - beside(pair, is_group)) * NEG_LARGE
        value = beside(pair, lambda slot: (q_slab[slot] if slot else q_in[chip]).astype(F32))
        wide40 = jnp.concatenate([zeros40, zeros40], axis=1)
        q_fm[:, span] = jnp.concatenate([value, code, wide40], axis=0).astype(BF16)

    arrived(some(seg_all, members - 1), recv_sem.at[SEG])

    def gather(number, own, slab, recv, take):
        take(0, own[chip])
        for i, pair in enumerate(PAIRS):
            pair = [slot for slot in pair if slot]
            arrived(some(slab, len(pair)), recv.at[i])
            for slot in pair:
                relay = recv.at[len(PAIRS) + i]
                copy(slab.at[slot], slab.at[chips + slot], send_sem.at[number], relay, twin).start()
            for slot in pair:
                take(slot, slab[slot])

    def gather_twin(slab, recv, take):
        for i, pair in enumerate(PAIRS):
            arrived(some(slab, 2), recv.at[len(PAIRS) + i])
            for slot in pair:
                take(chips + slot, slab[chips + slot])

    gather(K, k_in, k_slab, k_recv, take_key)
    gather_twin(k_slab, k_recv, take_key)
    gather(V, v_in, v_slab, v_recv, take_value)
    gather_twin(v_slab, v_recv, take_value)

    log_scale = math.log2(math.e) / math.sqrt(HEAD_DIM)
    score_scale = 1.0 / math.sqrt(HEAD_DIM)
    total = rows * members
    chunks = [slice(low, low + CHUNK) for low in range(0, total, CHUNK)]

    inverse = []
    for i, pair in enumerate(PAIRS):
        remote = [slot for slot in pair if slot]
        arrived(some(q_slab, len(remote)), q_recv.at[i])
        span = slice(i * TILE, (i + 1) * TILE)
        take_queries(pair, span)
        tile = q_fm[:, span]
        top = None
        for chunk in chunks:
            peak = jnp.max(nn(k_tm[chunk, :], tile), axis=0, keepdims=True)
            top = peak if top is None else jnp.maximum(top, peak)
        top = top * log_scale
        for chunk in chunks:
            p_ref[chunk, span] = jnp.exp2(nn(k_tm[chunk, :], tile) * log_scale - top).astype(BF16)
        accum = nn(v_fm[...], p_ref[:, span])
        denom = accum[HEAD_DIM : HEAD_DIM + 1]
        inverse.append(1.0 / denom)
        attn = (accum[:HEAD_DIM] / denom).astype(BF16)
        for j, slot in enumerate(pair):
            att_out[slot] = attn[:, columns(j)]
            if slot:
                copy(att_out.at[slot], attn_all.at[chip], send_sem.at[ATTN], recv_sem.at[ATTN], same(slot)).start()
            else:
                attn_all[chip] = attn[:, columns(j)]
        scaled = q_fm[:HEAD_DIM, span].astype(F32) * (inverse[i] * score_scale)
        qs_fm[:, span] = jnp.concatenate([scaled, jnp.zeros((FM - HEAD_DIM, TILE), F32)], axis=0).astype(BF16)

    @pl.when(leads)
    def _():
        pl.semaphore_wait(barrier, members + groups - 2)
        for shift in range(1, members):
            peer = (dp, lax.rem(me + shift, members))
            pl.semaphore_signal(ready, inc=1, device_id=peer, device_id_type=MESH)

    loads[4].wait()
    loads[5].wait()
    arrived(some(attn_all, chips - 1), recv_sem.at[ATTN])
    stacked = [attn_all[h].astype(F32) for h in range(HEADS)] + [jnp.zeros((FEAT_PAD - FEAT, rows), F32)]
    attn_tm[...] = jnp.concatenate(stacked, axis=0).T.astype(BF16)
    copy(attn_tm, attn_in, send_sem.at[AT], recv_sem.at[AT], twin).start()
    own_live = me * rows + lax.broadcasted_iota(jnp.int32, (rows, 1), 0) < length
    output = nn(attn_tm[:, :FEAT], w_ref[...])
    error = jnp.where(own_live, output - t_ref[...].astype(F32), 0.0)
    dout_t = (2.0 * error).T
    dout_t = dout_t.astype(BF16)
    dt_ref[...] = dout_t.reshape(dt_ref.shape)
    grad = nn(w_ref[...], dout_t)
    for h in range(HEADS):
        g_out[h] = grad[HEAD_DIM * h : HEAD_DIM * (h + 1)].astype(BF16)
    for s in order:
        slot = chips - s
        copy(g_out.at[far(s)], g_slab.at[slot], send_sem.at[G], g_recv.at[group_of[slot]], same(s)).start()

    for x in range(XS):
        copy(dt_ref.at[2 * x + 1 - core], dt_in.at[x], send_sem.at[DT], recv_sem.at[DT], twin).start()
    loss_part = jnp.sum(jnp.sum(error * error, axis=0, keepdims=True), axis=1, keepdims=True)
    tile_own[...] = jnp.broadcast_to(loss_part, tile_own.shape)
    for shift in range(1, members):
        peer = (dp, lax.rem(me + shift, members))
        copy(tile_own, tile_all.at[members - shift], send_sem.at[TILE_SUM], recv_sem.at[TILE_SUM], peer).start()
    tile_all[0] = tile_own[...]
    arrived(attn_in, recv_sem.at[AT])
    arrived(dt_in, recv_sem.at[DT])
    tall = ZH * share
    left = jnp.concatenate(
        [jnp.concatenate([dt_ref[2 * x + core], dt_in[x]], axis=1) for x in range(XS)], axis=0
    )
    right = jnp.concatenate([attn_tm[...], attn_in[...]], axis=0)
    xa_ref[...] = nn(left, right[:, :X_LANES]).astype(BF16).reshape(XS, tall, X_LANES)

    @pl.when(jnp.logical_not(leads))
    def _():
        pl.semaphore_wait(ready, 1)

    for d in range(1, XS):
        x = lax.rem(cx + d, XS)
        item = copy(xa_ref.at[x], xa_in.at[XS - d - 1], send_sem.at[XA], recv_sem.at[XA], (x * ZS + cz, me))
        item.start()
    part = nn(left, right[:, X_LANES:])
    for x in range(XS):
        for j in range(ZH):
            low = x * tall + j * share
            za_ref[j, x] = part[low : low + share].astype(BF16)

    def along_z(source, landing, number):
        for j in range(ZH):
            target = ZH * core + j

            @pl.when(target != cz)
            def _():
                slot = lax.rem(cz - target + 2 * ZS - 1, ZS)
                device = (cx * ZS + target, me)
                copy(source.at[j], landing.at[slot], send_sem.at[number], recv_sem.at[number], device).start()

    along_z(za_ref, za_in, ZA)
    near = core == cz // ZH
    away = core != cz // ZH
    mine = lax.rem(cz, ZH)

    def take_grads(i, pair, span):
        wide = beside(pair, lambda slot: (g_slab[slot] if slot else g_out[chip]).astype(F32))
        attn = beside(pair, lambda slot: att_out[slot].astype(F32))
        delta = -jnp.sum(wide * attn, axis=0, keepdims=True)
        high = delta.astype(BF16).astype(F32)
        middle = (delta - high).astype(BF16).astype(F32)
        low = delta - high - middle
        index = lax.broadcasted_iota(jnp.int32, (8, TILE), 0)
        extra = jnp.where(index == 0, high, jnp.where(index == 1, middle, jnp.where(index == 2, low, 0.0)))
        g_fm[:, span] = jnp.concatenate([wide, extra, jnp.zeros((48, TILE), F32)], axis=0).astype(BF16)
        scaled = jnp.concatenate([wide * inverse[i], jnp.zeros((FM - HEAD_DIM, TILE), F32)], axis=0)
        gs_fm[:, span] = scaled.astype(BF16)

    def send_home(slot, out, ref, number):
        if slot:
            copy(out.at[slot], ref.at[chip], send_sem.at[number], recv_sem.at[number], same(slot)).start()
        else:
            item = pltpu.make_async_copy(out.at[0], ref.at[chip], load_sem.at[(DQ, DV, DK).index(number)])
            item.start()
            local.append(item)

    local = []
    for i, pair in enumerate(PAIRS):
        remote = [slot for slot in pair if slot]
        arrived(some(g_slab, len(remote)), g_recv.at[i])
        span = slice(i * TILE, (i + 1) * TILE)
        take_grads(i, pair, span)
        tile = g_fm[:, span]
        for c, chunk in enumerate(chunks):
            dprobs = nn(v_tm[chunk, :], tile)
            ds_ref[chunk, span] = (p_ref[chunk, span].astype(F32) * dprobs).astype(BF16)
        dq = nn(k_fm[...], ds_ref[:, span])
        dq = (dq[:HEAD_DIM] * (inverse[i] * score_scale)).astype(BF16)
        for j, slot in enumerate(pair):
            oq[slot] = dq[:, columns(j)]
            send_home(slot, oq, dq_ref, DQ)

    half = len(chunks) // 2

    def key_side(c, left, right_ref, target):
        result = nt(left, right_ref[chunks[c], :])
        for j in range(CHUNK // rows):
            target[(c % half) * (CHUNK // rows) + j] = result[:HEAD_DIM, columns(j)]

    def swap(out_ref, in_ref, number):
        copy(out_ref, in_ref, send_sem.at[number], recv_sem.at[number], twin).start()

    def key_home(mine, in_ref, number, out, ref, home):
        arrived(in_ref, recv_sem.at[number])
        for slot in order + [0]:
            out[slot] = (mine[slot] + in_ref[slot]).astype(BF16)
            send_home(slot, out, ref, home)

    arrived(some(tile_all, members - 1), recv_sem.at[TILE_SUM])
    pack_loss = tile_all[0]
    for slot in range(1, members):
        pack_loss = pack_loss + tile_all[slot]
    sum_own[...] = jnp.where(lane == 0, pack_loss, length.astype(F32))
    for shift in range(1, groups):
        peer = (lax.rem(dp + shift, groups), me)
        copy(sum_own, sum_all.at[groups - shift], send_sem.at[ALL_SUM], recv_sem.at[ALL_SUM], peer).start()
    local.append(pltpu.make_async_copy(sum_own, sum_all.at[0], load_sem.at[3]))
    local[-1].start()

    for c in range(half, 2 * half):
        key_side(c, gs_fm[...], p_ref, xv_out)
    swap(xv_out, xv_in, XV)
    for c in range(half):
        key_side(c, gs_fm[...], p_ref, v_own)
    arrived(xa_in, recv_sem.at[XA])
    summed = xa_ref[cx].astype(F32)
    for i in range(XS - 1):
        summed = summed + xa_in[i].astype(F32)
    for j in range(ZH):
        zb_ref[j] = summed[j * share : (j + 1) * share].astype(BF16)
    along_z(zb_ref, zb_in, ZB)

    for c in range(half, 2 * half):
        key_side(c, qs_fm[...], ds_ref, xk_out)
    swap(xk_out, xk_in, XK)
    key_home(v_own, xv_in, XV, ov, dv_ref, DV)
    for c in range(half):
        key_side(c, qs_fm[...], ds_ref, k_own)
    key_home(k_own, xk_in, XK, ok, dk_ref, DK)

    @pl.when(near)
    def _():
        arrived(some(za_in, ZS - 1), recv_sem.at[ZA])
        for x in range(XS):
            summed = za_ref[mine, x].astype(F32)
            for i in range(ZS - 1):
                summed = summed + za_in[i, x].astype(F32)
            xb_ref[x] = summed.astype(BF16)
        for d in range(1, XS):
            x = lax.rem(cx + d, XS)
            item = copy(xb_ref.at[x], xb_in.at[XS - d - 1], send_sem.at[XB], recv_sem.at[XB], (x * ZS + cz, me))
            item.start()

    third = features // 3

    @pl.when(near)
    def _():
        arrived(some(zb_in, ZS - 1), recv_sem.at[ZB])
        summed = zb_ref[mine].astype(F32)
        for i in range(ZS - 1):
            summed = summed + zb_in[i].astype(F32)
        arrived(xb_in, recv_sem.at[XB])
        other = xb_ref[cx].astype(F32)
        for i in range(XS - 1):
            other = other + xb_in[i].astype(F32)
        whole = jnp.concatenate([summed, other], axis=1)
        rolled = [whole] + [pltpu.roll(whole, FEAT_PAD - third * i, 1) for i in (1, 2)]
        turned = jnp.concatenate(rolled + [jnp.zeros((LANES - 3 * share, FEAT_PAD), F32)], axis=0).T
        for t in range(members):
            piece_ref[t] = turned[t * features : t * features + third].astype(BF16)
        for shift in range(1, members):
            target = lax.rem(me + shift, members)
            copy(piece_ref.at[target], yb_ref.at[chip], send_sem.at[Y], recv_sem.at[Y], (dp, target)).start()
        pltpu.make_async_copy(piece_ref.at[me], yb_ref.at[chip], load_sem.at[4]).start()

    arrived(some(sum_all, groups - 1), recv_sem.at[ALL_SUM])

    for ref, number in ((dv_ref, DV), (dq_ref, DQ), (dk_ref, DK)):
        arrived(some(ref, chips - 1), recv_sem.at[number])

    @pl.when(near)
    def _():
        arrived(some(yb_ref, chips - 1), recv_sem.at[Y])
        pltpu.make_async_copy(piece_ref.at[me], yb_ref.at[chip], load_sem.at[4]).wait()

    @pl.when(away)
    def _():
        arrived(yb_ref, recv_sem.at[Y])

    for item in local:
        item.wait()
    sent(some(seg_all, members - 1), send_sem.at[SEG])
    sent(some(k_slab, members - 1), send_sem.at[K])
    sent(some(v_slab, members - 1), send_sem.at[V])
    for ref, number in ((q_slab, Q), (attn_all, ATTN), (g_slab, G), (dq_ref, DQ), (dv_ref, DV), (dk_ref, DK)):
        sent(some(ref, chips - 1), send_sem.at[number])
    for ref, number in ((attn_tm, AT), (dt_in, DT), (xv_in, XV), (xk_in, XK)):
        sent(ref, send_sem.at[number])
    sent(some(tile_all, members - 1), send_sem.at[TILE_SUM])
    sent(some(sum_all, groups - 1), send_sem.at[ALL_SUM])

    sent(xa_in, send_sem.at[XA])

    @pl.when(near)
    def _():
        sent(some(za_ref, ZH - 1), send_sem.at[ZA])
        sent(some(zb_ref, ZH - 1), send_sem.at[ZB])
        sent(xb_in, send_sem.at[XB])
        sent(some(piece_ref, members - 1), send_sem.at[Y])

    @pl.when(away)
    def _():
        sent(za_ref, send_sem.at[ZA])
        sent(zb_ref, send_sem.at[ZB])


def scale_kernel(
    slots,
    total,
    sum_hbm,
    dq_hbm,
    dk_hbm,
    dv_hbm,
    yb_hbm,
    query_hbm,
    key_hbm,
    value_hbm,
    weight_ref,
    loss_ref,
    sum_ref,
    slab_ref,
    yb_ref,
    out_ref,
    in_sem,
    out_sem,
):
    sources = [(sum_hbm, sum_ref), (yb_hbm, yb_ref)]
    sources += [(ref, slab_ref.at[i]) for i, ref in enumerate((dv_hbm, dq_hbm, dk_hbm))]
    loads = [pltpu.make_async_copy(src, dst, in_sem.at[i]) for i, (src, dst) in enumerate(sources)]
    for load in loads:
        load.start()
    loads[0].wait()
    totals = sum_ref[0]
    for i in range(1, sum_ref.shape[0]):
        totals = totals + sum_ref[i]
    count = totals[:, 1:2]
    ratio = slots / count
    stores = []
    for i, target in enumerate((value_hbm, query_hbm, key_hbm)):
        loads[i + 2].wait()
        for h in range(HEADS):
            out_ref[i, HEAD_DIM * h : HEAD_DIM * (h + 1), :] = slab_ref[i, h].astype(F32) * ratio
        stores.append(pltpu.make_async_copy(out_ref.at[i], target, out_sem.at[i]))
        stores[-1].start()
    loads[1].wait()
    result = yb_ref[0].astype(F32)
    for i in range(1, yb_ref.shape[0]):
        result = result + yb_ref[i].astype(F32)
    result = result * (ratio / total)
    third, share = result.shape[0], weight_ref.shape[1]
    for i in range(3):
        weight_ref[i * third : (i + 1) * third, :] = result[:, i * share : (i + 1) * share]
    loss_ref[...] = totals[:, 0:1] / (count * WIDTH)
    for store in stores:
        store.wait()


def solution(mesh):
    members, groups = mesh.shape["patch"], mesh.shape["dp"]

    def local(query_rows, key_rows, value_rows, out_weight, target, lengths, segments):
        rows = query_rows.shape[1]
        total = rows * members
        chips = members // 2
        queries = rows * chips
        share = WIDTH // groups
        vmem = pl.BlockSpec(memory_space=pltpu.VMEM)
        hbm = pl.BlockSpec(memory_space=pltpu.HBM)
        dma = pltpu.SemaphoreType.DMA
        slab = (HEAD_DIM, rows)

        def heads(value):
            return value[0].T.reshape(HEADS, HEAD_DIM, rows)

        def bf(*shape):
            return pltpu.VMEM(shape, BF16)

        def fl(*shape):
            return pltpu.VMEM(shape, F32)

        outs = pl.pallas_call(
            functools.partial(kernel, members, groups),
            out_shape=(
                jax.ShapeDtypeStruct((HEADS, HEAD_DIM, rows), BF16),
                jax.ShapeDtypeStruct((HEADS, HEAD_DIM, rows), BF16),
                jax.ShapeDtypeStruct((HEADS, HEAD_DIM, rows), BF16),
                jax.ShapeDtypeStruct((chips, FEAT // members // 3, LANES), BF16),
                jax.ShapeDtypeStruct((groups, 1, LANES), F32),
            ),
            in_specs=[pl.BlockSpec(memory_space=pltpu.SMEM)] + [hbm] * 6,
            out_specs=(hbm,) * 5,
            scratch_shapes=[
                bf(HEADS, *slab),
                bf(HEADS, *slab),
                bf(HEADS, *slab),
                bf(FEAT, WIDTH),
                bf(rows, WIDTH),
                pltpu.VMEM((1, rows), jnp.int32),
                pltpu.VMEM((members, 1, rows), jnp.int32),
                bf(chips, *slab),
                bf(members, *slab),
                bf(members, *slab),
                bf(total, LANES),
                bf(total, LANES),
                bf(FM, total),
                bf(FM, total),
                bf(LANES, queries),
                bf(LANES, queries),
                bf(FM, queries),
                bf(FM, queries),
                bf(total, queries),
                bf(total, queries),
                bf(chips, *slab),
                bf(HEADS, *slab),
                bf(rows, FEAT_PAD),
                bf(rows, FEAT_PAD),
                bf(2 * XS, ZH * share, rows),
                bf(XS, ZH * share, rows),
                bf(HEADS, *slab),
                bf(chips, *slab),
                fl(chips, *slab),
                fl(chips, *slab),
                fl(chips, *slab),
                fl(chips, *slab),
                fl(chips, *slab),
                fl(chips, *slab),
                bf(chips, *slab),
                bf(chips, *slab),
                bf(chips, *slab),
                bf(XS, ZH * share, X_LANES),
                bf(XS - 1, ZH * share, X_LANES),
                bf(ZH, XS, share, Z_LANES),
                bf(ZS, XS, share, Z_LANES),
                bf(ZH, share, X_LANES),
                bf(ZS, share, X_LANES),
                bf(XS, share, Z_LANES),
                bf(XS - 1, share, Z_LANES),
                bf(members, FEAT // members // 3, LANES),
                fl(1, LANES),
                fl(members, 1, LANES),
                fl(1, LANES),
                pltpu.SemaphoreType.REGULAR,
                dma((6,)),
                dma((20,)),
                dma((16,)),
                dma((2 * len(PAIRS),)),
                dma((2 * len(PAIRS),)),
                dma((len(PAIRS),)),
                dma((len(PAIRS),)),
            ],
            compiler_params=pltpu.CompilerParams(collective_id=0, has_side_effects=True, vmem_limit_bytes=65900000),
            name="sublayer",
        )(
            lengths,
            segments,
            heads(query_rows),
            heads(key_rows),
            heads(value_rows),
            out_weight,
            target[0],
        )
        final = pl.pallas_call(
            functools.partial(scale_kernel, groups * total, total),
            out_shape=(
                jax.ShapeDtypeStruct((FEAT, rows), F32),
                jax.ShapeDtypeStruct((FEAT, rows), F32),
                jax.ShapeDtypeStruct((FEAT, rows), F32),
                jax.ShapeDtypeStruct((FEAT // members, share), F32),
                jax.ShapeDtypeStruct((1, 1), F32),
            ),
            in_specs=[hbm] * 5,
            out_specs=(hbm, hbm, hbm, vmem, vmem),
            scratch_shapes=[
                fl(groups, 1, LANES),
                bf(3, HEADS, *slab),
                bf(chips, FEAT // members // 3, LANES),
                fl(3, FEAT, rows),
                dma((5,)),
                dma((3,)),
            ],
            compiler_params=pltpu.CompilerParams(vmem_limit_bytes=65900000),
            name="scale",
        )(outs[4], *outs[:4])
        return (final[0].T[None], final[1].T[None], final[2].T[None], final[3], final[4].reshape(()))

    placed = (
        P("dp", "patch", None),
        P("dp", "patch", None),
        P("dp", "patch", None),
        P(),
        P("dp", "patch", None),
        P("dp"),
        P("dp", "patch"),
    )
    return jax.shard_map(
        local,
        mesh=mesh,
        in_specs=placed,
        out_specs=(
            P("dp", "patch", None),
            P("dp", "patch", None),
            P("dp", "patch", None),
            P("patch", "dp"),
            P(),
        ),
        check_vma=False,
    )
```

```python
import functools
import math

import jax
import jax.numpy as jnp
from jax import lax
from jax.experimental import pallas as pl
from jax.experimental.pallas import tpu as pltpu
from jax.sharding import PartitionSpec as P

MESH = pl.DeviceIdType.MESH
WIDTH = 1152
HEADS = 8
HEAD_DIM = 72
FEAT = 576
FEAT_PAD = 640
FM = 80
LANES = 128
SPAN = 256
TILE = 256
CHUNK = 256
NEG_LARGE = -1e30
F32 = jnp.float32
BF16 = jnp.bfloat16
XS, ZS = 4, 8
ZH = ZS // 2
X_LANES = 384
LEADER = 1
Z_LANES = 256
PAIRS = ((4, 0), (3, 5), (2, 6), (1, 7))


def nt(left, right):
    return lax.dot_general(left, right, (((1,), (1,)), ((), ())), preferred_element_type=F32)


def nn(left, right):
    return lax.dot_general(left, right, (((1,), (0,)), ((), ())), preferred_element_type=F32)


def tn(left, right):
    return lax.dot_general(left, right, (((0,), (0,)), ((), ())), preferred_element_type=F32)


def kernel(
    members,
    groups,
    len_ref,
    seg_ref,
    q_ref,
    k_ref,
    v_ref,
    w_hbm,
    t_hbm,
    dq_ref,
    dk_ref,
    dv_ref,
    yb_ref,
    sum_all,
    q_in,
    k_in,
    v_in,
    w_ref,
    t_ref,
    seg_row,
    seg_all,
    q_slab,
    k_slab,
    v_slab,
    k_tm,
    v_tm,
    k_fm,
    v_fm,
    q_fm,
    g_fm,
    qs_fm,
    gs_fm,
    p_ref,
    ds_ref,
    att_out,
    attn_all,
    attn_tm,
    attn_in,
    dt_ref,
    dt_in,
    g_out,
    g_slab,
    xv_out,
    xv_in,
    xk_out,
    xk_in,
    v_own,
    v_twin,
    k_own,
    oq,
    ok,
    ov,
    xa_ref,
    xa_in,
    za_ref,
    za_in,
    zb_ref,
    zb_in,
    xb_ref,
    xb_in,
    piece_ref,
    tile_own,
    tile_all,
    sum_own,
    ready,
    load_sem,
    send_sem,
    recv_sem,
    k_recv,
    v_recv,
    q_recv,
    g_recv,
):
    rows = t_ref.shape[0]
    chips = members // 2
    share = WIDTH // groups
    features = FEAT // members
    me = lax.axis_index("patch")
    dp = lax.axis_index("dp")
    chip, core = me // 2, me % 2
    cx, cz = dp // ZS, dp % ZS
    partner = chip * 2 + 1 - core

    loads = [
        pltpu.make_async_copy(src, dst, load_sem.at[i])
        for i, (src, dst) in enumerate(
            [(seg_ref, seg_row), (k_ref, k_in), (v_ref, v_in), (q_ref, q_in), (w_hbm, w_ref), (t_hbm, t_ref)]
        )
    ]
    for load in loads:
        load.start()

    barrier = pltpu.get_barrier_semaphore()
    for shift in range(1, members):
        pl.semaphore_signal(barrier, inc=1, device_id=(dp, lax.rem(me + shift, members)), device_id_type=MESH)
    for load in loads[:4]:
        load.wait()
    seg_all[0] = seg_row[...]
    leads = me == LEADER

    @pl.when(jnp.logical_not(leads))
    def _():
        pl.semaphore_wait(barrier, members - 1)

    @pl.when(me == LEADER - 1)
    def _():
        pl.semaphore_signal(ready, inc=1, device_id=(dp, LEADER), device_id_type=MESH)

    @pl.when(leads)
    def _():
        pl.semaphore_wait(ready, 1)
        for shift in range(1, groups):
            pl.semaphore_signal(barrier, inc=1, device_id=(lax.rem(dp + shift, groups), me), device_id_type=MESH)

    def copy(src, dst, send, recv, device):
        return pltpu.make_async_remote_copy(
            src_ref=src, dst_ref=dst, send_sem=send, recv_sem=recv, device_id=device, device_id_type=MESH
        )

    def arrived(ref, recv):
        copy(ref, ref, send_sem.at[0], recv, (dp, partner)).wait_recv()

    def sent(ref, send):
        copy(ref, ref, send, recv_sem.at[0], (dp, partner)).wait_send()

    def some(ref, n):
        return ref.at[pl.ds(0, n)]

    SEG, ATTN, XV, XK, DQ, DK, DV, TILE_SUM, ALL_SUM, DT, AT, XA, ZA, ZB, XB, Y, K, V, Q, G = range(20)
    twin = (dp, partner)

    def far(shift):
        return lax.rem(chip + shift, chips)

    def index_of(shift, flip):
        return far(shift) * 2 + (1 - core if flip else core)

    def peer_of(shift):
        return (dp, index_of(shift, True))

    def other_of(shift):
        return (dp, index_of(shift, not shift))

    group_of = {slot: i for i, pair in enumerate(PAIRS) for slot in pair}
    order = [slot for pair in PAIRS for slot in pair if slot]
    position = {slot: i for i, slot in enumerate(slot for pair in PAIRS for slot in pair)}

    for s in order:
        copy(seg_row, seg_all.at[chips - s], send_sem.at[SEG], recv_sem.at[SEG], peer_of(s)).start()
    for s in order + [0]:
        slot = chips + (chips - s) % chips
        copy(seg_row, seg_all.at[slot], send_sem.at[SEG], recv_sem.at[SEG], other_of(s)).start()
    for number, source, slab, recv in ((K, k_in, k_slab, k_recv), (V, v_in, v_slab, v_recv)):
        copy(source.at[chip], slab.at[chips], send_sem.at[number], recv.at[len(PAIRS)], twin).start()
    for number, source, slab, recv in ((K, k_in, k_slab, k_recv), (V, v_in, v_slab, v_recv), (Q, q_in, q_slab, q_recv)):
        for s in order:
            slot = chips - s
            copy(source.at[far(s)], slab.at[slot], send_sem.at[number], recv.at[group_of[slot]], peer_of(s)).start()

    length = len_ref[0]
    lane = lax.broadcasted_iota(jnp.int32, (1, rows), 1)
    sublane = lax.broadcasted_iota(jnp.int32, (16, rows), 0)

    def is_group(slot):
        owner = index_of(slot % chips, (slot % chips > 0) == (slot < chips))
        group = jnp.where(owner * rows + lane < length, seg_all[slot], -1) + 1
        return jnp.where(jnp.broadcast_to(group, (16, rows)) == sublane, 1.0, 0.0)

    zeros40 = jnp.zeros((40, rows), F32)
    zeros48 = jnp.zeros((48, rows), F32)
    zeros8 = jnp.zeros((8, rows), F32)
    ones8 = jnp.ones((8, rows), F32)

    def columns(slot):
        return slice(slot * rows, (slot + 1) * rows)

    def query_columns(slot):
        return columns(position[slot])

    def take_key(slot, value):
        full = jnp.concatenate([value.astype(F32), is_group(slot), zeros40], axis=0)
        k_fm[:, columns(slot)] = full[:FM].astype(BF16)
        k_tm[columns(slot), :] = full.T.astype(BF16)

    def take_value(slot, value):
        full = jnp.concatenate([value.astype(F32), ones8, zeros48], axis=0)
        v_fm[:, columns(slot)] = full[:FM].astype(BF16)
        v_tm[columns(slot), :] = full.T.astype(BF16)

    def beside(pair, slots):
        return jnp.concatenate([slots(slot) for slot in pair], axis=1)

    def take_queries(pair, span):
        code = (1.0 - beside(pair, is_group)) * NEG_LARGE
        value = beside(pair, lambda slot: (q_slab[slot] if slot else q_in[chip]).astype(F32))
        wide40 = jnp.concatenate([zeros40, zeros40], axis=1)
        q_fm[:, span] = jnp.concatenate([value, code, wide40], axis=0).astype(BF16)

    arrived(some(seg_all, members - 1), recv_sem.at[SEG])

    def gather(number, own, slab, recv, take):
        take(0, own[chip])
        for i, pair in enumerate(PAIRS):
            pair = [slot for slot in pair if slot]
            arrived(some(slab, len(pair)), recv.at[i])
            for slot in pair:
                relay = recv.at[len(PAIRS) + i]
                copy(slab.at[slot], slab.at[chips + slot], send_sem.at[number], relay, twin).start()
            for slot in pair:
                take(slot, slab[slot])

    def gather_twin(slab, recv, take):
        for i, pair in enumerate(PAIRS):
            arrived(some(slab, 2), recv.at[len(PAIRS) + i])
            for slot in pair:
                take(chips + slot, slab[chips + slot])

    gather(K, k_in, k_slab, k_recv, take_key)
    gather_twin(k_slab, k_recv, take_key)
    gather(V, v_in, v_slab, v_recv, take_value)
    gather_twin(v_slab, v_recv, take_value)

    log_scale = math.log2(math.e) / math.sqrt(HEAD_DIM)
    score_scale = 1.0 / math.sqrt(HEAD_DIM)
    total = rows * members
    chunks = [slice(low, low + CHUNK) for low in range(0, total, CHUNK)]

    inverse = []
    for i, pair in enumerate(PAIRS):
        remote = [slot for slot in pair if slot]
        arrived(some(q_slab, len(remote)), q_recv.at[i])
        span = slice(i * TILE, (i + 1) * TILE)
        take_queries(pair, span)
        tile = q_fm[:, span]
        top = None
        for chunk in chunks:
            peak = jnp.max(nn(k_tm[chunk, :], tile), axis=0, keepdims=True)
            top = peak if top is None else jnp.maximum(top, peak)
        top = top * log_scale
        for chunk in chunks:
            p_ref[chunk, span] = jnp.exp2(nn(k_tm[chunk, :], tile) * log_scale - top).astype(BF16)
        accum = nn(v_fm[...], p_ref[:, span])
        denom = accum[HEAD_DIM : HEAD_DIM + 1]
        inverse.append(1.0 / denom)
        attn = (accum[:HEAD_DIM] / denom).astype(BF16)
        for j, slot in enumerate(pair):
            att_out[slot] = attn[:, columns(j)]
            if slot:
                copy(att_out.at[slot], attn_all.at[chip], send_sem.at[ATTN], recv_sem.at[ATTN], peer_of(slot)).start()
            else:
                attn_all[chip] = attn[:, columns(j)]
        scaled = q_fm[:HEAD_DIM, span].astype(F32) * (inverse[i] * score_scale)
        qs_fm[:, span] = jnp.concatenate([scaled, jnp.zeros((FM - HEAD_DIM, TILE), F32)], axis=0).astype(BF16)

    @pl.when(leads)
    def _():
        pl.semaphore_wait(barrier, members + groups - 2)
        for shift in range(1, members):
            peer = (dp, lax.rem(me + shift, members))
            pl.semaphore_signal(ready, inc=1, device_id=peer, device_id_type=MESH)

    loads[4].wait()
    loads[5].wait()
    arrived(some(attn_all, chips - 1), recv_sem.at[ATTN])
    stacked = [attn_all[h].astype(F32) for h in range(HEADS)] + [jnp.zeros((FEAT_PAD - FEAT, rows), F32)]
    attn_tm[...] = jnp.concatenate(stacked, axis=0).T.astype(BF16)
    copy(attn_tm, attn_in, send_sem.at[AT], recv_sem.at[AT], twin).start()
    own_live = me * rows + lax.broadcasted_iota(jnp.int32, (rows, 1), 0) < length
    output = nn(attn_tm[:, :FEAT], w_ref[...])
    error = jnp.where(own_live, output - t_ref[...].astype(F32), 0.0)
    dout_t = (2.0 * error).T
    dout_t = dout_t.astype(BF16)
    dt_ref[...] = dout_t.reshape(dt_ref.shape)
    for x in range(XS):
        copy(dt_ref.at[2 * x + 1 - core], dt_in.at[x], send_sem.at[DT], recv_sem.at[DT], twin).start()
    grad = nn(w_ref[...], dout_t)
    for h in range(HEADS):
        g_out[h] = grad[HEAD_DIM * h : HEAD_DIM * (h + 1)].astype(BF16)
    for s in order[::-1]:
        slot = chips - s
        copy(g_out.at[far(s)], g_slab.at[slot], send_sem.at[G], g_recv.at[group_of[slot]], peer_of(s)).start()

    loss_part = jnp.sum(jnp.sum(error * error, axis=0, keepdims=True), axis=1, keepdims=True)
    tile_own[...] = jnp.broadcast_to(loss_part, tile_own.shape)
    for shift in range(1, members):
        peer = (dp, lax.rem(me + shift, members))
        copy(tile_own, tile_all.at[members - shift], send_sem.at[TILE_SUM], recv_sem.at[TILE_SUM], peer).start()
    tile_all[0] = tile_own[...]
    arrived(attn_in, recv_sem.at[AT])
    arrived(dt_in, recv_sem.at[DT])
    tall = ZH * share
    left = jnp.concatenate(
        [jnp.concatenate([dt_ref[2 * x + core], dt_in[x]], axis=1) for x in range(XS)], axis=0
    )
    right = jnp.concatenate([attn_tm[...], attn_in[...]], axis=0)
    xa_ref[...] = nn(left, right[:, :X_LANES]).astype(BF16).reshape(XS, tall, X_LANES)

    @pl.when(jnp.logical_not(leads))
    def _():
        pl.semaphore_wait(ready, 1)

    for d in range(1, XS):
        x = lax.rem(cx + d, XS)
        item = copy(xa_ref.at[x], xa_in.at[XS - d - 1], send_sem.at[XA], recv_sem.at[XA], (x * ZS + cz, me))
        item.start()
    part = nn(left, right[:, X_LANES:])
    for x in range(XS):
        for j in range(ZH):
            low = x * tall + j * share
            za_ref[j, x] = part[low : low + share].astype(BF16)

    def along_z(source, landing, number):
        for j in range(ZH):
            target = ZH * core + j

            @pl.when(target != cz)
            def _():
                slot = lax.rem(cz - target + 2 * ZS - 1, ZS)
                device = (cx * ZS + target, me)
                copy(source.at[j], landing.at[slot], send_sem.at[number], recv_sem.at[number], device).start()

    along_z(za_ref, za_in, ZA)
    near = core == cz // ZH
    away = core != cz // ZH
    mine = lax.rem(cz, ZH)

    def take_grads(i, pair, span):
        wide = beside(pair, lambda slot: (g_slab[slot] if slot else g_out[chip]).astype(F32))
        attn = beside(pair, lambda slot: att_out[slot].astype(F32))
        delta = -jnp.sum(wide * attn, axis=0, keepdims=True)
        high = delta.astype(BF16).astype(F32)
        middle = (delta - high).astype(BF16).astype(F32)
        low = delta - high - middle
        index = lax.broadcasted_iota(jnp.int32, (8, TILE), 0)
        extra = jnp.where(index == 0, high, jnp.where(index == 1, middle, jnp.where(index == 2, low, 0.0)))
        g_fm[:, span] = jnp.concatenate([wide, extra, jnp.zeros((48, TILE), F32)], axis=0).astype(BF16)
        scaled = jnp.concatenate([wide * inverse[i], jnp.zeros((FM - HEAD_DIM, TILE), F32)], axis=0)
        gs_fm[:, span] = scaled.astype(BF16)

    def send_home(slot, out, ref, number):
        if slot:
            copy(out.at[slot], ref.at[chip], send_sem.at[number], recv_sem.at[number], peer_of(slot)).start()
        else:
            item = pltpu.make_async_copy(out.at[0], ref.at[chip], load_sem.at[(DQ, DV, DK).index(number)])
            item.start()
            local.append(item)

    local = []
    half = len(chunks) // 2
    each = CHUNK // rows

    def key_side(c, left, right, target, base=None):
        result = nt(left, right)[:HEAD_DIM]
        for j in range(each):
            slot = (c % half) * each + j
            value = result[:, columns(j)]
            target[slot] = value if base is None else base[slot] + value

    def swap(out_ref, in_ref, number):
        copy(out_ref, in_ref, send_sem.at[number], recv_sem.at[number], twin).start()

    def key_home(mine, in_ref, number, out, ref, home):
        arrived(in_ref, recv_sem.at[number])
        for slot in order + [0]:
            out[slot] = (mine[slot] + in_ref[slot]).astype(BF16)
            send_home(slot, out, ref, home)

    for i, pair in list(enumerate(PAIRS))[::-1]:
        remote = [slot for slot in pair if slot]
        arrived(some(g_slab, len(remote)), g_recv.at[i])
        span = slice(i * TILE, (i + 1) * TILE)
        take_grads(i, pair, span)
        first, last = i == len(PAIRS) - 1, i == 0
        for c in list(range(half, 2 * half)) + list(range(half)):
            side = v_twin if c >= half else v_own
            target = xv_out if c >= half and last else side
            key_side(c, gs_fm[:, span], p_ref[chunks[c], span], target, None if first else side)
            if last and c == 2 * half - 1:
                swap(xv_out, xv_in, XV)
        if last:
            arrived(xa_in, recv_sem.at[XA])
            summed = xa_ref[cx].astype(F32)
            for d in range(XS - 1):
                summed = summed + xa_in[d].astype(F32)
            for j in range(ZH):
                zb_ref[j] = summed[j * share : (j + 1) * share].astype(BF16)
            along_z(zb_ref, zb_in, ZB)
        tile = g_fm[:, span]
        for chunk in chunks:
            dprobs = nn(v_tm[chunk, :], tile)
            ds_ref[chunk, span] = (p_ref[chunk, span].astype(F32) * dprobs).astype(BF16)
        dq = nn(k_fm[...], ds_ref[:, span])
        dq = (dq[:HEAD_DIM] * (inverse[i] * score_scale)).astype(BF16)
        for j, slot in enumerate(pair):
            oq[slot] = dq[:, columns(j)]
            send_home(slot, oq, dq_ref, DQ)

    key_home(v_own, xv_in, XV, ov, dv_ref, DV)
    for c in range(half, 2 * half):
        key_side(c, qs_fm[...], ds_ref[chunks[c], :], xk_out)
    swap(xk_out, xk_in, XK)
    arrived(some(tile_all, members - 1), recv_sem.at[TILE_SUM])
    pack_loss = tile_all[0]
    for slot in range(1, members):
        pack_loss = pack_loss + tile_all[slot]
    sum_own[...] = jnp.where(lane == 0, pack_loss, length.astype(F32))
    for shift in range(1, groups):
        peer = (lax.rem(dp + shift, groups), me)
        copy(sum_own, sum_all.at[groups - shift], send_sem.at[ALL_SUM], recv_sem.at[ALL_SUM], peer).start()
    local.append(pltpu.make_async_copy(sum_own, sum_all.at[0], load_sem.at[3]))
    local[-1].start()

    for c in range(half):
        key_side(c, qs_fm[...], ds_ref[chunks[c], :], k_own)
    key_home(k_own, xk_in, XK, ok, dk_ref, DK)

    @pl.when(near)
    def _():
        arrived(some(za_in, ZS - 1), recv_sem.at[ZA])
        for x in range(XS):
            summed = za_ref[mine, x].astype(F32)
            for i in range(ZS - 1):
                summed = summed + za_in[i, x].astype(F32)
            xb_ref[x] = summed.astype(BF16)
        for d in range(1, XS):
            x = lax.rem(cx + d, XS)
            item = copy(xb_ref.at[x], xb_in.at[XS - d - 1], send_sem.at[XB], recv_sem.at[XB], (x * ZS + cz, me))
            item.start()

    third = features // 3

    @pl.when(near)
    def _():
        arrived(some(zb_in, ZS - 1), recv_sem.at[ZB])
        summed = zb_ref[mine].astype(F32)
        for i in range(ZS - 1):
            summed = summed + zb_in[i].astype(F32)
        arrived(xb_in, recv_sem.at[XB])
        other = xb_ref[cx].astype(F32)
        for i in range(XS - 1):
            other = other + xb_in[i].astype(F32)
        whole = jnp.concatenate([summed, other], axis=1)
        rolled = [whole] + [pltpu.roll(whole, FEAT_PAD - third * i, 1) for i in (1, 2)]
        turned = jnp.concatenate(rolled + [jnp.zeros((LANES - 3 * share, FEAT_PAD), F32)], axis=0).T
        for t in range(members):
            piece_ref[t] = turned[t * features : t * features + third].astype(BF16)
        for shift in range(1, members):
            target = lax.rem(me + shift, members)
            copy(piece_ref.at[target], yb_ref.at[chip], send_sem.at[Y], recv_sem.at[Y], (dp, target)).start()
        pltpu.make_async_copy(piece_ref.at[me], yb_ref.at[chip], load_sem.at[4]).start()

    arrived(some(sum_all, groups - 1), recv_sem.at[ALL_SUM])

    for ref, number in ((dv_ref, DV), (dq_ref, DQ), (dk_ref, DK)):
        arrived(some(ref, chips - 1), recv_sem.at[number])

    @pl.when(near)
    def _():
        arrived(some(yb_ref, chips - 1), recv_sem.at[Y])
        pltpu.make_async_copy(piece_ref.at[me], yb_ref.at[chip], load_sem.at[4]).wait()

    @pl.when(away)
    def _():
        arrived(yb_ref, recv_sem.at[Y])

    for item in local:
        item.wait()
    sent(some(seg_all, members - 1), send_sem.at[SEG])
    sent(some(k_slab, members - 1), send_sem.at[K])
    sent(some(v_slab, members - 1), send_sem.at[V])
    for ref, number in ((q_slab, Q), (attn_all, ATTN), (g_slab, G), (dq_ref, DQ), (dv_ref, DV), (dk_ref, DK)):
        sent(some(ref, chips - 1), send_sem.at[number])
    for ref, number in ((attn_tm, AT), (dt_in, DT), (xv_in, XV), (xk_in, XK)):
        sent(ref, send_sem.at[number])
    sent(some(tile_all, members - 1), send_sem.at[TILE_SUM])
    sent(some(sum_all, groups - 1), send_sem.at[ALL_SUM])

    sent(xa_in, send_sem.at[XA])

    @pl.when(near)
    def _():
        sent(some(za_ref, ZH - 1), send_sem.at[ZA])
        sent(some(zb_ref, ZH - 1), send_sem.at[ZB])
        sent(xb_in, send_sem.at[XB])
        sent(some(piece_ref, members - 1), send_sem.at[Y])

    @pl.when(away)
    def _():
        sent(za_ref, send_sem.at[ZA])
        sent(zb_ref, send_sem.at[ZB])


def scale_kernel(
    slots,
    total,
    sum_hbm,
    dq_hbm,
    dk_hbm,
    dv_hbm,
    yb_hbm,
    query_hbm,
    key_hbm,
    value_hbm,
    weight_ref,
    loss_ref,
    sum_ref,
    slab_ref,
    yb_ref,
    out_ref,
    in_sem,
    out_sem,
):
    sources = [(sum_hbm, sum_ref), (yb_hbm, yb_ref)]
    sources += [(ref, slab_ref.at[i]) for i, ref in enumerate((dv_hbm, dq_hbm, dk_hbm))]
    loads = [pltpu.make_async_copy(src, dst, in_sem.at[i]) for i, (src, dst) in enumerate(sources)]
    for load in loads:
        load.start()
    loads[0].wait()
    totals = sum_ref[0]
    for i in range(1, sum_ref.shape[0]):
        totals = totals + sum_ref[i]
    count = totals[:, 1:2]
    ratio = slots / count
    stores = []
    for i, target in enumerate((value_hbm, query_hbm, key_hbm)):
        loads[i + 2].wait()
        for h in range(HEADS):
            out_ref[i, HEAD_DIM * h : HEAD_DIM * (h + 1), :] = slab_ref[i, h].astype(F32) * ratio
        stores.append(pltpu.make_async_copy(out_ref.at[i], target, out_sem.at[i]))
        stores[-1].start()
    loads[1].wait()
    result = yb_ref[0].astype(F32)
    for i in range(1, yb_ref.shape[0]):
        result = result + yb_ref[i].astype(F32)
    result = result * (ratio / total)
    third, share = result.shape[0], weight_ref.shape[1]
    for i in range(3):
        weight_ref[i * third : (i + 1) * third, :] = result[:, i * share : (i + 1) * share]
    loss_ref[...] = totals[:, 0:1] / (count * WIDTH)
    for store in stores:
        store.wait()


def solution(mesh):
    members, groups = mesh.shape["patch"], mesh.shape["dp"]

    def local(query_rows, key_rows, value_rows, out_weight, target, lengths, segments):
        rows = query_rows.shape[1]
        total = rows * members
        chips = members // 2
        queries = rows * chips
        share = WIDTH // groups
        vmem = pl.BlockSpec(memory_space=pltpu.VMEM)
        hbm = pl.BlockSpec(memory_space=pltpu.HBM)
        dma = pltpu.SemaphoreType.DMA
        slab = (HEAD_DIM, rows)

        def heads(value):
            return value[0].T.reshape(HEADS, HEAD_DIM, rows)

        def bf(*shape):
            return pltpu.VMEM(shape, BF16)

        def fl(*shape):
            return pltpu.VMEM(shape, F32)

        outs = pl.pallas_call(
            functools.partial(kernel, members, groups),
            out_shape=(
                jax.ShapeDtypeStruct((HEADS, HEAD_DIM, rows), BF16),
                jax.ShapeDtypeStruct((HEADS, HEAD_DIM, rows), BF16),
                jax.ShapeDtypeStruct((HEADS, HEAD_DIM, rows), BF16),
                jax.ShapeDtypeStruct((chips, FEAT // members // 3, LANES), BF16),
                jax.ShapeDtypeStruct((groups, 1, LANES), F32),
            ),
            in_specs=[pl.BlockSpec(memory_space=pltpu.SMEM)] + [hbm] * 6,
            out_specs=(hbm,) * 5,
            scratch_shapes=[
                bf(HEADS, *slab),
                bf(HEADS, *slab),
                bf(HEADS, *slab),
                bf(FEAT, WIDTH),
                bf(rows, WIDTH),
                pltpu.VMEM((1, rows), jnp.int32),
                pltpu.VMEM((members, 1, rows), jnp.int32),
                bf(chips, *slab),
                bf(members, *slab),
                bf(members, *slab),
                bf(total, LANES),
                bf(total, LANES),
                bf(FM, total),
                bf(FM, total),
                bf(LANES, queries),
                bf(LANES, queries),
                bf(FM, queries),
                bf(FM, queries),
                bf(total, queries),
                bf(total, queries),
                bf(chips, *slab),
                bf(HEADS, *slab),
                bf(rows, FEAT_PAD),
                bf(rows, FEAT_PAD),
                bf(2 * XS, ZH * share, rows),
                bf(XS, ZH * share, rows),
                bf(HEADS, *slab),
                bf(chips, *slab),
                fl(chips, *slab),
                fl(chips, *slab),
                fl(chips, *slab),
                fl(chips, *slab),
                fl(chips, *slab),
                fl(chips, *slab),
                fl(chips, *slab),
                bf(chips, *slab),
                bf(chips, *slab),
                bf(chips, *slab),
                bf(XS, ZH * share, X_LANES),
                bf(XS - 1, ZH * share, X_LANES),
                bf(ZH, XS, share, Z_LANES),
                bf(ZS, XS, share, Z_LANES),
                bf(ZH, share, X_LANES),
                bf(ZS, share, X_LANES),
                bf(XS, share, Z_LANES),
                bf(XS - 1, share, Z_LANES),
                bf(members, FEAT // members // 3, LANES),
                fl(1, LANES),
                fl(members, 1, LANES),
                fl(1, LANES),
                pltpu.SemaphoreType.REGULAR,
                dma((6,)),
                dma((20,)),
                dma((16,)),
                dma((2 * len(PAIRS),)),
                dma((2 * len(PAIRS),)),
                dma((len(PAIRS),)),
                dma((len(PAIRS),)),
            ],
            compiler_params=pltpu.CompilerParams(collective_id=0, has_side_effects=True, vmem_limit_bytes=65900000),
            name="sublayer",
        )(
            lengths,
            segments,
            heads(query_rows),
            heads(key_rows),
            heads(value_rows),
            out_weight,
            target[0],
        )
        final = pl.pallas_call(
            functools.partial(scale_kernel, groups * total, total),
            out_shape=(
                jax.ShapeDtypeStruct((FEAT, rows), F32),
                jax.ShapeDtypeStruct((FEAT, rows), F32),
                jax.ShapeDtypeStruct((FEAT, rows), F32),
                jax.ShapeDtypeStruct((FEAT // members, share), F32),
                jax.ShapeDtypeStruct((1, 1), F32),
            ),
            in_specs=[hbm] * 5,
            out_specs=(hbm, hbm, hbm, vmem, vmem),
            scratch_shapes=[
                fl(groups, 1, LANES),
                bf(3, HEADS, *slab),
                bf(chips, FEAT // members // 3, LANES),
                fl(3, FEAT, rows),
                dma((5,)),
                dma((3,)),
            ],
            compiler_params=pltpu.CompilerParams(vmem_limit_bytes=65900000),
            name="scale",
        )(outs[4], *outs[:4])
        return (final[0].T[None], final[1].T[None], final[2].T[None], final[3], final[4].reshape(()))

    placed = (
        P("dp", "patch", None),
        P("dp", "patch", None),
        P("dp", "patch", None),
        P(),
        P("dp", "patch", None),
        P("dp"),
        P("dp", "patch"),
    )
    return jax.shard_map(
        local,
        mesh=mesh,
        in_specs=placed,
        out_specs=(
            P("dp", "patch", None),
            P("dp", "patch", None),
            P("dp", "patch", None),
            P("patch", "dp"),
            P(),
        ),
        check_vma=False,
    )
```

```python
import functools
import math

import jax
import jax.numpy as jnp
from jax import lax
from jax.experimental import pallas as pl
from jax.experimental.pallas import tpu as pltpu
from jax.sharding import PartitionSpec as P

MESH = pl.DeviceIdType.MESH
WIDTH = 1152
HEADS = 8
HEAD_DIM = 72
FEAT = 576
FEAT_PAD = 640
FM = 80
LANES = 128
SPAN = 256
TILE = 256
CHUNK = 256
NEG_LARGE = -1e30
F32 = jnp.float32
BF16 = jnp.bfloat16
XS, ZS = 4, 8
ZH = ZS // 2
X_LANES = 384
LEADER = 1
Z_LANES = 256
PAIRS = ((4, 0), (3, 5), (2, 6), (1, 7))


def nt(left, right):
    return lax.dot_general(left, right, (((1,), (1,)), ((), ())), preferred_element_type=F32)


def nn(left, right):
    return lax.dot_general(left, right, (((1,), (0,)), ((), ())), preferred_element_type=F32)


def tn(left, right):
    return lax.dot_general(left, right, (((0,), (0,)), ((), ())), preferred_element_type=F32)


def kernel(
    members,
    groups,
    len_ref,
    seg_ref,
    q_ref,
    k_ref,
    v_ref,
    w_hbm,
    t_hbm,
    dq_ref,
    dk_ref,
    dv_ref,
    yb_ref,
    sum_all,
    q_in,
    k_in,
    v_in,
    w_ref,
    t_ref,
    seg_row,
    seg_all,
    q_slab,
    k_slab,
    v_slab,
    k_tm,
    v_tm,
    k_fm,
    v_fm,
    q_fm,
    g_fm,
    qs_fm,
    gs_fm,
    p_ref,
    ds_ref,
    att_out,
    attn_all,
    attn_tm,
    attn_in,
    dt_ref,
    dt_in,
    g_out,
    g_slab,
    xv_out,
    xv_in,
    xk_out,
    xk_in,
    v_own,
    v_twin,
    k_own,
    oq,
    ok,
    ov,
    xa_ref,
    xa_in,
    za_ref,
    za_in,
    zb_ref,
    zb_in,
    xb_ref,
    xb_in,
    piece_ref,
    tile_own,
    tile_all,
    sum_own,
    ready,
    load_sem,
    send_sem,
    recv_sem,
    k_recv,
    v_recv,
    q_recv,
    g_recv,
):
    rows = t_ref.shape[0]
    chips = members // 2
    share = WIDTH // groups
    features = FEAT // members
    me = lax.axis_index("patch")
    dp = lax.axis_index("dp")
    chip, core = me // 2, me % 2
    cx, cz = dp // ZS, dp % ZS
    partner = chip * 2 + 1 - core
    side = 1 - core

    loads = [
        pltpu.make_async_copy(src, dst, load_sem.at[i])
        for i, (src, dst) in enumerate(
            [(seg_ref, seg_row), (k_ref, k_in), (v_ref, v_in), (q_ref, q_in), (w_hbm, w_ref), (t_hbm, t_ref)]
        )
    ]
    for load in loads:
        load.start()

    barrier = pltpu.get_barrier_semaphore()
    for shift in range(1, members):
        pl.semaphore_signal(barrier, inc=1, device_id=(dp, lax.rem(me + shift, members)), device_id_type=MESH)
    for load in loads[:4]:
        load.wait()
    seg_all[0] = seg_row[...]
    leads = me == LEADER

    @pl.when(jnp.logical_not(leads))
    def _():
        pl.semaphore_wait(barrier, members - 1)

    @pl.when(me == LEADER - 1)
    def _():
        pl.semaphore_signal(ready, inc=1, device_id=(dp, LEADER), device_id_type=MESH)

    @pl.when(leads)
    def _():
        pl.semaphore_wait(ready, 1)
        for shift in range(1, groups):
            pl.semaphore_signal(barrier, inc=1, device_id=(lax.rem(dp + shift, groups), me), device_id_type=MESH)

    def copy(src, dst, send, recv, device):
        return pltpu.make_async_remote_copy(
            src_ref=src, dst_ref=dst, send_sem=send, recv_sem=recv, device_id=device, device_id_type=MESH
        )

    def arrived(ref, recv):
        copy(ref, ref, send_sem.at[0], recv, (dp, partner)).wait_recv()

    def sent(ref, send):
        copy(ref, ref, send, recv_sem.at[0], (dp, partner)).wait_send()

    def some(ref, n):
        return ref.at[pl.ds(0, n)]

    SEG, ATTN, XV, XK, DQ, DK, DV, TILE_SUM, ALL_SUM, DT, AT, XA, ZA, ZB, XB, Y, K, V, Q, G = range(20)
    twin = (dp, partner)

    def far(shift):
        return lax.rem(chip + shift, chips)

    def index_of(shift, flip):
        return far(shift) * 2 + (1 - core if flip else core)

    def peer_of(shift):
        return (dp, index_of(shift, True))

    def other_of(shift):
        return (dp, index_of(shift, not shift))

    group_of = {slot: i for i, pair in enumerate(PAIRS) for slot in pair}
    order = [slot for pair in PAIRS for slot in pair if slot]
    position = {slot: i for i, slot in enumerate(slot for pair in PAIRS for slot in pair)}

    for s in order:
        copy(seg_row, seg_all.at[chips - s], send_sem.at[SEG], recv_sem.at[SEG], peer_of(s)).start()
    for s in order + [0]:
        slot = chips + (chips - s) % chips
        copy(seg_row, seg_all.at[slot], send_sem.at[SEG], recv_sem.at[SEG], other_of(s)).start()
    for number, source, slab, recv in ((K, k_in, k_slab, k_recv), (V, v_in, v_slab, v_recv)):
        copy(source.at[chip], slab.at[chips], send_sem.at[number], recv.at[len(PAIRS)], twin).start()
    for number, source, slab, recv in ((K, k_in, k_slab, k_recv), (V, v_in, v_slab, v_recv), (Q, q_in, q_slab, q_recv)):
        for s in order:
            slot = chips - s
            copy(source.at[far(s)], slab.at[slot], send_sem.at[number], recv.at[group_of[slot]], peer_of(s)).start()

    length = len_ref[0]
    lane = lax.broadcasted_iota(jnp.int32, (1, rows), 1)
    sublane = lax.broadcasted_iota(jnp.int32, (16, rows), 0)

    def is_group(slot):
        owner = index_of(slot % chips, (slot % chips > 0) == (slot < chips))
        group = jnp.where(owner * rows + lane < length, seg_all[slot], -1) + 1
        return jnp.where(jnp.broadcast_to(group, (16, rows)) == sublane, 1.0, 0.0)

    zeros40 = jnp.zeros((40, rows), F32)
    zeros48 = jnp.zeros((48, rows), F32)
    zeros8 = jnp.zeros((8, rows), F32)
    ones8 = jnp.ones((8, rows), F32)

    def columns(slot):
        return slice(slot * rows, (slot + 1) * rows)

    def query_columns(slot):
        return columns(position[slot])

    def take_key(slot, value):
        full = jnp.concatenate([value.astype(F32), is_group(slot), zeros40], axis=0)
        k_fm[:, columns(slot)] = full[:FM].astype(BF16)
        k_tm[columns(slot), :] = full.T.astype(BF16)

    def take_value(slot, value):
        full = jnp.concatenate([value.astype(F32), ones8, zeros48], axis=0)
        v_fm[:, columns(slot)] = full[:FM].astype(BF16)
        v_tm[columns(slot), :] = full.T.astype(BF16)

    def beside(pair, slots):
        return jnp.concatenate([slots(slot) for slot in pair], axis=1)

    def take_queries(pair, span):
        code = (1.0 - beside(pair, is_group)) * NEG_LARGE
        value = beside(pair, lambda slot: (q_slab[slot] if slot else q_in[chip]).astype(F32))
        wide40 = jnp.concatenate([zeros40, zeros40], axis=1)
        q_fm[:, span] = jnp.concatenate([value, code, wide40], axis=0).astype(BF16)

    arrived(some(seg_all, members - 1), recv_sem.at[SEG])

    def gather(number, own, slab, recv, take):
        take(0, own[chip])
        for i, pair in enumerate(PAIRS):
            pair = [slot for slot in pair if slot]
            arrived(some(slab, len(pair)), recv.at[i])
            for slot in pair:
                relay = recv.at[len(PAIRS) + i]
                copy(slab.at[slot], slab.at[chips + slot], send_sem.at[number], relay, twin).start()
            for slot in pair:
                take(slot, slab[slot])

    def gather_twin(slab, recv, take):
        for i, pair in enumerate(PAIRS):
            arrived(some(slab, 2), recv.at[len(PAIRS) + i])
            for slot in pair:
                take(chips + slot, slab[chips + slot])

    gather(K, k_in, k_slab, k_recv, take_key)
    gather_twin(k_slab, k_recv, take_key)
    gather(V, v_in, v_slab, v_recv, take_value)
    gather_twin(v_slab, v_recv, take_value)

    log_scale = math.log2(math.e) / math.sqrt(HEAD_DIM)
    score_scale = 1.0 / math.sqrt(HEAD_DIM)
    total = rows * members
    chunks = [slice(low, low + CHUNK) for low in range(0, total, CHUNK)]

    inverse = []
    for i, pair in enumerate(PAIRS):
        remote = [slot for slot in pair if slot]
        arrived(some(q_slab, len(remote)), q_recv.at[i])
        span = slice(i * TILE, (i + 1) * TILE)
        take_queries(pair, span)
        tile = q_fm[:, span]
        top = None
        for chunk in chunks:
            peak = jnp.max(nn(k_tm[chunk, :], tile), axis=0, keepdims=True)
            top = peak if top is None else jnp.maximum(top, peak)
        top = top * log_scale
        for chunk in chunks:
            p_ref[chunk, span] = jnp.exp2(nn(k_tm[chunk, :], tile) * log_scale - top).astype(BF16)
        accum = nn(v_fm[...], p_ref[:, span])
        denom = accum[HEAD_DIM : HEAD_DIM + 1]
        inverse.append(1.0 / denom)
        attn = (accum[:HEAD_DIM] / denom).astype(BF16)
        for j, slot in enumerate(pair):
            att_out[slot] = attn[:, columns(j)]
            if slot:
                copy(att_out.at[slot], attn_all.at[chip], send_sem.at[ATTN], recv_sem.at[ATTN], peer_of(slot)).start()
            else:
                attn_all[chip] = attn[:, columns(j)]
        scaled = q_fm[:HEAD_DIM, span].astype(F32) * (inverse[i] * score_scale)
        qs_fm[:, span] = jnp.concatenate([scaled, jnp.zeros((FM - HEAD_DIM, TILE), F32)], axis=0).astype(BF16)

    @pl.when(leads)
    def _():
        pl.semaphore_wait(barrier, members + groups - 2)
        for shift in range(1, members):
            peer = (dp, lax.rem(me + shift, members))
            pl.semaphore_signal(ready, inc=1, device_id=peer, device_id_type=MESH)

    loads[4].wait()
    loads[5].wait()
    arrived(some(attn_all, chips - 1), recv_sem.at[ATTN])
    stacked = [attn_all[h].astype(F32) for h in range(HEADS)] + [jnp.zeros((FEAT_PAD - FEAT, rows), F32)]
    attn_tm[...] = jnp.concatenate(stacked, axis=0).T.astype(BF16)
    copy(attn_tm, attn_in, send_sem.at[AT], recv_sem.at[AT], twin).start()
    own_live = me * rows + lax.broadcasted_iota(jnp.int32, (rows, 1), 0) < length
    output = nn(attn_tm[:, :FEAT], w_ref[...])
    error = jnp.where(own_live, output - t_ref[...].astype(F32), 0.0)
    dout_t = (2.0 * error).T
    dout_t = dout_t.astype(BF16)
    dt_ref[...] = dout_t.reshape(dt_ref.shape)
    for x in range(XS):
        copy(dt_ref.at[2 * x + 1 - side], dt_in.at[x], send_sem.at[DT], recv_sem.at[DT], twin).start()
    grad = nn(w_ref[...], dout_t)
    for h in range(HEADS):
        g_out[h] = grad[HEAD_DIM * h : HEAD_DIM * (h + 1)].astype(BF16)
    for s in order[::-1]:
        slot = chips - s
        copy(g_out.at[far(s)], g_slab.at[slot], send_sem.at[G], g_recv.at[group_of[slot]], peer_of(s)).start()

    loss_part = jnp.sum(jnp.sum(error * error, axis=0, keepdims=True), axis=1, keepdims=True)
    tile_own[...] = jnp.broadcast_to(loss_part, tile_own.shape)
    for shift in range(1, members):
        peer = (dp, lax.rem(me + shift, members))
        copy(tile_own, tile_all.at[members - shift], send_sem.at[TILE_SUM], recv_sem.at[TILE_SUM], peer).start()
    tile_all[0] = tile_own[...]
    arrived(attn_in, recv_sem.at[AT])
    arrived(dt_in, recv_sem.at[DT])
    tall = ZH * share
    left = jnp.concatenate(
        [jnp.concatenate([dt_ref[2 * x + side], dt_in[x]], axis=1) for x in range(XS)], axis=0
    )
    right = jnp.concatenate([attn_tm[...], attn_in[...]], axis=0)
    xa_ref[...] = nn(left, right[:, :X_LANES]).astype(BF16).reshape(XS, tall, X_LANES)

    @pl.when(jnp.logical_not(leads))
    def _():
        pl.semaphore_wait(ready, 1)

    for d in range(1, XS):
        x = lax.rem(cx + d, XS)
        item = copy(xa_ref.at[x], xa_in.at[XS - d - 1], send_sem.at[XA], recv_sem.at[XA], (x * ZS + cz, me))
        item.start()
    part = nn(left, right[:, X_LANES:])
    for x in range(XS):
        for j in range(ZH):
            low = x * tall + j * share
            za_ref[j, x] = part[low : low + share].astype(BF16)

    def along_z(source, landing, number):
        for j in range(ZH):
            target = ZH * side + j

            @pl.when(target != cz)
            def _():
                slot = lax.rem(cz - target + 2 * ZS - 1, ZS)
                device = (cx * ZS + target, me)
                copy(source.at[j], landing.at[slot], send_sem.at[number], recv_sem.at[number], device).start()

    along_z(za_ref, za_in, ZA)
    near = side == cz // ZH
    away = side != cz // ZH
    mine = lax.rem(cz, ZH)

    def take_grads(i, pair, span):
        wide = beside(pair, lambda slot: (g_slab[slot] if slot else g_out[chip]).astype(F32))
        attn = beside(pair, lambda slot: att_out[slot].astype(F32))
        delta = -jnp.sum(wide * attn, axis=0, keepdims=True)
        high = delta.astype(BF16).astype(F32)
        middle = (delta - high).astype(BF16).astype(F32)
        low = delta - high - middle
        index = lax.broadcasted_iota(jnp.int32, (8, TILE), 0)
        extra = jnp.where(index == 0, high, jnp.where(index == 1, middle, jnp.where(index == 2, low, 0.0)))
        g_fm[:, span] = jnp.concatenate([wide, extra, jnp.zeros((48, TILE), F32)], axis=0).astype(BF16)
        scaled = jnp.concatenate([wide * inverse[i], jnp.zeros((FM - HEAD_DIM, TILE), F32)], axis=0)
        gs_fm[:, span] = scaled.astype(BF16)

    def send_home(slot, out, ref, number):
        if slot:
            copy(out.at[slot], ref.at[chip], send_sem.at[number], recv_sem.at[number], peer_of(slot)).start()
        else:
            item = pltpu.make_async_copy(out.at[0], ref.at[chip], load_sem.at[(DQ, DV, DK).index(number)])
            item.start()
            local.append(item)

    local = []
    half = len(chunks) // 2
    each = CHUNK // rows

    def key_side(c, left, right, target, base=None):
        result = nt(left, right)[:HEAD_DIM]
        for j in range(each):
            slot = (c % half) * each + j
            value = result[:, columns(j)]
            target[slot] = value if base is None else base[slot] + value

    def swap(out_ref, in_ref, number):
        copy(out_ref, in_ref, send_sem.at[number], recv_sem.at[number], twin).start()

    def key_home(mine, in_ref, number, out, ref, home):
        arrived(in_ref, recv_sem.at[number])
        for slot in order + [0]:
            out[slot] = (mine[slot] + in_ref[slot]).astype(BF16)
            send_home(slot, out, ref, home)

    for i, pair in list(enumerate(PAIRS))[::-1]:
        remote = [slot for slot in pair if slot]
        arrived(some(g_slab, len(remote)), g_recv.at[i])
        span = slice(i * TILE, (i + 1) * TILE)
        take_grads(i, pair, span)
        first, last = i == len(PAIRS) - 1, i == 0
        for c in list(range(half, 2 * half)) + list(range(half)):
            base = v_twin if c >= half else v_own
            target = xv_out if c >= half and last else base
            key_side(c, gs_fm[:, span], p_ref[chunks[c], span], target, None if first else base)
            if last and c == 2 * half - 1:
                swap(xv_out, xv_in, XV)
        if last:
            arrived(some(tile_all, members - 1), recv_sem.at[TILE_SUM])
            pack_loss = tile_all[0]
            for slot in range(1, members):
                pack_loss = pack_loss + tile_all[slot]
            sum_own[...] = jnp.where(lane == 0, pack_loss, length.astype(F32))
            for shift in range(1, groups):
                peer = (lax.rem(dp + shift, groups), me)
                copy(sum_own, sum_all.at[groups - shift], send_sem.at[ALL_SUM], recv_sem.at[ALL_SUM], peer).start()
            local.append(pltpu.make_async_copy(sum_own, sum_all.at[0], load_sem.at[3]))
            local[-1].start()
            arrived(xa_in, recv_sem.at[XA])
            summed = xa_ref[cx].astype(F32)
            for d in range(XS - 1):
                summed = summed + xa_in[d].astype(F32)
            for j in range(ZH):
                zb_ref[j] = summed[j * share : (j + 1) * share].astype(BF16)
            along_z(zb_ref, zb_in, ZB)
        tile = g_fm[:, span]
        for chunk in chunks:
            dprobs = nn(v_tm[chunk, :], tile)
            ds_ref[chunk, span] = (p_ref[chunk, span].astype(F32) * dprobs).astype(BF16)
        dq = nn(k_fm[...], ds_ref[:, span])
        dq = (dq[:HEAD_DIM] * (inverse[i] * score_scale)).astype(BF16)
        for j, slot in enumerate(pair):
            oq[slot] = dq[:, columns(j)]
            send_home(slot, oq, dq_ref, DQ)

    key_home(v_own, xv_in, XV, ov, dv_ref, DV)
    for c in range(half, 2 * half):
        key_side(c, qs_fm[...], ds_ref[chunks[c], :], xk_out)
    swap(xk_out, xk_in, XK)
    for c in range(half):
        key_side(c, qs_fm[...], ds_ref[chunks[c], :], k_own)
    key_home(k_own, xk_in, XK, ok, dk_ref, DK)

    @pl.when(near)
    def _():
        arrived(some(za_in, ZS - 1), recv_sem.at[ZA])
        for x in range(XS):
            summed = za_ref[mine, x].astype(F32)
            for i in range(ZS - 1):
                summed = summed + za_in[i, x].astype(F32)
            xb_ref[x] = summed.astype(BF16)
        for d in range(1, XS):
            x = lax.rem(cx + d, XS)
            item = copy(xb_ref.at[x], xb_in.at[XS - d - 1], send_sem.at[XB], recv_sem.at[XB], (x * ZS + cz, me))
            item.start()

    third = features // 3

    @pl.when(near)
    def _():
        arrived(some(zb_in, ZS - 1), recv_sem.at[ZB])
        summed = zb_ref[mine].astype(F32)
        for i in range(ZS - 1):
            summed = summed + zb_in[i].astype(F32)
        arrived(xb_in, recv_sem.at[XB])
        other = xb_ref[cx].astype(F32)
        for i in range(XS - 1):
            other = other + xb_in[i].astype(F32)
        whole = jnp.concatenate([summed, other], axis=1)
        rolled = [whole] + [pltpu.roll(whole, FEAT_PAD - third * i, 1) for i in (1, 2)]
        turned = jnp.concatenate(rolled + [jnp.zeros((LANES - 3 * share, FEAT_PAD), F32)], axis=0).T
        for t in range(members):
            piece_ref[t] = turned[t * features : t * features + third].astype(BF16)
        for shift in range(1, members):
            target = lax.rem(me + shift, members)
            copy(piece_ref.at[target], yb_ref.at[chip], send_sem.at[Y], recv_sem.at[Y], (dp, target)).start()
        pltpu.make_async_copy(piece_ref.at[me], yb_ref.at[chip], load_sem.at[4]).start()

    arrived(some(sum_all, groups - 1), recv_sem.at[ALL_SUM])

    for ref, number in ((dv_ref, DV), (dq_ref, DQ), (dk_ref, DK)):
        arrived(some(ref, chips - 1), recv_sem.at[number])

    @pl.when(near)
    def _():
        arrived(some(yb_ref, chips - 1), recv_sem.at[Y])
        pltpu.make_async_copy(piece_ref.at[me], yb_ref.at[chip], load_sem.at[4]).wait()

    @pl.when(away)
    def _():
        arrived(yb_ref, recv_sem.at[Y])

    for item in local:
        item.wait()
    sent(some(seg_all, members - 1), send_sem.at[SEG])
    sent(some(k_slab, members - 1), send_sem.at[K])
    sent(some(v_slab, members - 1), send_sem.at[V])
    for ref, number in ((q_slab, Q), (attn_all, ATTN), (g_slab, G), (dq_ref, DQ), (dv_ref, DV), (dk_ref, DK)):
        sent(some(ref, chips - 1), send_sem.at[number])
    for ref, number in ((attn_tm, AT), (dt_in, DT), (xv_in, XV), (xk_in, XK)):
        sent(ref, send_sem.at[number])
    sent(some(tile_all, members - 1), send_sem.at[TILE_SUM])
    sent(some(sum_all, groups - 1), send_sem.at[ALL_SUM])

    sent(xa_in, send_sem.at[XA])

    @pl.when(near)
    def _():
        sent(some(za_ref, ZH - 1), send_sem.at[ZA])
        sent(some(zb_ref, ZH - 1), send_sem.at[ZB])
        sent(xb_in, send_sem.at[XB])
        sent(some(piece_ref, members - 1), send_sem.at[Y])

    @pl.when(away)
    def _():
        sent(za_ref, send_sem.at[ZA])
        sent(zb_ref, send_sem.at[ZB])


def scale_kernel(
    slots,
    total,
    sum_hbm,
    dq_hbm,
    dk_hbm,
    dv_hbm,
    yb_hbm,
    query_hbm,
    key_hbm,
    value_hbm,
    weight_hbm,
    loss_hbm,
    sum_ref,
    slab_ref,
    yb_ref,
    out_ref,
    weight_ref,
    loss_ref,
    in_sem,
    out_sem,
):
    def fetch(src, dst, i):
        return pltpu.make_async_copy(src, dst, in_sem.at[i])

    fetch(sum_hbm, sum_ref, 0).start()
    grads = list(enumerate(((dv_hbm, value_hbm), (dq_hbm, query_hbm), (dk_hbm, key_hbm))))
    pieces = [pl.ds(h, 2) for h in range(0, HEADS, 2)]
    for i, (source, _) in grads:
        for piece in pieces:
            fetch(source.at[piece], slab_ref.at[i, piece], i + 2).start()
    fetch(yb_hbm, yb_ref, 1).start()
    fetch(sum_hbm, sum_ref, 0).wait()
    totals = sum_ref[0]
    for i in range(1, sum_ref.shape[0]):
        totals = totals + sum_ref[i]
    count = totals[:, 1:2]
    ratio = slots / count
    stores = []
    for i, (source, target) in grads:
        fetch(source, slab_ref.at[i], i + 2).wait()
        for h in range(HEADS):
            out_ref[i, HEAD_DIM * h : HEAD_DIM * (h + 1), :] = slab_ref[i, h].astype(F32) * ratio
            if h % 2:
                part = pl.ds(HEAD_DIM * (h - 1), 2 * HEAD_DIM)
                pltpu.make_async_copy(out_ref.at[i, part], target.at[part], out_sem.at[i]).start()
        stores.append(pltpu.make_async_copy(out_ref.at[i], target, out_sem.at[i]))
    fetch(yb_hbm, yb_ref, 1).wait()
    result = yb_ref[0].astype(F32)
    for i in range(1, yb_ref.shape[0]):
        result = result + yb_ref[i].astype(F32)
    result = result * (ratio / total)
    third, share = result.shape[0], weight_ref.shape[1]
    for i in range(3):
        weight_ref[i * third : (i + 1) * third, :] = result[:, i * share : (i + 1) * share]
    loss_ref[...] = totals[:, 0:1] / (count * WIDTH)
    for i, (source, target) in enumerate(((weight_ref, weight_hbm), (loss_ref, loss_hbm))):
        stores.append(pltpu.make_async_copy(source, target, out_sem.at[3 + i]))
        stores[-1].start()
    for store in stores:
        store.wait()


def solution(mesh):
    members, groups = mesh.shape["patch"], mesh.shape["dp"]

    def local(query_rows, key_rows, value_rows, out_weight, target, lengths, segments):
        rows = query_rows.shape[1]
        total = rows * members
        chips = members // 2
        queries = rows * chips
        share = WIDTH // groups
        hbm = pl.BlockSpec(memory_space=pltpu.HBM)
        dma = pltpu.SemaphoreType.DMA
        slab = (HEAD_DIM, rows)

        def heads(value):
            return value[0].T.reshape(HEADS, HEAD_DIM, rows)

        def bf(*shape):
            return pltpu.VMEM(shape, BF16)

        def fl(*shape):
            return pltpu.VMEM(shape, F32)

        outs = pl.pallas_call(
            functools.partial(kernel, members, groups),
            out_shape=(
                jax.ShapeDtypeStruct((HEADS, HEAD_DIM, rows), BF16),
                jax.ShapeDtypeStruct((HEADS, HEAD_DIM, rows), BF16),
                jax.ShapeDtypeStruct((HEADS, HEAD_DIM, rows), BF16),
                jax.ShapeDtypeStruct((chips, FEAT // members // 3, LANES), BF16),
                jax.ShapeDtypeStruct((groups, 1, LANES), F32),
            ),
            in_specs=[pl.BlockSpec(memory_space=pltpu.SMEM)] + [hbm] * 6,
            out_specs=(hbm,) * 5,
            scratch_shapes=[
                bf(HEADS, *slab),
                bf(HEADS, *slab),
                bf(HEADS, *slab),
                bf(FEAT, WIDTH),
                bf(rows, WIDTH),
                pltpu.VMEM((1, rows), jnp.int32),
                pltpu.VMEM((members, 1, rows), jnp.int32),
                bf(chips, *slab),
                bf(members, *slab),
                bf(members, *slab),
                bf(total, LANES),
                bf(total, LANES),
                bf(FM, total),
                bf(FM, total),
                bf(LANES, queries),
                bf(LANES, queries),
                bf(FM, queries),
                bf(FM, queries),
                bf(total, queries),
                bf(total, queries),
                bf(chips, *slab),
                bf(HEADS, *slab),
                bf(rows, FEAT_PAD),
                bf(rows, FEAT_PAD),
                bf(2 * XS, ZH * share, rows),
                bf(XS, ZH * share, rows),
                bf(HEADS, *slab),
                bf(chips, *slab),
                fl(chips, *slab),
                fl(chips, *slab),
                fl(chips, *slab),
                fl(chips, *slab),
                fl(chips, *slab),
                fl(chips, *slab),
                fl(chips, *slab),
                bf(chips, *slab),
                bf(chips, *slab),
                bf(chips, *slab),
                bf(XS, ZH * share, X_LANES),
                bf(XS - 1, ZH * share, X_LANES),
                bf(ZH, XS, share, Z_LANES),
                bf(ZS, XS, share, Z_LANES),
                bf(ZH, share, X_LANES),
                bf(ZS, share, X_LANES),
                bf(XS, share, Z_LANES),
                bf(XS - 1, share, Z_LANES),
                bf(members, FEAT // members // 3, LANES),
                fl(1, LANES),
                fl(members, 1, LANES),
                fl(1, LANES),
                pltpu.SemaphoreType.REGULAR,
                dma((6,)),
                dma((20,)),
                dma((16,)),
                dma((2 * len(PAIRS),)),
                dma((2 * len(PAIRS),)),
                dma((len(PAIRS),)),
                dma((len(PAIRS),)),
            ],
            compiler_params=pltpu.CompilerParams(collective_id=0, has_side_effects=True, vmem_limit_bytes=65900000),
            name="sublayer",
        )(
            lengths,
            segments,
            heads(query_rows),
            heads(key_rows),
            heads(value_rows),
            out_weight,
            target[0],
        )
        final = pl.pallas_call(
            functools.partial(scale_kernel, groups * total, total),
            out_shape=(
                jax.ShapeDtypeStruct((FEAT, rows), F32),
                jax.ShapeDtypeStruct((FEAT, rows), F32),
                jax.ShapeDtypeStruct((FEAT, rows), F32),
                jax.ShapeDtypeStruct((FEAT // members, share), F32),
                jax.ShapeDtypeStruct((1, 1), F32),
            ),
            in_specs=[hbm] * 5,
            out_specs=(hbm,) * 5,
            scratch_shapes=[
                fl(groups, 1, LANES),
                bf(3, HEADS, *slab),
                bf(chips, FEAT // members // 3, LANES),
                fl(3, FEAT, rows),
                fl(FEAT // members, share),
                fl(1, 1),
                dma((5,)),
                dma((5,)),
            ],
            compiler_params=pltpu.CompilerParams(vmem_limit_bytes=65900000),
            name="scale",
        )(outs[4], *outs[:4])
        return (final[0].T[None], final[1].T[None], final[2].T[None], final[3], final[4].reshape(()))

    placed = (
        P("dp", "patch", None),
        P("dp", "patch", None),
        P("dp", "patch", None),
        P(),
        P("dp", "patch", None),
        P("dp"),
        P("dp", "patch"),
    )
    return jax.shard_map(
        local,
        mesh=mesh,
        in_specs=placed,
        out_specs=(
            P("dp", "patch", None),
            P("dp", "patch", None),
            P("dp", "patch", None),
            P("patch", "dp"),
            P(),
        ),
        check_vma=False,
    )
```

```python
import functools
import math

import jax
import jax.numpy as jnp
from jax import lax
from jax.experimental import pallas as pl
from jax.experimental.pallas import tpu as pltpu
from jax.sharding import PartitionSpec as P

MESH = pl.DeviceIdType.MESH
WIDTH = 1152
HEADS = 8
HEAD_DIM = 72
FEAT = 576
FEAT_PAD = 640
FM = 80
LANES = 128
SPAN = 256
TILE = 256
CHUNK = 256
NEG_LARGE = -1e30
F32 = jnp.float32
BF16 = jnp.bfloat16
XS, ZS = 4, 8
ZH = ZS // 2
X_LANES = 384
LEADER = 1
Z_LANES = 256
PAIRS = ((4, 0), (3, 5), (2, 6), (1, 7))


def nt(left, right):
    return lax.dot_general(left, right, (((1,), (1,)), ((), ())), preferred_element_type=F32)


def nn(left, right):
    return lax.dot_general(left, right, (((1,), (0,)), ((), ())), preferred_element_type=F32)


def tn(left, right):
    return lax.dot_general(left, right, (((0,), (0,)), ((), ())), preferred_element_type=F32)


def kernel(
    members,
    groups,
    len_ref,
    seg_ref,
    q_ref,
    k_ref,
    v_ref,
    w_hbm,
    t_hbm,
    dq_ref,
    dk_ref,
    dv_ref,
    yb_ref,
    sum_all,
    q_in,
    k_in,
    v_in,
    w_ref,
    t_ref,
    len_row,
    seg_row,
    seg_all,
    q_slab,
    k_slab,
    v_slab,
    k_tm,
    v_tm,
    k_fm,
    v_fm,
    q_fm,
    g_fm,
    qs_fm,
    gs_fm,
    p_ref,
    ds_ref,
    att_out,
    attn_all,
    attn_tm,
    attn_in,
    dt_ref,
    dt_in,
    g_out,
    g_slab,
    xv_out,
    xv_in,
    xk_out,
    xk_in,
    v_own,
    v_twin,
    k_own,
    oq,
    ok,
    ov,
    xa_ref,
    xa_in,
    za_ref,
    za_in,
    zb_ref,
    zb_in,
    xb_ref,
    xb_in,
    piece_ref,
    tile_own,
    tile_all,
    sum_own,
    ready,
    load_sem,
    send_sem,
    recv_sem,
    k_recv,
    v_recv,
    q_recv,
    g_recv,
):
    rows = t_ref.shape[0]
    chips = members // 2
    share = WIDTH // groups
    features = FEAT // members
    me = lax.axis_index("patch")
    dp = lax.axis_index("dp")
    chip, core = me // 2, me % 2
    cx, cz = dp // ZS, dp % ZS
    partner = chip * 2 + 1 - core
    side = 1 - core

    loads = [
        pltpu.make_async_copy(src, dst, load_sem.at[i])
        for i, (src, dst) in enumerate(
            [(seg_ref, seg_row), (k_ref, k_in), (v_ref, v_in), (q_ref, q_in), (w_hbm, w_ref), (t_hbm, t_ref), (len_ref, len_row)]
        )
    ]
    for load in loads:
        load.start()

    barrier = pltpu.get_barrier_semaphore()
    for shift in range(1, members):
        pl.semaphore_signal(barrier, inc=1, device_id=(dp, lax.rem(me + shift, members)), device_id_type=MESH)
    for load in loads[:4] + loads[6:]:
        load.wait()
    seg_all[0] = seg_row[...]
    leads = me == LEADER

    @pl.when(jnp.logical_not(leads))
    def _():
        pl.semaphore_wait(barrier, members - 1)

    @pl.when(me == LEADER - 1)
    def _():
        pl.semaphore_signal(ready, inc=1, device_id=(dp, LEADER), device_id_type=MESH)

    @pl.when(leads)
    def _():
        pl.semaphore_wait(ready, 1)
        for shift in range(1, groups):
            pl.semaphore_signal(barrier, inc=1, device_id=(lax.rem(dp + shift, groups), me), device_id_type=MESH)

    def copy(src, dst, send, recv, device):
        return pltpu.make_async_remote_copy(
            src_ref=src, dst_ref=dst, send_sem=send, recv_sem=recv, device_id=device, device_id_type=MESH
        )

    def arrived(ref, recv):
        copy(ref, ref, send_sem.at[0], recv, (dp, partner)).wait_recv()

    def sent(ref, send):
        copy(ref, ref, send, recv_sem.at[0], (dp, partner)).wait_send()

    def some(ref, n):
        return ref.at[pl.ds(0, n)]

    SEG, ATTN, XV, XK, DQ, DK, DV, TILE_SUM, ALL_SUM, DT, AT, XA, ZA, ZB, XB, Y, K, V, Q, G = range(20)
    twin = (dp, partner)

    def far(shift):
        return lax.rem(chip + shift, chips)

    def index_of(shift, flip):
        return far(shift) * 2 + (1 - core if flip else core)

    def peer_of(shift):
        return (dp, index_of(shift, True))

    def other_of(shift):
        return (dp, index_of(shift, not shift))

    group_of = {slot: i for i, pair in enumerate(PAIRS) for slot in pair}
    order = [slot for pair in PAIRS for slot in pair if slot]
    position = {slot: i for i, slot in enumerate(slot for pair in PAIRS for slot in pair)}

    for s in order:
        copy(seg_row, seg_all.at[chips - s], send_sem.at[SEG], recv_sem.at[SEG], peer_of(s)).start()
    for s in order + [0]:
        slot = chips + (chips - s) % chips
        copy(seg_row, seg_all.at[slot], send_sem.at[SEG], recv_sem.at[SEG], other_of(s)).start()
    for number, source, slab, recv in ((K, k_in, k_slab, k_recv), (V, v_in, v_slab, v_recv)):
        copy(source.at[chip], slab.at[chips], send_sem.at[number], recv.at[len(PAIRS)], twin).start()
    for number, source, slab, recv in ((K, k_in, k_slab, k_recv), (V, v_in, v_slab, v_recv), (Q, q_in, q_slab, q_recv)):
        for s in order:
            slot = chips - s
            copy(source.at[far(s)], slab.at[slot], send_sem.at[number], recv.at[group_of[slot]], peer_of(s)).start()

    length = len_row[...]
    lane = lax.broadcasted_iota(jnp.int32, (1, rows), 1)
    sublane = lax.broadcasted_iota(jnp.int32, (16, rows), 0)

    def is_group(slot):
        owner = index_of(slot % chips, (slot % chips > 0) == (slot < chips))
        group = jnp.where(owner * rows + lane < length, seg_all[slot], -1) + 1
        return jnp.where(jnp.broadcast_to(group, (16, rows)) == sublane, 1.0, 0.0)

    zeros40 = jnp.zeros((40, rows), F32)
    zeros48 = jnp.zeros((48, rows), F32)
    zeros8 = jnp.zeros((8, rows), F32)
    ones8 = jnp.ones((8, rows), F32)

    def columns(slot):
        return slice(slot * rows, (slot + 1) * rows)

    def query_columns(slot):
        return columns(position[slot])

    def take_key(slot, value):
        full = jnp.concatenate([value.astype(F32), is_group(slot), zeros40], axis=0)
        k_fm[:, columns(slot)] = full[:FM].astype(BF16)
        k_tm[columns(slot), :] = full.T.astype(BF16)

    def take_value(slot, value):
        full = jnp.concatenate([value.astype(F32), ones8, zeros48], axis=0)
        v_fm[:, columns(slot)] = full[:FM].astype(BF16)
        v_tm[columns(slot), :] = full.T.astype(BF16)

    def beside(pair, slots):
        return jnp.concatenate([slots(slot) for slot in pair], axis=1)

    def take_queries(pair, span):
        code = (1.0 - beside(pair, is_group)) * NEG_LARGE
        value = beside(pair, lambda slot: (q_slab[slot] if slot else q_in[chip]).astype(F32))
        wide40 = jnp.concatenate([zeros40, zeros40], axis=1)
        q_fm[:, span] = jnp.concatenate([value, code, wide40], axis=0).astype(BF16)

    arrived(some(seg_all, members - 1), recv_sem.at[SEG])

    def gather(number, own, slab, recv, take):
        take(0, own[chip])
        for i, pair in enumerate(PAIRS):
            pair = [slot for slot in pair if slot]
            arrived(some(slab, len(pair)), recv.at[i])
            for slot in pair:
                relay = recv.at[len(PAIRS) + i]
                copy(slab.at[slot], slab.at[chips + slot], send_sem.at[number], relay, twin).start()
            for slot in pair:
                take(slot, slab[slot])

    def gather_twin(slab, recv, take):
        for i, pair in enumerate(PAIRS):
            arrived(some(slab, 2), recv.at[len(PAIRS) + i])
            for slot in pair:
                take(chips + slot, slab[chips + slot])

    gather(K, k_in, k_slab, k_recv, take_key)
    gather_twin(k_slab, k_recv, take_key)
    gather(V, v_in, v_slab, v_recv, take_value)
    gather_twin(v_slab, v_recv, take_value)

    log_scale = math.log2(math.e) / math.sqrt(HEAD_DIM)
    score_scale = 1.0 / math.sqrt(HEAD_DIM)
    total = rows * members
    chunks = [slice(low, low + CHUNK) for low in range(0, total, CHUNK)]

    inverse = []
    for i, pair in enumerate(PAIRS):
        remote = [slot for slot in pair if slot]
        arrived(some(q_slab, len(remote)), q_recv.at[i])
        span = slice(i * TILE, (i + 1) * TILE)
        take_queries(pair, span)
        tile = q_fm[:, span]
        top = None
        for chunk in chunks:
            peak = jnp.max(nn(k_tm[chunk, :], tile), axis=0, keepdims=True)
            top = peak if top is None else jnp.maximum(top, peak)
        top = top * log_scale
        for chunk in chunks:
            p_ref[chunk, span] = jnp.exp2(nn(k_tm[chunk, :], tile) * log_scale - top).astype(BF16)
        accum = nn(v_fm[...], p_ref[:, span])
        denom = accum[HEAD_DIM : HEAD_DIM + 1]
        inverse.append(1.0 / denom)
        attn = (accum[:HEAD_DIM] / denom).astype(BF16)
        for j, slot in enumerate(pair):
            att_out[slot] = attn[:, columns(j)]
            if slot:
                copy(att_out.at[slot], attn_all.at[chip], send_sem.at[ATTN], recv_sem.at[ATTN], peer_of(slot)).start()
            else:
                attn_all[chip] = attn[:, columns(j)]
        scaled = q_fm[:HEAD_DIM, span].astype(F32) * (inverse[i] * score_scale)
        qs_fm[:, span] = jnp.concatenate([scaled, jnp.zeros((FM - HEAD_DIM, TILE), F32)], axis=0).astype(BF16)

    @pl.when(leads)
    def _():
        pl.semaphore_wait(barrier, members + groups - 2)
        for shift in range(1, members):
            peer = (dp, lax.rem(me + shift, members))
            pl.semaphore_signal(ready, inc=1, device_id=peer, device_id_type=MESH)

    loads[4].wait()
    loads[5].wait()
    arrived(some(attn_all, chips - 1), recv_sem.at[ATTN])
    stacked = [attn_all[h].astype(F32) for h in range(HEADS)] + [jnp.zeros((FEAT_PAD - FEAT, rows), F32)]
    attn_tm[...] = jnp.concatenate(stacked, axis=0).T.astype(BF16)
    copy(attn_tm, attn_in, send_sem.at[AT], recv_sem.at[AT], twin).start()
    own_live = me * rows + lax.broadcasted_iota(jnp.int32, (rows, 1), 0) < length
    output = nn(attn_tm[:, :FEAT], w_ref[...])
    error = jnp.where(own_live, output - t_ref[...].astype(F32), 0.0)
    dout_t = (2.0 * error).T
    dout_t = dout_t.astype(BF16)
    dt_ref[...] = dout_t.reshape(dt_ref.shape)
    for x in range(XS):
        copy(dt_ref.at[2 * x + 1 - side], dt_in.at[x], send_sem.at[DT], recv_sem.at[DT], twin).start()
    grad = nn(w_ref[...], dout_t)
    for h in range(HEADS):
        g_out[h] = grad[HEAD_DIM * h : HEAD_DIM * (h + 1)].astype(BF16)
    for s in order[::-1]:
        slot = chips - s
        copy(g_out.at[far(s)], g_slab.at[slot], send_sem.at[G], g_recv.at[group_of[slot]], peer_of(s)).start()

    loss_part = jnp.sum(jnp.sum(error * error, axis=0, keepdims=True), axis=1, keepdims=True)
    tile_own[...] = jnp.broadcast_to(loss_part, tile_own.shape)
    for shift in range(1, members):
        peer = (dp, lax.rem(me + shift, members))
        copy(tile_own, tile_all.at[members - shift], send_sem.at[TILE_SUM], recv_sem.at[TILE_SUM], peer).start()
    tile_all[0] = tile_own[...]
    arrived(attn_in, recv_sem.at[AT])
    arrived(dt_in, recv_sem.at[DT])
    tall = ZH * share
    left = jnp.concatenate(
        [jnp.concatenate([dt_ref[2 * x + side], dt_in[x]], axis=1) for x in range(XS)], axis=0
    )
    right = jnp.concatenate([attn_tm[...], attn_in[...]], axis=0)
    xa_ref[...] = nn(left, right[:, :X_LANES]).astype(BF16).reshape(XS, tall, X_LANES)

    @pl.when(jnp.logical_not(leads))
    def _():
        pl.semaphore_wait(ready, 1)

    for d in range(1, XS):
        x = lax.rem(cx + d, XS)
        item = copy(xa_ref.at[x], xa_in.at[XS - d - 1], send_sem.at[XA], recv_sem.at[XA], (x * ZS + cz, me))
        item.start()
    part = nn(left, right[:, X_LANES:])
    for x in range(XS):
        for j in range(ZH):
            low = x * tall + j * share
            za_ref[j, x] = part[low : low + share].astype(BF16)

    def along_z(source, landing, number):
        for j in range(ZH):
            target = ZH * side + j

            @pl.when(target != cz)
            def _():
                slot = lax.rem(cz - target + 2 * ZS - 1, ZS)
                device = (cx * ZS + target, me)
                copy(source.at[j], landing.at[slot], send_sem.at[number], recv_sem.at[number], device).start()

    along_z(za_ref, za_in, ZA)
    near = side == cz // ZH
    away = side != cz // ZH
    mine = lax.rem(cz, ZH)

    def take_grads(i, pair, span):
        wide = beside(pair, lambda slot: (g_slab[slot] if slot else g_out[chip]).astype(F32))
        attn = beside(pair, lambda slot: att_out[slot].astype(F32))
        delta = -jnp.sum(wide * attn, axis=0, keepdims=True)
        high = delta.astype(BF16).astype(F32)
        middle = (delta - high).astype(BF16).astype(F32)
        low = delta - high - middle
        index = lax.broadcasted_iota(jnp.int32, (8, TILE), 0)
        extra = jnp.where(index == 0, high, jnp.where(index == 1, middle, jnp.where(index == 2, low, 0.0)))
        g_fm[:, span] = jnp.concatenate([wide, extra, jnp.zeros((48, TILE), F32)], axis=0).astype(BF16)
        scaled = jnp.concatenate([wide * inverse[i], jnp.zeros((FM - HEAD_DIM, TILE), F32)], axis=0)
        gs_fm[:, span] = scaled.astype(BF16)

    def send_home(slot, out, ref, number):
        if slot:
            copy(out.at[slot], ref.at[chip], send_sem.at[number], recv_sem.at[number], peer_of(slot)).start()
        else:
            item = pltpu.make_async_copy(out.at[0], ref.at[chip], load_sem.at[(DQ, DV, DK).index(number)])
            item.start()
            local.append(item)

    local = []
    half = len(chunks) // 2
    each = CHUNK // rows

    def key_side(c, left, right, target, base=None):
        result = nt(left, right)[:HEAD_DIM]
        for j in range(each):
            slot = (c % half) * each + j
            value = result[:, columns(j)]
            target[slot] = value if base is None else base[slot] + value

    def swap(out_ref, in_ref, number):
        copy(out_ref, in_ref, send_sem.at[number], recv_sem.at[number], twin).start()

    def key_home(mine, in_ref, number, out, ref, home):
        arrived(in_ref, recv_sem.at[number])
        for slot in order + [0]:
            out[slot] = (mine[slot] + in_ref[slot]).astype(BF16)
            send_home(slot, out, ref, home)

    for i, pair in list(enumerate(PAIRS))[::-1]:
        remote = [slot for slot in pair if slot]
        arrived(some(g_slab, len(remote)), g_recv.at[i])
        span = slice(i * TILE, (i + 1) * TILE)
        take_grads(i, pair, span)
        first, last = i == len(PAIRS) - 1, i == 0
        for c in list(range(half, 2 * half)) + list(range(half)):
            base = v_twin if c >= half else v_own
            target = xv_out if c >= half and last else base
            key_side(c, gs_fm[:, span], p_ref[chunks[c], span], target, None if first else base)
            if last and c == 2 * half - 1:
                swap(xv_out, xv_in, XV)
        if last:
            arrived(some(tile_all, members - 1), recv_sem.at[TILE_SUM])
            pack_loss = tile_all[0]
            for slot in range(1, members):
                pack_loss = pack_loss + tile_all[slot]
            sum_own[...] = jnp.where(lane == 0, pack_loss, length.astype(F32))
            for shift in range(1, groups):
                peer = (lax.rem(dp + shift, groups), me)
                copy(sum_own, sum_all.at[groups - shift], send_sem.at[ALL_SUM], recv_sem.at[ALL_SUM], peer).start()
            local.append(pltpu.make_async_copy(sum_own, sum_all.at[0], load_sem.at[3]))
            local[-1].start()
        if i == 1:
            arrived(xa_in, recv_sem.at[XA])
            summed = xa_ref[cx].astype(F32)
            for d in range(XS - 1):
                summed = summed + xa_in[d].astype(F32)
            for j in range(ZH):
                zb_ref[j] = summed[j * share : (j + 1) * share].astype(BF16)
            along_z(zb_ref, zb_in, ZB)
        tile = g_fm[:, span]
        for chunk in chunks:
            dprobs = nn(v_tm[chunk, :], tile)
            ds_ref[chunk, span] = (p_ref[chunk, span].astype(F32) * dprobs).astype(BF16)
        dq = nn(k_fm[...], ds_ref[:, span])
        dq = (dq[:HEAD_DIM] * (inverse[i] * score_scale)).astype(BF16)
        for j, slot in enumerate(pair):
            oq[slot] = dq[:, columns(j)]
            send_home(slot, oq, dq_ref, DQ)

    key_home(v_own, xv_in, XV, ov, dv_ref, DV)
    for c in range(half, 2 * half):
        key_side(c, qs_fm[...], ds_ref[chunks[c], :], xk_out)
    swap(xk_out, xk_in, XK)
    for c in range(half):
        key_side(c, qs_fm[...], ds_ref[chunks[c], :], k_own)
    key_home(k_own, xk_in, XK, ok, dk_ref, DK)

    @pl.when(near)
    def _():
        arrived(some(za_in, ZS - 1), recv_sem.at[ZA])
        for x in range(XS):
            summed = za_ref[mine, x].astype(F32)
            for i in range(ZS - 1):
                summed = summed + za_in[i, x].astype(F32)
            xb_ref[x] = summed.astype(BF16)
        for d in range(1, XS):
            x = lax.rem(cx + d, XS)
            item = copy(xb_ref.at[x], xb_in.at[XS - d - 1], send_sem.at[XB], recv_sem.at[XB], (x * ZS + cz, me))
            item.start()

    third = features // 3

    @pl.when(near)
    def _():
        arrived(some(zb_in, ZS - 1), recv_sem.at[ZB])
        summed = zb_ref[mine].astype(F32)
        for i in range(ZS - 1):
            summed = summed + zb_in[i].astype(F32)
        arrived(xb_in, recv_sem.at[XB])
        other = xb_ref[cx].astype(F32)
        for i in range(XS - 1):
            other = other + xb_in[i].astype(F32)
        whole = jnp.concatenate([summed, other], axis=1)
        rolled = [whole] + [pltpu.roll(whole, FEAT_PAD - third * i, 1) for i in (1, 2)]
        turned = jnp.concatenate(rolled + [jnp.zeros((LANES - 3 * share, FEAT_PAD), F32)], axis=0).T
        for t in range(members):
            piece_ref[t] = turned[t * features : t * features + third].astype(BF16)
        for shift in range(1, members):
            target = lax.rem(me + shift, members)
            copy(piece_ref.at[target], yb_ref.at[chip], send_sem.at[Y], recv_sem.at[Y], (dp, target)).start()
        pltpu.make_async_copy(piece_ref.at[me], yb_ref.at[chip], load_sem.at[4]).start()

    arrived(some(sum_all, groups - 1), recv_sem.at[ALL_SUM])

    for ref, number in ((dv_ref, DV), (dq_ref, DQ), (dk_ref, DK)):
        arrived(some(ref, chips - 1), recv_sem.at[number])

    @pl.when(near)
    def _():
        arrived(some(yb_ref, chips - 1), recv_sem.at[Y])
        pltpu.make_async_copy(piece_ref.at[me], yb_ref.at[chip], load_sem.at[4]).wait()

    @pl.when(away)
    def _():
        arrived(yb_ref, recv_sem.at[Y])

    for item in local:
        item.wait()
    sent(some(seg_all, members - 1), send_sem.at[SEG])
    sent(some(k_slab, members - 1), send_sem.at[K])
    sent(some(v_slab, members - 1), send_sem.at[V])
    for ref, number in ((q_slab, Q), (attn_all, ATTN), (g_slab, G), (dq_ref, DQ), (dv_ref, DV), (dk_ref, DK)):
        sent(some(ref, chips - 1), send_sem.at[number])
    for ref, number in ((attn_tm, AT), (dt_in, DT), (xv_in, XV), (xk_in, XK)):
        sent(ref, send_sem.at[number])
    sent(some(tile_all, members - 1), send_sem.at[TILE_SUM])
    sent(some(sum_all, groups - 1), send_sem.at[ALL_SUM])

    sent(xa_in, send_sem.at[XA])

    @pl.when(near)
    def _():
        sent(some(za_ref, ZH - 1), send_sem.at[ZA])
        sent(some(zb_ref, ZH - 1), send_sem.at[ZB])
        sent(xb_in, send_sem.at[XB])
        sent(some(piece_ref, members - 1), send_sem.at[Y])

    @pl.when(away)
    def _():
        sent(za_ref, send_sem.at[ZA])
        sent(zb_ref, send_sem.at[ZB])


def scale_kernel(
    slots,
    total,
    sum_hbm,
    dq_hbm,
    dk_hbm,
    dv_hbm,
    yb_hbm,
    query_hbm,
    key_hbm,
    value_hbm,
    weight_hbm,
    loss_hbm,
    sum_ref,
    slab_ref,
    yb_ref,
    out_ref,
    weight_ref,
    loss_ref,
    in_sem,
    out_sem,
):
    def fetch(src, dst, i):
        return pltpu.make_async_copy(src, dst, in_sem.at[i])

    fetch(sum_hbm, sum_ref, 0).start()
    grads = list(enumerate(((dv_hbm, value_hbm), (dq_hbm, query_hbm), (dk_hbm, key_hbm))))
    pieces = [pl.ds(h, 2) for h in range(0, HEADS, 2)]
    for i, (source, _) in grads:
        for piece in pieces:
            fetch(source.at[piece], slab_ref.at[i, piece], i + 2).start()
    fetch(yb_hbm, yb_ref, 1).start()
    fetch(sum_hbm, sum_ref, 0).wait()
    totals = sum_ref[0]
    for i in range(1, sum_ref.shape[0]):
        totals = totals + sum_ref[i]
    count = totals[:, 1:2]
    ratio = slots / count
    stores = []
    for i, (source, target) in grads:
        fetch(source, slab_ref.at[i], i + 2).wait()
        for h in range(HEADS):
            out_ref[i, HEAD_DIM * h : HEAD_DIM * (h + 1), :] = slab_ref[i, h].astype(F32) * ratio
            if h % 2:
                part = pl.ds(HEAD_DIM * (h - 1), 2 * HEAD_DIM)
                pltpu.make_async_copy(out_ref.at[i, part], target.at[part], out_sem.at[i]).start()
        stores.append(pltpu.make_async_copy(out_ref.at[i], target, out_sem.at[i]))
    fetch(yb_hbm, yb_ref, 1).wait()
    result = yb_ref[0].astype(F32)
    for i in range(1, yb_ref.shape[0]):
        result = result + yb_ref[i].astype(F32)
    result = result * (ratio / total)
    third, share = result.shape[0], weight_ref.shape[1]
    for i in range(3):
        weight_ref[i * third : (i + 1) * third, :] = result[:, i * share : (i + 1) * share]
    loss_ref[...] = totals[:, 0:1] / (count * WIDTH)
    for i, (source, target) in enumerate(((weight_ref, weight_hbm), (loss_ref, loss_hbm))):
        stores.append(pltpu.make_async_copy(source, target, out_sem.at[3 + i]))
        stores[-1].start()
    for store in stores:
        store.wait()


def solution(mesh):
    members, groups = mesh.shape["patch"], mesh.shape["dp"]

    def local(query_rows, key_rows, value_rows, out_weight, target, lengths, segments):
        rows = query_rows.shape[1]
        total = rows * members
        chips = members // 2
        queries = rows * chips
        share = WIDTH // groups
        hbm = pl.BlockSpec(memory_space=pltpu.HBM)
        dma = pltpu.SemaphoreType.DMA
        slab = (HEAD_DIM, rows)

        def heads(value):
            return value[0].T.reshape(HEADS, HEAD_DIM, rows)

        def bf(*shape):
            return pltpu.VMEM(shape, BF16)

        def fl(*shape):
            return pltpu.VMEM(shape, F32)

        outs = pl.pallas_call(
            functools.partial(kernel, members, groups),
            out_shape=(
                jax.ShapeDtypeStruct((HEADS, HEAD_DIM, rows), BF16),
                jax.ShapeDtypeStruct((HEADS, HEAD_DIM, rows), BF16),
                jax.ShapeDtypeStruct((HEADS, HEAD_DIM, rows), BF16),
                jax.ShapeDtypeStruct((chips, FEAT // members // 3, LANES), BF16),
                jax.ShapeDtypeStruct((groups, 1, LANES), F32),
            ),
            in_specs=[hbm] * 7,
            out_specs=(hbm,) * 5,
            scratch_shapes=[
                bf(HEADS, *slab),
                bf(HEADS, *slab),
                bf(HEADS, *slab),
                bf(FEAT, WIDTH),
                bf(rows, WIDTH),
                pltpu.VMEM((1, 1), jnp.int32),
                pltpu.VMEM((1, rows), jnp.int32),
                pltpu.VMEM((members, 1, rows), jnp.int32),
                bf(chips, *slab),
                bf(members, *slab),
                bf(members, *slab),
                bf(total, LANES),
                bf(total, LANES),
                bf(FM, total),
                bf(FM, total),
                bf(LANES, queries),
                bf(LANES, queries),
                bf(FM, queries),
                bf(FM, queries),
                bf(total, queries),
                bf(total, queries),
                bf(chips, *slab),
                bf(HEADS, *slab),
                bf(rows, FEAT_PAD),
                bf(rows, FEAT_PAD),
                bf(2 * XS, ZH * share, rows),
                bf(XS, ZH * share, rows),
                bf(HEADS, *slab),
                bf(chips, *slab),
                fl(chips, *slab),
                fl(chips, *slab),
                fl(chips, *slab),
                fl(chips, *slab),
                fl(chips, *slab),
                fl(chips, *slab),
                fl(chips, *slab),
                bf(chips, *slab),
                bf(chips, *slab),
                bf(chips, *slab),
                bf(XS, ZH * share, X_LANES),
                bf(XS - 1, ZH * share, X_LANES),
                bf(ZH, XS, share, Z_LANES),
                bf(ZS, XS, share, Z_LANES),
                bf(ZH, share, X_LANES),
                bf(ZS, share, X_LANES),
                bf(XS, share, Z_LANES),
                bf(XS - 1, share, Z_LANES),
                bf(members, FEAT // members // 3, LANES),
                fl(1, LANES),
                fl(members, 1, LANES),
                fl(1, LANES),
                pltpu.SemaphoreType.REGULAR,
                dma((7,)),
                dma((20,)),
                dma((16,)),
                dma((2 * len(PAIRS),)),
                dma((2 * len(PAIRS),)),
                dma((len(PAIRS),)),
                dma((len(PAIRS),)),
            ],
            compiler_params=pltpu.CompilerParams(collective_id=0, has_side_effects=True, vmem_limit_bytes=65900000),
            name="sublayer",
        )(
            lengths.reshape(1, 1),
            segments,
            heads(query_rows),
            heads(key_rows),
            heads(value_rows),
            out_weight,
            target[0],
        )
        final = pl.pallas_call(
            functools.partial(scale_kernel, groups * total, total),
            out_shape=(
                jax.ShapeDtypeStruct((FEAT, rows), F32),
                jax.ShapeDtypeStruct((FEAT, rows), F32),
                jax.ShapeDtypeStruct((FEAT, rows), F32),
                jax.ShapeDtypeStruct((FEAT // members, share), F32),
                jax.ShapeDtypeStruct((1, 1), F32),
            ),
            in_specs=[hbm] * 5,
            out_specs=(hbm,) * 5,
            scratch_shapes=[
                fl(groups, 1, LANES),
                bf(3, HEADS, *slab),
                bf(chips, FEAT // members // 3, LANES),
                fl(3, FEAT, rows),
                fl(FEAT // members, share),
                fl(1, 1),
                dma((5,)),
                dma((5,)),
            ],
            compiler_params=pltpu.CompilerParams(vmem_limit_bytes=65900000),
            name="scale",
        )(outs[4], *outs[:4])
        return (final[0].T[None], final[1].T[None], final[2].T[None], final[3], final[4].reshape(()))

    placed = (
        P("dp", "patch", None),
        P("dp", "patch", None),
        P("dp", "patch", None),
        P(),
        P("dp", "patch", None),
        P("dp"),
        P("dp", "patch"),
    )
    return jax.shard_map(
        local,
        mesh=mesh,
        in_specs=placed,
        out_specs=(
            P("dp", "patch", None),
            P("dp", "patch", None),
            P("dp", "patch", None),
            P("patch", "dp"),
            P(),
        ),
        check_vma=False,
    )
```
